32 devices in a mesh: dp: 1 (over z), tp: 4 (over y), cp: 8 (over x, core).
Axes of the slice: x: 4, y: 4, z: 1, core: 2. Of those that a mesh axis runs over, the one named last changes fastest.
The devices are a block of a 4x4x8 slice.
Arguments:
- hidden_in: bfloat16 [512, 5120], P(('dp', 'cp', 'tp'))
- positions: int32 [512], P(('dp', 'cp', 'tp'))
- cache_len: int32 [1], P('dp')
- cache_k: bfloat16 [32768, 1024], P(('dp', 'cp', 'tp'))
- cache_v: bfloat16 [32768, 1024], P(('dp', 'cp', 'tp'))
- norm1_gain: bfloat16 [5120], replicated
- w_query: bfloat16 [5120, 4096], P(None, 'tp')
- w_key: bfloat16 [5120, 1024], P(None, 'tp')
- w_value: bfloat16 [5120, 1024], P(None, 'tp')
- w_out: bfloat16 [4096, 5120], P('tp')
- norm2_gain: bfloat16 [5120], replicated
- w_gate: bfloat16 [5120, 14336], P(None, 'tp')
- w_up: bfloat16 [5120, 14336], P(None, 'tp')
- w_down: bfloat16 [14336, 5120], P('tp')
Outputs:
- output: bfloat16 [512, 5120], P(('dp', 'cp', 'tp'))
All inputs are finite; a program needn't handle non-finite values.
Results may differ from the reference program's by a relative error of at most 0.00935577.
Values are sent between devices in bfloat16 or wider.
A program may use at most 768 MiB of HBM per device.

```python
import math
import jax
import jax.numpy as jnp
from jax import lax

TOKENS = 512
PREFIX = 32768
D_MODEL = 5120
Q_HEADS = 32
KV_HEADS = 8
HEAD_DIM = 128
FFN_DIM = 14336
SHARD_COUNT = 32
SHARD_ROWS = 16
QUERY_BLOCK = 16
ROPE_BASE = 500000.0
NORM_EPS = 1e-5


def normal_draw(rand_key, out_shape, spread):
    return (jax.random.normal(rand_key, out_shape, jnp.float32) * spread).astype(jnp.bfloat16)


def setup_inputs(seed: int = 0, part: int = 0) -> dict:
    base_key = jax.random.key(seed)
    part_keys = jax.random.split(jax.random.fold_in(base_key, part), 4)
    shared_keys = jax.random.split(jax.random.key(seed + 1), 9)
    cache_len = jax.random.randint(part_keys[0], (1,), PREFIX // 16, PREFIX + 1, dtype=jnp.int32)
    row_ids = jnp.arange(TOKENS, dtype=jnp.int32)
    half_rows = SHARD_ROWS // 2
    shard_ids = row_ids // SHARD_ROWS
    within = row_ids % SHARD_ROWS
    segment = jnp.where(within < half_rows, shard_ids, 2 * SHARD_COUNT - 1 - shard_ids)
    positions = cache_len[0] + segment * half_rows + within % half_rows
    qk_std = math.log((PREFIX + TOKENS) / 4.0) ** 0.25
    width_std = D_MODEL ** -0.5
    kv_width = KV_HEADS * HEAD_DIM
    return {
        'hidden_in': normal_draw(part_keys[1], (TOKENS, D_MODEL), 1.0),
        'positions': positions,
        'cache_len': cache_len,
        'cache_k': normal_draw(part_keys[2], (PREFIX, kv_width), qk_std),
        'cache_v': normal_draw(part_keys[3], (PREFIX, kv_width), 1.0),
        'norm1_gain': (1.0 + 0.3 * jax.random.normal(shared_keys[0], (D_MODEL,), jnp.float32)).astype(jnp.bfloat16),
        'w_query': normal_draw(shared_keys[1], (D_MODEL, Q_HEADS * HEAD_DIM), qk_std * width_std),
        'w_key': normal_draw(shared_keys[2], (D_MODEL, kv_width), qk_std * width_std),
        'w_value': normal_draw(shared_keys[3], (D_MODEL, kv_width), width_std),
        'w_out': normal_draw(shared_keys[4], (Q_HEADS * HEAD_DIM, D_MODEL), 2.0 * (Q_HEADS * HEAD_DIM) ** -0.5),
        'norm2_gain': (1.0 + 0.3 * jax.random.normal(shared_keys[5], (D_MODEL,), jnp.float32)).astype(jnp.bfloat16),
        'w_gate': normal_draw(shared_keys[6], (D_MODEL, FFN_DIM), width_std),
        'w_up': normal_draw(shared_keys[7], (D_MODEL, FFN_DIM), width_std),
        'w_down': normal_draw(shared_keys[8], (FFN_DIM, D_MODEL), FFN_DIM ** -0.5),
    }


def rms_norm(hidden, norm_gain):
    values = hidden.astype(jnp.float32)
    inv_rms = lax.rsqrt(jnp.mean(values * values, axis=-1, keepdims=True) + NORM_EPS)
    return (values * inv_rms * norm_gain.astype(jnp.float32)).astype(jnp.bfloat16)


def rotary(projected, positions):
    half_dim = HEAD_DIM // 2
    inv_freq = 1.0 / (ROPE_BASE ** (jnp.arange(half_dim, dtype=jnp.float32) * (2.0 / HEAD_DIM)))
    angles = positions.astype(jnp.float32)[:, None] * inv_freq[None, :]
    expand = (angles.shape[0],) + (1,) * (projected.ndim - 2) + (half_dim,)
    cos_table = jnp.cos(angles).reshape(expand)
    sin_table = jnp.sin(angles).reshape(expand)
    first_half = projected[..., :half_dim]
    second_half = projected[..., half_dim:]
    rotated = jnp.concatenate([first_half * cos_table - second_half * sin_table, second_half * cos_table + first_half * sin_table], axis=-1)
    return rotated.astype(jnp.bfloat16)


def reference(hidden_in, positions, cache_len, cache_k, cache_v, norm1_gain, w_query, w_key, w_value, w_out, norm2_gain, w_gate, w_up, w_down):
    groups = Q_HEADS // KV_HEADS
    block_count = TOKENS // QUERY_BLOCK
    score_scale = 1.0 / math.sqrt(HEAD_DIM)
    normed = rms_norm(hidden_in, norm1_gain)
    queries = rotary(jnp.dot(normed, w_query, preferred_element_type=jnp.float32).reshape(TOKENS, KV_HEADS, groups, HEAD_DIM), positions)
    new_keys = rotary(jnp.dot(normed, w_key, preferred_element_type=jnp.float32).reshape(TOKENS, KV_HEADS, HEAD_DIM), positions)
    new_values = jnp.dot(normed, w_value, preferred_element_type=jnp.float32).astype(jnp.bfloat16).reshape(TOKENS, KV_HEADS, HEAD_DIM)
    head_keys = jnp.moveaxis(new_keys, 1, 0)
    head_values = jnp.moveaxis(new_values, 1, 0)
    cached_keys = jnp.moveaxis(cache_k.reshape(PREFIX, KV_HEADS, HEAD_DIM), 1, 0)
    cached_values = jnp.moveaxis(cache_v.reshape(PREFIX, KV_HEADS, HEAD_DIM), 1, 0)
    cache_valid = jnp.arange(PREFIX) < cache_len[0]
    query_blocks = jnp.moveaxis(queries.reshape(block_count, QUERY_BLOCK, KV_HEADS, groups, HEAD_DIM), 2, 1)
    position_blocks = positions.reshape(block_count, QUERY_BLOCK)

    def attend_block(block_item):
        block_queries, block_pos = block_item
        causal = positions[None, None, :] <= block_pos[None, :, None]

        def attend_head(head_item):
            head_queries, cache_key_head, cache_value_head, new_key_head, new_value_head = head_item
            query_wide = head_queries.astype(jnp.float32)
            cache_scores = jnp.einsum('rgd,sd->grs', query_wide, cache_key_head.astype(jnp.float32)) * score_scale
            new_scores = jnp.einsum('rgd,sd->grs', query_wide, new_key_head.astype(jnp.float32)) * score_scale
            cache_scores = jnp.where(cache_valid[None, None, :], cache_scores, -jnp.inf)
            new_scores = jnp.where(causal, new_scores, -jnp.inf)
            row_max = jnp.maximum(jnp.max(cache_scores, axis=-1, keepdims=True), jnp.max(new_scores, axis=-1, keepdims=True))
            cache_probs = jnp.exp(cache_scores - row_max)
            new_probs = jnp.exp(new_scores - row_max)
            normalizer = jnp.sum(cache_probs, axis=-1, keepdims=True) + jnp.sum(new_probs, axis=-1, keepdims=True)
            weighted = jnp.einsum('grs,sd->grd', cache_probs.astype(jnp.bfloat16).astype(jnp.float32), cache_value_head.astype(jnp.float32))
            weighted = weighted + jnp.einsum('grs,sd->grd', new_probs.astype(jnp.bfloat16).astype(jnp.float32), new_value_head.astype(jnp.float32))
            return (weighted / normalizer).astype(jnp.bfloat16)

        return lax.map(attend_head, (block_queries, cached_keys, cached_values, head_keys, head_values))

    attended = lax.map(attend_block, (query_blocks, position_blocks))
    attended = jnp.transpose(attended, (0, 3, 1, 2, 4)).reshape(TOKENS, Q_HEADS * HEAD_DIM)
    residual_mid = (hidden_in.astype(jnp.float32) + jnp.dot(attended, w_out, preferred_element_type=jnp.float32)).astype(jnp.bfloat16)
    normed_mid = rms_norm(residual_mid, norm2_gain)
    gate_proj = jnp.dot(normed_mid, w_gate, preferred_element_type=jnp.float32)
    up_proj = jnp.dot(normed_mid, w_up, preferred_element_type=jnp.float32)
    hidden_mlp = (jax.nn.silu(gate_proj) * up_proj).astype(jnp.bfloat16)
    return (residual_mid.astype(jnp.float32) + jnp.dot(hidden_mlp, w_down, preferred_element_type=jnp.float32)).astype(jnp.bfloat16)
```

```python
import functools
import math
import jax
import jax.numpy as jnp
from jax import lax
from jax.experimental import pallas as pl
from jax.experimental.pallas import tpu as pltpu
from jax.sharding import PartitionSpec as P

HEAD_DIM = 128
ROPE_BASE = 500000.0
NORM_EPS = 1e-5
MESH = pl.DeviceIdType.MESH
F32 = jnp.float32
BF16 = jnp.bfloat16
M_INIT = -3e38
EXP_SCALE = math.log2(math.e) / math.sqrt(HEAD_DIM)
RING = 4
ANY = pl.BlockSpec(memory_space=pl.ANY)
VMEM = pl.BlockSpec(memory_space=pltpu.VMEM)
SMEM = pl.BlockSpec(memory_space=pltpu.SMEM)


class Place:
    def __init__(self):
        self.y = lax.axis_index('tp')
        cp = lax.axis_index('cp')
        self.x = cp // 2
        self.core = cp % 2

    def at(self, dx=0, dy=0, other=False):
        core = 1 - self.core if other else self.core
        return {'tp': (self.y + dy) % RING, 'cp': ((self.x + dx) % RING) * 2 + core}


def remote(src, dst, send_sem, recv_sem, device):
    return pltpu.make_async_remote_copy(src_ref=src, dst_ref=dst, send_sem=send_sem, recv_sem=recv_sem, device_id=device, device_id_type=MESH)


def barrier(devices):
    sem = pltpu.get_barrier_semaphore()
    for device in devices:
        pl.semaphore_signal(sem, inc=1, device_id=device, device_id_type=MESH)
    pl.semaphore_wait(sem, len(devices))


def ring_gather(pos, right, left, block, half, sends, recvs, own=None, partner=None, core=None, psends=None, precvs=None, between=None):
    prev, nxt, far = (pos + 3) % RING, (pos + 1) % RING, (pos + 2) % RING
    mine = block(pos, core) if own is None else own
    to_right = remote(mine, block(pos, core), sends.at[0], recvs.at[0], right)
    to_left = remote(mine, block(pos, core), sends.at[1], recvs.at[1], left)
    to_right.start()
    to_left.start()
    copies = [to_right, to_left]
    given = []

    def give(p, i, source=None):
        if partner is not None:
            copy = remote(block(p, core) if source is None else source, block(p, core), psends.at[i], precvs.at[i], partner)
            copy.start()
            given.append(copy)

    give(pos, 0, mine)
    remote(block(prev, core), block(prev, core), sends.at[0], recvs.at[0], left).wait_recv()
    fwd_right = remote(half(prev, core, 0), half(prev, core, 0), sends.at[2], recvs.at[2], right)
    fwd_right.start()
    give(prev, 1)
    remote(block(nxt, core), block(nxt, core), sends.at[1], recvs.at[1], right).wait_recv()
    fwd_left = remote(half(nxt, core, 1), half(nxt, core, 1), sends.at[3], recvs.at[3], left)
    fwd_left.start()
    give(nxt, 2)
    copies += [fwd_right, fwd_left]
    if between is not None:
        between()
    remote(half(far, core, 0), half(far, core, 0), sends.at[2], recvs.at[2], left).wait_recv()
    remote(half(far, core, 1), half(far, core, 1), sends.at[3], recvs.at[3], right).wait_recv()
    give(far, 3)
    if partner is not None:
        for i, p in enumerate((pos, prev, nxt, far)):
            remote(block(p, 1 - core), block(p, 1 - core), psends.at[i], precvs.at[i], partner).wait_recv()
    return copies + given


def attention_kernel(x_in, len_ref, ck, cv, gain, wq, wk, wv, cos_ref, sin_ref, relq_ref, relk_ref, o_out, xres_out,
                     xbuf, abuf, wqv, wkv, wvv, kbuf, vbuf, vt, qall, knew, vnew, acc, r1l, r1r, r2l, r2r, obuf,
                     lsem, xs, xr, ps, pr, kvs, kvr, qs, qr, rs, rr, os, orr):
    me = Place()
    x, y, core = me.x, me.y, me.core
    width = x_in.shape[1]
    half_w = width // 2
    slots = ck.shape[0]
    rows = qall.shape[0]
    chip_rows = rows // RING
    heads = acc.shape[0]
    head_w = heads * HEAD_DIM
    col = [(dy, dk) for dy in (0, 1, 3, 2) for dk in (0, 1)]
    partner = me.at(other=True)
    up, down = me.at(dy=1), me.at(dy=-1 + RING)
    right, left = me.at(dx=1), me.at(dx=-1 + RING)

    local = [
        pltpu.make_async_copy(x_in, xbuf.at[y, core], lsem.at[0]),
        pltpu.make_async_copy(wq.at[:, pl.ds(pl.multiple_of(core * head_w, head_w), head_w)], wqv, lsem.at[1]),
        pltpu.make_async_copy(wk.at[:, pl.ds(pl.multiple_of(core * HEAD_DIM, HEAD_DIM), HEAD_DIM)], wkv, lsem.at[2]),
        pltpu.make_async_copy(wv.at[:, pl.ds(pl.multiple_of(core * HEAD_DIM, HEAD_DIM), HEAD_DIM)], wvv, lsem.at[3]),
    ]
    for copy in local:
        copy.start()

    barrier([me.at(dy=dy, other=bool(dk)) for dy, dk in col[1:]] + [right, left])

    kv_copies = []

    def send_kv():
        for s, (dy, dk) in enumerate(col):
            head = 2 * ((y + dy) % RING) + (1 - core if dk else core)
            lanes = pl.ds(pl.multiple_of(head * HEAD_DIM, HEAD_DIM), HEAD_DIM)
            for i, (src, dst) in enumerate(((ck, kbuf), (cv, vbuf))):
                if s == 0:
                    copy = pltpu.make_async_copy(src.at[:, lanes], dst.at[s], kvr.at[s, i])
                else:
                    copy = remote(src.at[:, lanes], dst.at[s], kvs.at[s, i], kvr.at[s, i], me.at(dy=dy, other=bool(dk)))
                    kv_copies.append(copy)
                copy.start()

    x_copies = ring_gather(
        y, up, down, lambda p, c: xbuf.at[p, c], lambda p, c, i: xbuf.at[p, c, :, pl.ds(i * half_w, half_w)],
        xs, xr, own=x_in, partner=partner, core=core, psends=ps, precvs=pr, between=send_kv)
    local[0].wait()

    def norm_block(i, carry):
        values = xbuf[i].reshape(2 * xbuf.shape[2], width).astype(F32)
        inv = lax.rsqrt(jnp.mean(values * values, axis=-1, keepdims=True) + NORM_EPS)
        abuf[i] = (values * inv * gain[...].astype(F32)).astype(BF16)
        return carry

    lax.fori_loop(0, RING, norm_block, 0)
    xres_out[...] = xbuf[y, :, :, pl.ds(pl.multiple_of(core * half_w, half_w), half_w)].reshape(xres_out.shape)

    for copy in local[1:]:
        copy.wait()
    normed = abuf[...].reshape(chip_rows, width)
    cos, sin = cos_ref[...], sin_ref[...]

    def rotate(v):
        return (v * cos + pltpu.roll(v, HEAD_DIM // 2, 1) * sin).astype(BF16)

    my_rows = pl.ds(pl.multiple_of(x * chip_rows, chip_rows), chip_rows)
    q = jnp.dot(normed, wqv[...], preferred_element_type=F32)
    for h in range(heads):
        qall[my_rows, h * HEAD_DIM:(h + 1) * HEAD_DIM] = rotate(q[:, h * HEAD_DIM:(h + 1) * HEAD_DIM])
    knew[...] = rotate(jnp.dot(normed, wkv[...], preferred_element_type=F32))
    vnew[...] = jnp.dot(normed, wvv[...], preferred_element_type=F32).astype(BF16)

    def q_rows(p):
        return pl.ds(pl.multiple_of(p * chip_rows, chip_rows), chip_rows)

    q_copies = ring_gather(
        x, right, left, lambda p, c: qall.at[q_rows(p), :],
        lambda p, c, i: qall.at[q_rows(p), pl.ds(i * head_w // 2, head_w // 2)], qs, qr)

    tile = 256
    tiles = rows // tile

    def softmax_step(keys, vt_value, h, j, mask_of, first):
        lanes = pl.ds(j * tile, tile)
        queries = qall[j * tile:(j + 1) * tile, pl.ds(pl.multiple_of(h * HEAD_DIM, HEAD_DIM), HEAD_DIM)]
        s = lax.dot_general(keys, queries, (((1,), (1,)), ((), ())), preferred_element_type=F32)
        s = jnp.where(mask_of(j, s.shape), s, -jnp.inf)
        top = jnp.max(s, axis=0, keepdims=True)
        if first:
            m_new = jnp.maximum(top, M_INIT)
        else:
            m_old = acc[h, HEAD_DIM:HEAD_DIM + 1, lanes]
            l_old = acc[h, HEAD_DIM + 1:HEAD_DIM + 2, lanes]
            m_new = jnp.maximum(top, m_old)
        e = jnp.exp2(s * EXP_SCALE - m_new * EXP_SCALE)
        l_new = jnp.sum(e, axis=0, keepdims=True)
        o = jnp.dot(vt_value, e.astype(BF16), preferred_element_type=F32)
        if not first:
            alpha = jnp.exp2((m_old - m_new) * EXP_SCALE)
            l_new = l_new + l_old * alpha
            o = o + acc[h, 0:HEAD_DIM, lanes] * alpha
        acc[h, 0:HEAD_DIM, lanes] = o
        acc[h, HEAD_DIM:HEAD_DIM + 1, lanes] = m_new
        acc[h, HEAD_DIM + 1:HEAD_DIM + 2, lanes] = l_new

    vnew_t = vnew[...].astype(F32).T.astype(BF16)
    relk = relk_ref[...]

    def new_head(h, carry):
        for j in range(tiles):
            softmax_step(knew[...], vnew_t, h, j, lambda j, shape: jnp.broadcast_to(relk, shape) <= jnp.broadcast_to(relq_ref[:, j * tile:(j + 1) * tile], shape), True)
        return carry

    lax.fori_loop(0, heads, new_head, 0)
    cache_len = len_ref[0]

    def source(s, carry):
        u, dk = s // 2, s % 2
        dy = u + (u // 2) * (1 - 2 * (u % 2))
        src_core = core + dk * (1 - 2 * core)
        src_y = (y - dy + RING) % RING
        base = ((2 * x + src_core) * RING + src_y) * slots
        for i, (src, dst) in enumerate(((ck, kbuf), (cv, vbuf))):
            pltpu.make_async_copy(src.at[:, pl.ds(0, HEAD_DIM)], dst.at[s], kvr.at[s, i]).wait()
        vt[...] = vbuf[s].astype(F32).T.astype(BF16)
        seen = cache_len - base

        def head(h, c):
            for j in range(tiles):
                softmax_step(kbuf[s], vt[...], h, j, lambda j, shape: lax.broadcasted_iota(jnp.int32, shape, 0) < seen, False)
            return c

        return lax.fori_loop(0, heads, head, carry)

    lax.fori_loop(0, len(col), source, 0)

    hh = heads // 2
    far, nxt, prev = (x + 2) % RING, (x + 1) % RING, (x + 3) % RING
    p1 = [remote(acc.at[pl.ds(0, hh), :, q_rows(far)], r1l, rs.at[0], rr.at[0], right),
          remote(acc.at[pl.ds(hh, hh), :, q_rows(far)], r1r, rs.at[1], rr.at[1], left)]
    for copy in p1:
        copy.start()

    def merge(a, b):
        ma, mb = a[:, HEAD_DIM:HEAD_DIM + 1, :], b[:, HEAD_DIM:HEAD_DIM + 1, :]
        m = jnp.maximum(ma, mb)
        wa, wb = jnp.exp2((ma - m) * EXP_SCALE), jnp.exp2((mb - m) * EXP_SCALE)
        o = a[:, 0:HEAD_DIM, :] * wa + b[:, 0:HEAD_DIM, :] * wb
        l = a[:, HEAD_DIM + 1:HEAD_DIM + 2, :] * wa + b[:, HEAD_DIM + 1:HEAD_DIM + 2, :] * wb
        return o, m, l

    def merge_into(lo, p, other):
        o, m, l = merge(acc[lo:lo + hh, :, q_rows(p)], other[...])
        acc[lo:lo + hh, 0:HEAD_DIM, q_rows(p)] = o
        acc[lo:lo + hh, HEAD_DIM:HEAD_DIM + 1, q_rows(p)] = m
        acc[lo:lo + hh, HEAD_DIM + 1:HEAD_DIM + 2, q_rows(p)] = l

    p1[0].wait_recv()
    merge_into(0, nxt, r1l)
    p1[1].wait_recv()
    merge_into(hh, prev, r1r)
    p2 = [remote(acc.at[:, :, q_rows(nxt)], r2l, rs.at[2], rr.at[2], right),
          remote(acc.at[:, :, q_rows(prev)], r2r, rs.at[3], rr.at[3], left)]
    for copy in p2:
        copy.start()
    for copy in p2:
        copy.wait_recv()
    for h in range(heads):
        a, b, d = acc[h:h + 1, :, q_rows(x)], r2l[h:h + 1], r2r[h:h + 1]
        o, m, l = merge(a, b)
        md = d[:, HEAD_DIM:HEAD_DIM + 1, :]
        top = jnp.maximum(m, md)
        w, wd = jnp.exp2((m - top) * EXP_SCALE), jnp.exp2((md - top) * EXP_SCALE)
        o = o * w + d[:, 0:HEAD_DIM, :] * wd
        l = l * w + d[:, HEAD_DIM + 1:HEAD_DIM + 2, :] * wd
        obuf[core, :, h * HEAD_DIM:(h + 1) * HEAD_DIM] = (o / l)[0].T.astype(BF16)
    swap = remote(obuf.at[core], obuf.at[core], os.at[0], orr.at[0], partner)
    swap.start()
    remote(obuf.at[1 - core], obuf.at[1 - core], os.at[0], orr.at[0], partner).wait_recv()
    o_out[:, 0:head_w] = obuf[0]
    o_out[:, head_w:2 * head_w] = obuf[1]
    for copy in x_copies + kv_copies + q_copies + p1 + p2 + [swap]:
        copy.wait_send()


def mlp_kernel(o_in, xres, gain, wo, wg, wu, wd, out,
               wov, wgv, wuv, wdv, part, r1l, r1r, r2l, r2r, hbuf, hres, ubuf, fin, fbuf,
               wosem, wgsem, wusem, wdsem, s1, q1, s2, q2, hs, hr, ps, pr, us, ur, fs, fr):
    me = Place()
    y, core = me.y, me.core
    nc, _, _, cw = part.shape
    half_w = nc * cw
    width = 2 * half_w
    rows = o_in.shape[0]
    block_rows = rows // RING
    nu, _, uw = wgv.shape
    half_f = nu * uw
    nd = wdv.shape[0]
    partner = me.at(other=True)
    up, down = me.at(dy=1), me.at(dy=-1 + RING)
    far, nxt, prev = (y + 2) % RING, (y + 1) % RING, (y + 3) % RING
    col0 = core * half_w

    def lanes(start, size):
        return pl.ds(pl.multiple_of(start, 128), size)

    def wo_copy(j):
        return pltpu.make_async_copy(wo.at[:, lanes(col0 + j * cw, cw)], wov.at[j], wosem.at[j])

    def wd_copy(j):
        return pltpu.make_async_copy(wd.at[:, lanes(col0 + j * cw, cw)], wdv.at[j % nd], wdsem.at[j % nd])

    def wg_copy(j):
        return pltpu.make_async_copy(wg.at[:, lanes(core * half_f + j * uw, uw)], wgv.at[j], wgsem.at[j])

    def wu_copy(j):
        return pltpu.make_async_copy(wu.at[:, lanes(core * half_f + j * uw, uw)], wuv.at[j], wusem.at[j])

    for j in range(nc):
        wo_copy(j).start()
    for j in range(nu):
        wg_copy(j).start()
        wu_copy(j).start()
    for j in range(nd):
        wd_copy(j).start()

    barrier([up, down, partner])

    hc = cw // 2

    def first_sends(j):
        return (remote(part.at[j, far, :, pl.ds(0, hc)], r1l.at[j], s1.at[0, j], q1.at[0, j], up),
                remote(part.at[j, far, :, pl.ds(hc, hc)], r1r.at[j], s1.at[1, j], q1.at[1, j], down))

    def second_sends(j):
        return (remote(part.at[j, nxt], r2l.at[j], s2.at[0, j], q2.at[0, j], up),
                remote(part.at[j, prev], r2r.at[j], s2.at[1, j], q2.at[1, j], down))

    def relay(j, carry):
        a, b = first_sends(j)
        a.wait_recv()
        part[j, nxt, :, 0:hc] = part[j, nxt, :, 0:hc] + r1l[j]
        b.wait_recv()
        part[j, prev, :, hc:cw] = part[j, prev, :, hc:cw] + r1r[j]
        for copy in second_sends(j):
            copy.start()
        return carry

    def total(j):
        for copy in second_sends(j):
            copy.wait_recv()
        return part[j, y] + r2l[j] + r2r[j]

    def drain(j, carry):
        for copy in first_sends(j) + second_sends(j):
            copy.wait_send()
        return carry

    attended = o_in[...]

    def out_chunk(j, carry):
        wo_copy(j).wait()
        part[j] = jnp.dot(attended, wov[j], preferred_element_type=F32).reshape(RING, block_rows, cw)
        for copy in first_sends(j):
            copy.start()
        return carry

    lax.fori_loop(0, nc, out_chunk, 0)
    lax.fori_loop(0, nc, relay, 0)

    def mid_chunk(j, carry):
        c = lanes(j * cw, cw)
        mid = (xres[:, c].astype(F32) + total(j)).astype(BF16)
        hres[:, c] = mid
        hbuf[core, y, :, c] = mid
        return carry

    lax.fori_loop(0, nc, mid_chunk, 0)
    h_copies = ring_gather(
        y, up, down, lambda p, c: hbuf.at[c, p], lambda p, c, i: hbuf.at[c, p, :, pl.ds(i * (half_w // 2), half_w // 2)],
        hs, hr, partner=partner, core=core, psends=ps, precvs=pr)
    for copy in h_copies:
        copy.wait_send()
    lax.fori_loop(0, nc, drain, 0)

    def norm_block(i, carry):
        v0, v1 = hbuf[0, i].astype(F32), hbuf[1, i].astype(F32)
        mean = (jnp.sum(v0 * v0, axis=-1, keepdims=True) + jnp.sum(v1 * v1, axis=-1, keepdims=True)) / width
        inv = lax.rsqrt(mean + NORM_EPS)
        hbuf[0, i] = (v0 * inv * gain[0:1, :].astype(F32)).astype(BF16)
        hbuf[1, i] = (v1 * inv * gain[1:2, :].astype(F32)).astype(BF16)
        return carry

    lax.fori_loop(0, RING, norm_block, 0)
    b0, b1 = hbuf[0].reshape(rows, half_w), hbuf[1].reshape(rows, half_w)

    def u_copy(j, c):
        at = ubuf.at[:, lanes(c * half_f + j * uw, uw)]
        return remote(at, at, us.at[j], ur.at[j], partner)

    def up_chunk(j, carry):
        wg_copy(j).wait()
        wu_copy(j).wait()
        gate = jnp.dot(b0, wgv[j, 0:half_w, :], preferred_element_type=F32) + jnp.dot(b1, wgv[j, half_w:width, :], preferred_element_type=F32)
        upper = jnp.dot(b0, wuv[j, 0:half_w, :], preferred_element_type=F32) + jnp.dot(b1, wuv[j, half_w:width, :], preferred_element_type=F32)
        ubuf[:, lanes(core * half_f + j * uw, uw)] = (jax.nn.silu(gate) * upper).astype(BF16)
        u_copy(j, core).start()
        return carry

    lax.fori_loop(0, nu, up_chunk, 0)
    for j in range(nu):
        u_copy(j, 1 - core).wait_recv()

    for j in range(nc):
        wd_copy(j).wait()
        part[j] = jnp.dot(ubuf[...], wdv[j % nd], preferred_element_type=F32).reshape(RING, block_rows, cw)
        if j + nd < nc:
            wd_copy(j + nd).start()
        for copy in first_sends(j):
            copy.start()
    lax.fori_loop(0, nc, relay, 0)

    def last_chunk(j, carry):
        c = lanes(j * cw, cw)
        fin[:, :, c] = (hres[:, c].astype(F32) + total(j)).astype(BF16).reshape(2, block_rows // 2, cw)
        return carry

    lax.fori_loop(0, nc, last_chunk, 0)
    swap = remote(fin.at[1 - core], fbuf.at[core], fs.at[0], fr.at[0], partner)
    swap.start()
    own = fin[core]
    out[:, lanes(col0, half_w)] = own
    remote(fin.at[core], fbuf.at[1 - core], fs.at[0], fr.at[0], partner).wait_recv()
    out[:, lanes((1 - core) * half_w, half_w)] = fbuf[1 - core]
    for j in range(nu):
        u_copy(j, core).wait_send()
    lax.fori_loop(0, nc, drain, 0)
    swap.wait_send()


def dma(*shape):
    return pltpu.SemaphoreType.DMA(shape)


def relative_positions(chips, shards, row_count):
    r = jnp.arange(row_count, dtype=jnp.int32)
    per_chip = 2 * RING * 16
    x = chips + r // per_chip
    y, core, w = (r % per_chip) // 32, (r % 32) // 16, r % 16
    k = (2 * x + core) * RING + y
    run = jnp.where(w < 8, k, 2 * shards - 1 - k)
    return run * 8 + w % 8


def solution(mesh):
    token_spec = P(('dp', 'cp', 'tp'), None)
    column_spec = P(None, 'tp')
    row_spec = P('tp', None)
    shards = mesh.shape['tp'] * mesh.shape['cp']

    def device_layer(hidden_loc, pos_loc, cache_len, cache_k, cache_v, norm1_gain, w_query, w_key, w_value, w_out, norm2_gain, w_gate, w_up, w_down):
        shard_rows, width = hidden_loc.shape
        half_w = width // 2
        chip_rows = 2 * RING * shard_rows
        rows = RING * chip_rows
        slots = cache_k.shape[0]
        head_w = w_query.shape[1] // 2
        heads = head_w // HEAD_DIM
        x = lax.axis_index('cp') // 2
        half = HEAD_DIM // 2
        relk = relative_positions(x, shards, chip_rows)
        relq = relative_positions(0, shards, rows)
        inv_freq = 1.0 / (ROPE_BASE ** (jnp.arange(half, dtype=F32) * (2.0 / HEAD_DIM)))
        angles = (cache_len[0] + relk).astype(F32)[:, None] * inv_freq[None, :]
        cos, sin = jnp.cos(angles), jnp.sin(angles)
        cos = jnp.concatenate([cos, cos], axis=1)
        sin = jnp.concatenate([-sin, sin], axis=1)
        block = (heads, HEAD_DIM + 8, chip_rows)
        part_block = (heads // 2,) + block[1:]
        attended, xres = pl.pallas_call(
            attention_kernel,
            out_shape=(jax.ShapeDtypeStruct((chip_rows, 2 * head_w), BF16), jax.ShapeDtypeStruct((2 * shard_rows, half_w), BF16)),
            in_specs=[ANY, SMEM, ANY, ANY, VMEM, ANY, ANY, ANY, VMEM, VMEM, VMEM, VMEM],
            out_specs=(VMEM, VMEM),
            scratch_shapes=[
                pltpu.VMEM((RING, 2, shard_rows, width), BF16),
                pltpu.VMEM((RING, 2 * shard_rows, width), BF16),
                pltpu.VMEM((width, head_w), BF16),
                pltpu.VMEM((width, HEAD_DIM), BF16),
                pltpu.VMEM((width, HEAD_DIM), BF16),
                pltpu.VMEM((2 * RING, slots, HEAD_DIM), BF16),
                pltpu.VMEM((2 * RING, slots, HEAD_DIM), BF16),
                pltpu.VMEM((HEAD_DIM, slots), BF16),
                pltpu.VMEM((rows, head_w), BF16),
                pltpu.VMEM((chip_rows, HEAD_DIM), BF16),
                pltpu.VMEM((chip_rows, HEAD_DIM), BF16),
                pltpu.VMEM((heads, HEAD_DIM + 8, rows), F32),
                pltpu.VMEM(part_block, F32),
                pltpu.VMEM(part_block, F32),
                pltpu.VMEM(block, F32),
                pltpu.VMEM(block, F32),
                pltpu.VMEM((2, chip_rows, head_w), BF16),
                dma(4), dma(4), dma(4), dma(4), dma(4), dma(2 * RING, 2), dma(2 * RING, 2),
                dma(4), dma(4), dma(4), dma(4), dma(1), dma(1),
            ],
            compiler_params=pltpu.CompilerParams(collective_id=0, has_side_effects=True, vmem_limit_bytes=48 * 2**20),
            name='attention',
        )(hidden_loc, cache_len, cache_k, cache_v, norm1_gain.reshape(1, width), w_query, w_key, w_value, cos, sin, relq.reshape(1, rows), relk.reshape(chip_rows, 1))

        cw = 512 if half_w % 512 == 0 and half_w > 512 else 256
        nc = half_w // cw
        half_f = w_gate.shape[1] // 2
        uw = 256
        nu = half_f // uw
        nd = max(1, nc - 1)
        br = 2 * shard_rows
        return pl.pallas_call(
            mlp_kernel,
            out_shape=jax.ShapeDtypeStruct((shard_rows, width), BF16),
            in_specs=[VMEM, VMEM, VMEM, ANY, ANY, ANY, ANY],
            out_specs=VMEM,
            scratch_shapes=[
                pltpu.VMEM((nc, 2 * head_w, cw), BF16),
                pltpu.VMEM((nu, width, uw), BF16),
                pltpu.VMEM((nu, width, uw), BF16),
                pltpu.VMEM((nd, 2 * half_f, cw), BF16),
                pltpu.VMEM((nc, RING, br, cw), F32),
                pltpu.VMEM((nc, br, cw // 2), F32),
                pltpu.VMEM((nc, br, cw // 2), F32),
                pltpu.VMEM((nc, br, cw), F32),
                pltpu.VMEM((nc, br, cw), F32),
                pltpu.VMEM((2, RING, br, half_w), BF16),
                pltpu.VMEM((br, half_w), BF16),
                pltpu.VMEM((chip_rows, 2 * half_f), BF16),
                pltpu.VMEM((2, shard_rows, half_w), BF16),
                pltpu.VMEM((2, shard_rows, half_w), BF16),
                dma(nc), dma(nu), dma(nu), dma(nd), dma(2, nc), dma(2, nc), dma(2, nc), dma(2, nc),
                dma(4), dma(4), dma(4), dma(4), dma(nu), dma(nu), dma(1), dma(1),
            ],
            compiler_params=pltpu.CompilerParams(collective_id=1, has_side_effects=True, vmem_limit_bytes=67043328),
            name='mlp',
        )(attended, xres, norm2_gain.reshape(2, half_w), w_out, w_gate, w_up, w_down)

    return jax.shard_map(device_layer, mesh=mesh, in_specs=(token_spec, P(('dp', 'cp', 'tp')), P('dp'), token_spec, token_spec, P(), column_spec, column_spec, column_spec, row_spec, P(), column_spec, column_spec, row_spec), out_specs=token_spec, check_vma=False)
```

```python
import functools
import math
import jax
import jax.numpy as jnp
from jax import lax
from jax.experimental import pallas as pl
from jax.experimental.pallas import tpu as pltpu
from jax.sharding import PartitionSpec as P

HEAD_DIM = 128
ROPE_BASE = 500000.0
NORM_EPS = 1e-5
MESH = pl.DeviceIdType.MESH
F32 = jnp.float32
BF16 = jnp.bfloat16
M_INIT = -1e38
MASKED = -3e38
EXP_SCALE = math.log2(math.e) / math.sqrt(HEAD_DIM)
RING = 4
STEP = 512
ANY = pl.BlockSpec(memory_space=pl.ANY)
VMEM = pl.BlockSpec(memory_space=pltpu.VMEM)
SMEM = pl.BlockSpec(memory_space=pltpu.SMEM)


class Place:
    def __init__(self):
        self.y = lax.axis_index('tp')
        cp = lax.axis_index('cp')
        self.x = cp // 2
        self.core = cp % 2
        self.vx = self.x + self.core * (self.y - self.x)
        self.vy = self.y + self.core * (self.x - self.y)

    def at(self, dx=0, dy=0, core=None):
        return {'tp': (self.y + dy) % RING, 'cp': ((self.x + dx) % RING) * 2 + (self.core if core is None else core)}

    def mirrored(self, core):
        return {'tp': self.x, 'cp': self.y * 2 + core}


def remote(src, dst, send_sem, recv_sem, device):
    return pltpu.make_async_remote_copy(src_ref=src, dst_ref=dst, send_sem=send_sem, recv_sem=recv_sem, device_id=device, device_id_type=MESH)


def barrier(devices):
    sem = pltpu.get_barrier_semaphore()
    for device in devices:
        pl.semaphore_signal(sem, inc=1, device_id=device, device_id_type=MESH)
    pl.semaphore_wait(sem, len(devices))


def ring_gather(pos, right, left, block, half, sends, recvs, own=None, partner=None, core=None, psends=None, precvs=None, between=None):
    prev, nxt, far = (pos + 3) % RING, (pos + 1) % RING, (pos + 2) % RING
    mine = block(pos, core) if own is None else own
    to_right = remote(mine, block(pos, core), sends.at[0], recvs.at[0], right)
    to_left = remote(mine, block(pos, core), sends.at[1], recvs.at[1], left)
    to_right.start()
    to_left.start()
    copies = [to_right, to_left]
    given = []

    def give(p, i, source=None):
        if partner is not None:
            copy = remote(block(p, core) if source is None else source, block(p, core), psends.at[i], precvs.at[i], partner)
            copy.start()
            given.append(copy)

    give(pos, 0, mine)
    remote(block(prev, core), block(prev, core), sends.at[0], recvs.at[0], left).wait_recv()
    fwd_right = remote(half(prev, core, 0), half(prev, core, 0), sends.at[2], recvs.at[2], right)
    fwd_right.start()
    give(prev, 1)
    remote(block(nxt, core), block(nxt, core), sends.at[1], recvs.at[1], right).wait_recv()
    fwd_left = remote(half(nxt, core, 1), half(nxt, core, 1), sends.at[3], recvs.at[3], left)
    fwd_left.start()
    give(nxt, 2)
    copies += [fwd_right, fwd_left]
    if between is not None:
        between()
    remote(half(far, core, 0), half(far, core, 0), sends.at[2], recvs.at[2], left).wait_recv()
    remote(half(far, core, 1), half(far, core, 1), sends.at[3], recvs.at[3], right).wait_recv()
    give(far, 3)
    if partner is not None:
        for i, p in enumerate((pos, prev, nxt, far)):
            remote(block(p, 1 - core), block(p, 1 - core), psends.at[i], precvs.at[i], partner).wait_recv()
    return copies + given


def attention_kernel(x_in, len_ref, ck, cv, gain, wq, wk, wv, cos_ref, sin_ref, relq_ref, relk_ref, o_out, xres_out,
                     xbuf, abuf, wqv, wkv, wvv, kbuf, vbuf, rk, rv, kaug, vt, qkv, qall, qaug, sa, sb, acc, r1l, r1r, r2l, r2r, otmp, obuf,
                     lsem, xs, xr, ps, pr, kvs, kvr, relay_r, ts, tr, qs, qr, rs, rr, os, orr):
    me = Place()
    x, y, core, vx, vy = me.x, me.y, me.core, me.vx, me.vy
    width = x_in.shape[1]
    half_w = width // 2
    slots = ck.shape[0]
    rows = qall.shape[0]
    chip_rows = rows // RING
    heads = acc.shape[0]
    head_w = heads * HEAD_DIM
    partner = me.at(core=1 - core)
    up, down = me.at(dy=1), me.at(dy=RING - 1)
    right, left = me.at(dx=1 - core, dy=core), me.at(dx=(1 - core) * (RING - 1), dy=core * (RING - 1))
    ahead, behind = me.at(dx=core, dy=1 - core), me.at(dx=core * (RING - 1), dy=(1 - core) * (RING - 1))
    moving = jnp.logical_and(core == 1, x != y)

    local = [
        pltpu.make_async_copy(x_in, xbuf.at[y, core], lsem.at[0]),
        pltpu.make_async_copy(wq.at[:, pl.ds(pl.multiple_of(core * head_w, head_w), head_w)], wqv, lsem.at[1]),
        pltpu.make_async_copy(wk.at[:, pl.ds(pl.multiple_of(core * HEAD_DIM, HEAD_DIM), HEAD_DIM)], wkv, lsem.at[2]),
        pltpu.make_async_copy(wv.at[:, pl.ds(pl.multiple_of(core * HEAD_DIM, HEAD_DIM), HEAD_DIM)], wvv, lsem.at[3]),
    ]
    for copy in local:
        copy.start()

    peers = [partner, me.mirrored(0), me.mirrored(1)]
    peers += [me.at(dy=d, core=c) for d in range(1, RING) for c in range(2)] + [me.at(dx=d, core=c) for d in range(1, RING) for c in range(2)]
    barrier(peers)

    def kv_lanes(head):
        return pl.ds(pl.multiple_of(head * HEAD_DIM, HEAD_DIM), HEAD_DIM)

    def target(role, d):
        return me.at(dx=d if role else 0, dy=0 if role else d, core=role)

    def target_lanes(role, d):
        return kv_lanes(2 * (((x if role else y) + d) % RING) + role)

    kv_copies = []

    def kv_send(src, dst, recv, device):
        copy = remote(src, dst, kvs.at[len(kv_copies)], recv, device)
        copy.start()
        kv_copies.append(copy)

    def send_near():
        other_vy = x + y - vy
        for i, (src, dst) in enumerate(((ck, kbuf), (cv, vbuf))):
            pltpu.make_async_copy(src.at[:, kv_lanes(2 * vy + core)], dst.at[core], kvr.at[core, i]).start()
            kv_send(src.at[:, kv_lanes(2 * other_vy + 1 - core)], dst.at[core], kvr.at[core, i], partner)
        for role in range(2):
            kv_send(ck.at[:, target_lanes(role, 2)], rk.at[core], relay_r.at[0, core], target(role, 1))
            kv_send(cv.at[:, target_lanes(role, 2)], rv.at[core], relay_r.at[1, core], target(role, RING - 1))

    def send_far():
        for i, (src, dst) in enumerate(((ck, kbuf), (cv, vbuf))):
            for role in range(2):
                for d, slot in ((1, 2), (3, 4)):
                    kv_send(src.at[:, target_lanes(role, d)], dst.at[slot + core], kvr.at[slot + core, i], target(role, d))
        for c in range(2):
            remote(rk.at[c], rk.at[c], kvs.at[0], relay_r.at[0, c], behind).wait_recv()
            kv_send(rk.at[c], kbuf.at[6 + c], kvr.at[6 + c, 0], ahead)
            remote(rv.at[c], rv.at[c], kvs.at[0], relay_r.at[1, c], ahead).wait_recv()
            kv_send(rv.at[c], vbuf.at[6 + c], kvr.at[6 + c, 1], behind)

    x_copies = ring_gather(
        y, up, down, lambda p, c: xbuf.at[p, c], lambda p, c, i: xbuf.at[p, c, :, pl.ds(i * half_w, half_w)],
        xs, xr, own=x_in, partner=partner, core=core, psends=ps, precvs=pr, between=send_near)
    local[0].wait()

    def norm_block(i, carry):
        values = xbuf[i].reshape(2 * xbuf.shape[2], width).astype(F32)
        inv = lax.rsqrt(jnp.mean(values * values, axis=-1, keepdims=True) + NORM_EPS)
        abuf[i] = (values * inv * gain[...].astype(F32)).astype(BF16)
        return carry

    lax.fori_loop(0, RING, norm_block, 0)
    xres_out[...] = xbuf[y, :, :, pl.ds(pl.multiple_of(core * half_w, half_w), half_w)].reshape(xres_out.shape)

    for copy in local[1:]:
        copy.wait()
    normed = abuf[...].reshape(chip_rows, width)
    cos, sin = cos_ref[...], sin_ref[...]

    def rotate(v):
        return (v * cos + pltpu.roll(v, HEAD_DIM // 2, 1) * sin).astype(BF16)

    q = jnp.dot(normed, wqv[...], preferred_element_type=F32)
    for h in range(heads):
        qkv[:, h * HEAD_DIM:(h + 1) * HEAD_DIM] = rotate(q[:, h * HEAD_DIM:(h + 1) * HEAD_DIM])
    qkv[:, head_w:head_w + HEAD_DIM] = rotate(jnp.dot(normed, wkv[...], preferred_element_type=F32))
    qkv[:, head_w + HEAD_DIM:] = jnp.dot(normed, wvv[...], preferred_element_type=F32).astype(BF16)

    def q_rows(p):
        return pl.ds(pl.multiple_of(p * chip_rows, chip_rows), chip_rows)

    across_in = remote(qkv, qall.at[q_rows(vx)], ts.at[0], tr.at[0], me.mirrored(core))
    mirror_send = remote(qkv, qall.at[q_rows(x)], ts.at[0], tr.at[0], me.mirrored(core))

    @pl.when(moving)
    def _():
        mirror_send.start()
        across_in.wait_recv()

    @pl.when(jnp.logical_not(moving))
    def _():
        qall[q_rows(vx), :] = qkv[...]

    q_copies = ring_gather(
        vx, right, left, lambda p, c: qall.at[q_rows(p), pl.ds(0, head_w)],
        lambda p, c, i: qall.at[q_rows(p), pl.ds(i * (head_w // 2), head_w // 2)], qs, qr, between=send_far)

    first_lane = jnp.where(lax.broadcasted_iota(jnp.int32, (rows, HEAD_DIM), 1) == 0, 1.0, 0.0).astype(BF16)
    for h in range(heads):
        qaug[h, :, 0:HEAD_DIM] = qall[:, h * HEAD_DIM:(h + 1) * HEAD_DIM]
        qaug[h, :, HEAD_DIM:] = first_lane

    tile = 256
    tiles = rows // tile
    contract_last = (((1,), (1,)), ((), ()))

    def finish(s_ref, e_top, vt_ref, h, j, first, depth):
        lanes = pl.ds(j * tile, tile)
        if first:
            m_new = jnp.maximum(e_top, M_INIT)
        else:
            m_old = acc[h, HEAD_DIM:HEAD_DIM + 1, lanes]
            l_old = acc[h, HEAD_DIM + 1:HEAD_DIM + 2, lanes]
            m_new = jnp.maximum(e_top, m_old)
        m_scaled = m_new * EXP_SCALE
        part_l, o = None, None
        step = min(STEP, depth)
        for k in range(0, depth, step):
            e = jnp.exp2(s_ref[k:k + step, :] * EXP_SCALE - m_scaled)
            total_e = jnp.sum(e.reshape(step // 8, 8, tile), axis=0)
            part_l = total_e if part_l is None else part_l + total_e
            term = jnp.dot(vt_ref[:, k:k + step], e.astype(BF16), preferred_element_type=F32)
            o = term if o is None else o + term
        l_new = jnp.sum(part_l, axis=0, keepdims=True)
        if not first:
            alpha = jnp.exp2((m_old - m_new) * EXP_SCALE)
            l_new = l_new + l_old * alpha
            o = o + acc[h, 0:HEAD_DIM, lanes] * alpha
        acc[h, 0:HEAD_DIM, lanes] = o
        acc[h, HEAD_DIM:HEAD_DIM + 1, lanes] = m_new
        acc[h, HEAD_DIM + 1:HEAD_DIM + 2, lanes] = l_new

    my_rows = q_rows(vx)
    vnew_t = qall[my_rows, head_w + HEAD_DIM:].T
    knew = qall[my_rows, head_w:head_w + HEAD_DIM]
    relk = relk_ref[...]

    def new_head(h, carry):
        for j in range(tiles):
            s = lax.dot_general(knew, qaug[h, j * tile:(j + 1) * tile, 0:HEAD_DIM], contract_last, preferred_element_type=F32)
            causal = jnp.broadcast_to(relk, s.shape) <= jnp.broadcast_to(relq_ref[:, j * tile:(j + 1) * tile], s.shape)
            s = jnp.where(causal, s, -jnp.inf)
            finish(s, jnp.max(s, axis=0, keepdims=True), vnew_t, h, j, True, chip_rows)
        return carry

    lax.fori_loop(0, heads, new_head, 0)
    cache_len = len_ref[0]
    slot_ids = lax.broadcasted_iota(jnp.int32, (slots, HEAD_DIM), 0)

    def scores(h, j, dst):
        s = lax.dot_general(kaug[...], qaug[h, j * tile:(j + 1) * tile, :], contract_last, preferred_element_type=F32)
        dst[...] = s
        return jnp.max(s, axis=0, keepdims=True)

    def source(s, carry):
        u, src_core = s // 2, s % 2
        d = u + (u // 2) * (1 - 2 * (u % 2))
        src_x = (x - core * d + RING) % RING
        src_y = (y - (1 - core) * d + RING) % RING
        base = ((2 * src_x + src_core) * RING + src_y) * slots
        for i, (src, dst) in enumerate(((ck, kbuf), (cv, vbuf))):
            pltpu.make_async_copy(src.at[:, pl.ds(0, HEAD_DIM)], dst.at[s], kvr.at[s, i]).wait()
        vt[...] = vbuf[s].T
        seen = slot_ids < cache_len - base
        kaug[:, 0:HEAD_DIM] = jnp.where(seen, kbuf[s].astype(F32), 0.0).astype(BF16)
        kaug[:, HEAD_DIM:] = jnp.where(seen, 0.0, MASKED).astype(BF16)

        def head(h, top_a):
            top_b = scores(h, 1, sb)
            finish(sa, top_a, vt, h, 0, False, slots)
            top_a = scores(jnp.minimum(h + 1, heads - 1), 0, sa)
            finish(sb, top_b, vt, h, 1, False, slots)
            return top_a

        lax.fori_loop(0, heads, head, scores(0, 0, sa))
        return carry

    lax.fori_loop(0, 2 * RING, source, 0)

    hh = heads // 2
    far, nxt, prev = (vx + 2) % RING, (vx + 1) % RING, (vx + 3) % RING
    p1 = [remote(acc.at[pl.ds(0, hh), :, q_rows(far)], r1l, rs.at[0], rr.at[0], right),
          remote(acc.at[pl.ds(hh, hh), :, q_rows(far)], r1r, rs.at[1], rr.at[1], left)]
    for copy in p1:
        copy.start()

    def merge(a, b):
        ma, mb = a[:, HEAD_DIM:HEAD_DIM + 1, :], b[:, HEAD_DIM:HEAD_DIM + 1, :]
        m = jnp.maximum(ma, mb)
        wa, wb = jnp.exp2((ma - m) * EXP_SCALE), jnp.exp2((mb - m) * EXP_SCALE)
        o = a[:, 0:HEAD_DIM, :] * wa + b[:, 0:HEAD_DIM, :] * wb
        l = a[:, HEAD_DIM + 1:HEAD_DIM + 2, :] * wa + b[:, HEAD_DIM + 1:HEAD_DIM + 2, :] * wb
        return o, m, l

    def merge_into(lo, p, other):
        o, m, l = merge(acc[lo:lo + hh, :, q_rows(p)], other[...])
        acc[lo:lo + hh, 0:HEAD_DIM, q_rows(p)] = o
        acc[lo:lo + hh, HEAD_DIM:HEAD_DIM + 1, q_rows(p)] = m
        acc[lo:lo + hh, HEAD_DIM + 1:HEAD_DIM + 2, q_rows(p)] = l

    p2 = [remote(acc.at[:, :, q_rows(nxt)], r2l, rs.at[2], rr.at[2], right),
          remote(acc.at[:, :, q_rows(prev)], r2r, rs.at[3], rr.at[3], left)]
    p1[0].wait_recv()
    merge_into(0, nxt, r1l)
    p2[0].start()
    p1[1].wait_recv()
    merge_into(hh, prev, r1r)
    p2[1].start()
    for copy in p2:
        copy.wait_recv()
    for h in range(heads):
        a, b, d = acc[h:h + 1, :, q_rows(vx)], r2l[h:h + 1], r2r[h:h + 1]
        o, m, l = merge(a, b)
        md = d[:, HEAD_DIM:HEAD_DIM + 1, :]
        top = jnp.maximum(m, md)
        w, wd = jnp.exp2((m - top) * EXP_SCALE), jnp.exp2((md - top) * EXP_SCALE)
        o = o * w + d[:, 0:HEAD_DIM, :] * wd
        l = l * w + d[:, HEAD_DIM + 1:HEAD_DIM + 2, :] * wd
        otmp[:, h * HEAD_DIM:(h + 1) * HEAD_DIM] = (o / l)[0].T.astype(BF16)

    other_at = {'tp': vy, 'cp': vx * 2 + 1 - core}
    other_out = remote(otmp, obuf.at[core], os.at[1], orr.at[1], other_at)
    other_out.start()
    same_out = remote(otmp, obuf.at[core], os.at[0], orr.at[0], me.mirrored(core))

    @pl.when(moving)
    def _():
        same_out.start()
        same_out.wait_recv()

    @pl.when(jnp.logical_not(moving))
    def _():
        obuf[core] = otmp[...]

    remote(otmp, obuf.at[1 - core], os.at[1], orr.at[1], partner).wait_recv()
    o_out[:, 0:head_w] = obuf[0]
    o_out[:, head_w:2 * head_w] = obuf[1]
    for copy in x_copies + kv_copies + q_copies + p1 + p2 + [other_out]:
        copy.wait_send()

    @pl.when(moving)
    def _():
        mirror_send.wait_send()
        same_out.wait_send()


def mlp_kernel(o_in, xres, gain, wo, wg, wu, wd, out,
               wov, wgv, wuv, wdv, part, r1l, r1r, r2l, r2r, hbuf, hres, ubuf, fin, fbuf,
               wosem, wgsem, wusem, wdsem, s1, q1, s2, q2, hs, hr, ps, pr, us, ur, fs, fr):
    me = Place()
    y, core = me.y, me.core
    nc, _, _, cw = part.shape
    half_w = nc * cw
    width = 2 * half_w
    rows = o_in.shape[0]
    block_rows = rows // RING
    nu, _, uw = wgv.shape
    half_f = nu * uw
    nd = wdv.shape[0]
    partner = me.at(core=1 - core)
    up, down = me.at(dy=1), me.at(dy=RING - 1)
    far, nxt, prev = (y + 2) % RING, (y + 1) % RING, (y + 3) % RING
    col0 = core * half_w

    def lanes(start, size):
        return pl.ds(pl.multiple_of(start, 128), size)

    def wo_copy(j):
        return pltpu.make_async_copy(wo.at[:, lanes(col0 + j * cw, cw)], wov.at[j], wosem.at[j])

    def wd_copy(j):
        return pltpu.make_async_copy(wd.at[:, lanes(col0 + j * cw, cw)], wdv.at[j % nd], wdsem.at[j % nd])

    def wg_copy(j):
        return pltpu.make_async_copy(wg.at[:, lanes(core * half_f + j * uw, uw)], wgv.at[j], wgsem.at[j])

    def wu_copy(j):
        return pltpu.make_async_copy(wu.at[:, lanes(core * half_f + j * uw, uw)], wuv.at[j], wusem.at[j])

    for j in range(nc):
        wo_copy(j).start()
    for j in range(nu):
        wg_copy(j).start()
        wu_copy(j).start()
    for j in range(nd):
        wd_copy(j).start()

    barrier([up, down, partner])

    hc = cw // 2

    def first_sends(j):
        return (remote(part.at[j, far, :, pl.ds(0, hc)], r1l.at[j], s1.at[0, j], q1.at[0, j], up),
                remote(part.at[j, far, :, pl.ds(hc, hc)], r1r.at[j], s1.at[1, j], q1.at[1, j], down))

    def second_sends(j):
        return (remote(part.at[j, nxt], r2l.at[j], s2.at[0, j], q2.at[0, j], up),
                remote(part.at[j, prev], r2r.at[j], s2.at[1, j], q2.at[1, j], down))

    def relay(j, carry):
        a, b = first_sends(j)
        a.wait_recv()
        part[j, nxt, :, 0:hc] = part[j, nxt, :, 0:hc] + r1l[j]
        b.wait_recv()
        part[j, prev, :, hc:cw] = part[j, prev, :, hc:cw] + r1r[j]
        for copy in second_sends(j):
            copy.start()
        return carry

    def total(j):
        for copy in second_sends(j):
            copy.wait_recv()
        return part[j, y] + r2l[j] + r2r[j]

    def drain(j, carry):
        for copy in first_sends(j) + second_sends(j):
            copy.wait_send()
        return carry

    attended = o_in[...]

    def out_chunk(j, carry):
        wo_copy(j).wait()
        part[j] = jnp.dot(attended, wov[j], preferred_element_type=F32).reshape(RING, block_rows, cw)
        for copy in first_sends(j):
            copy.start()
        return carry

    lax.fori_loop(0, nc, out_chunk, 0)
    lax.fori_loop(0, nc, relay, 0)

    def h_piece(c, p, j):
        return hbuf.at[c, p, :, lanes(j * cw, cw)]

    def h_half(c, p, j, i):
        return hbuf.at[c, p, :, lanes(j * cw + i * hc, hc)]

    def h_steps(j):
        return (remote(h_piece(core, y, j), h_piece(core, y, j), hs.at[0, j], hr.at[0, j], up),
                remote(h_piece(core, y, j), h_piece(core, y, j), hs.at[1, j], hr.at[1, j], down),
                remote(h_half(core, prev, j, 0), h_half(core, prev, j, 0), hs.at[2, j], hr.at[2, j], up),
                remote(h_half(core, nxt, j, 1), h_half(core, nxt, j, 1), hs.at[3, j], hr.at[3, j], down))

    def h_give(j, i, p, c):
        return remote(h_piece(c, p, j), h_piece(c, p, j), ps.at[i, j], pr.at[i, j], partner)

    def mid_chunk(j, carry):
        c = lanes(j * cw, cw)
        mid = (xres[:, c].astype(F32) + total(j)).astype(BF16)
        hres[:, c] = mid
        hbuf[core, y, :, c] = mid
        for copy in h_steps(j)[:2] + (h_give(j, 0, y, core),):
            copy.start()
        return carry

    lax.fori_loop(0, nc, mid_chunk, 0)

    def h_forward(j, carry):
        steps = h_steps(j)
        remote(h_piece(core, prev, j), h_piece(core, prev, j), hs.at[0, j], hr.at[0, j], down).wait_recv()
        steps[2].start()
        h_give(j, 1, prev, core).start()
        remote(h_piece(core, nxt, j), h_piece(core, nxt, j), hs.at[1, j], hr.at[1, j], up).wait_recv()
        steps[3].start()
        h_give(j, 2, nxt, core).start()
        return carry

    lax.fori_loop(0, nc, h_forward, 0)

    def h_last(j, carry):
        remote(h_half(core, far, j, 0), h_half(core, far, j, 0), hs.at[2, j], hr.at[2, j], down).wait_recv()
        remote(h_half(core, far, j, 1), h_half(core, far, j, 1), hs.at[3, j], hr.at[3, j], up).wait_recv()
        h_give(j, 3, far, core).start()
        return carry

    lax.fori_loop(0, nc, h_last, 0)

    def h_end(j, carry):
        for i, p in enumerate((y, prev, nxt, far)):
            h_give(j, i, p, 1 - core).wait_recv()
        for copy in h_steps(j):
            copy.wait_send()
        for i, p in enumerate((y, prev, nxt, far)):
            h_give(j, i, p, core).wait_send()
        return carry

    lax.fori_loop(0, nc, h_end, 0)
    lax.fori_loop(0, nc, drain, 0)

    def norm_block(i, carry):
        v0, v1 = hbuf[0, i].astype(F32), hbuf[1, i].astype(F32)
        mean = (jnp.sum(v0 * v0, axis=-1, keepdims=True) + jnp.sum(v1 * v1, axis=-1, keepdims=True)) / width
        inv = lax.rsqrt(mean + NORM_EPS)
        hbuf[0, i] = (v0 * inv * gain[0:1, :].astype(F32)).astype(BF16)
        hbuf[1, i] = (v1 * inv * gain[1:2, :].astype(F32)).astype(BF16)
        return carry

    lax.fori_loop(0, RING, norm_block, 0)
    b0, b1 = hbuf[0].reshape(rows, half_w), hbuf[1].reshape(rows, half_w)

    def u_copy(j, c):
        at = ubuf.at[:, lanes(c * half_f + j * uw, uw)]
        return remote(at, at, us.at[j], ur.at[j], partner)

    def up_chunk(j, carry):
        wg_copy(j).wait()
        wu_copy(j).wait()
        gate = jnp.dot(b0, wgv[j, 0:half_w, :], preferred_element_type=F32) + jnp.dot(b1, wgv[j, half_w:width, :], preferred_element_type=F32)
        upper = jnp.dot(b0, wuv[j, 0:half_w, :], preferred_element_type=F32) + jnp.dot(b1, wuv[j, half_w:width, :], preferred_element_type=F32)
        ubuf[:, lanes(core * half_f + j * uw, uw)] = (jax.nn.silu(gate) * upper).astype(BF16)
        u_copy(j, core).start()
        return carry

    lax.fori_loop(0, nu, up_chunk, 0)
    for j in range(nu):
        u_copy(j, 1 - core).wait_recv()

    for j in range(nc):
        wd_copy(j).wait()
        part[j] = jnp.dot(ubuf[...], wdv[j % nd], preferred_element_type=F32).reshape(RING, block_rows, cw)
        if j + nd < nc:
            wd_copy(j + nd).start()
        for copy in first_sends(j):
            copy.start()
    lax.fori_loop(0, nc, relay, 0)

    def last_chunk(j, carry):
        c = lanes(j * cw, cw)
        fin[:, :, c] = (hres[:, c].astype(F32) + total(j)).astype(BF16).reshape(2, block_rows // 2, cw)
        return carry

    lax.fori_loop(0, nc, last_chunk, 0)
    swap = remote(fin.at[1 - core], fbuf.at[core], fs.at[0], fr.at[0], partner)
    swap.start()
    own = fin[core]
    out[:, lanes(col0, half_w)] = own
    remote(fin.at[core], fbuf.at[1 - core], fs.at[0], fr.at[0], partner).wait_recv()
    out[:, lanes((1 - core) * half_w, half_w)] = fbuf[1 - core]
    for j in range(nu):
        u_copy(j, core).wait_send()
    lax.fori_loop(0, nc, drain, 0)
    swap.wait_send()


def dma(*shape):
    return pltpu.SemaphoreType.DMA(shape)


def relative_positions(chips, shards, row_count):
    r = jnp.arange(row_count, dtype=jnp.int32)
    per_chip = 2 * RING * 16
    x = chips + r // per_chip
    y, core, w = (r % per_chip) // 32, (r % 32) // 16, r % 16
    k = (2 * x + core) * RING + y
    run = jnp.where(w < 8, k, 2 * shards - 1 - k)
    return run * 8 + w % 8


def solution(mesh):
    token_spec = P(('dp', 'cp', 'tp'), None)
    column_spec = P(None, 'tp')
    row_spec = P('tp', None)
    shards = mesh.shape['tp'] * mesh.shape['cp']

    def device_layer(hidden_loc, pos_loc, cache_len, cache_k, cache_v, norm1_gain, w_query, w_key, w_value, w_out, norm2_gain, w_gate, w_up, w_down):
        shard_rows, width = hidden_loc.shape
        half_w = width // 2
        chip_rows = 2 * RING * shard_rows
        rows = RING * chip_rows
        slots = cache_k.shape[0]
        head_w = w_query.shape[1] // 2
        heads = head_w // HEAD_DIM
        cp, y = lax.axis_index('cp'), lax.axis_index('tp')
        half = HEAD_DIM // 2
        own_rel = relative_positions(cp // 2, shards, chip_rows)
        relk = relative_positions(jnp.where(cp % 2 == 0, cp // 2, y), shards, chip_rows)
        relq = relative_positions(0, shards, rows)
        inv_freq = 1.0 / (ROPE_BASE ** (jnp.arange(half, dtype=F32) * (2.0 / HEAD_DIM)))
        angles = (cache_len[0] + own_rel).astype(F32)[:, None] * inv_freq[None, :]
        cos, sin = jnp.cos(angles), jnp.sin(angles)
        cos = jnp.concatenate([cos, cos], axis=1)
        sin = jnp.concatenate([-sin, sin], axis=1)
        block = (heads, HEAD_DIM + 8, chip_rows)
        part_block = (heads // 2,) + block[1:]
        attended, xres = pl.pallas_call(
            attention_kernel,
            out_shape=(jax.ShapeDtypeStruct((chip_rows, 2 * head_w), BF16), jax.ShapeDtypeStruct((2 * shard_rows, half_w), BF16)),
            in_specs=[ANY, SMEM, ANY, ANY, VMEM, ANY, ANY, ANY, VMEM, VMEM, VMEM, VMEM],
            out_specs=(VMEM, VMEM),
            scratch_shapes=[
                pltpu.VMEM((RING, 2, shard_rows, width), BF16),
                pltpu.VMEM((RING, 2 * shard_rows, width), BF16),
                pltpu.VMEM((width, head_w), BF16),
                pltpu.VMEM((width, HEAD_DIM), BF16),
                pltpu.VMEM((width, HEAD_DIM), BF16),
                pltpu.VMEM((2 * RING, slots, HEAD_DIM), BF16),
                pltpu.VMEM((2 * RING, slots, HEAD_DIM), BF16),
                pltpu.VMEM((2, slots, HEAD_DIM), BF16),
                pltpu.VMEM((2, slots, HEAD_DIM), BF16),
                pltpu.VMEM((slots, 2 * HEAD_DIM), BF16),
                pltpu.VMEM((HEAD_DIM, slots), BF16),
                pltpu.VMEM((chip_rows, head_w + 2 * HEAD_DIM), BF16),
                pltpu.VMEM((rows, head_w + 2 * HEAD_DIM), BF16),
                pltpu.VMEM((heads, rows, 2 * HEAD_DIM), BF16),
                pltpu.VMEM((slots, 256), F32),
                pltpu.VMEM((slots, 256), F32),
                pltpu.VMEM((heads, HEAD_DIM + 8, rows), F32),
                pltpu.VMEM(part_block, F32),
                pltpu.VMEM(part_block, F32),
                pltpu.VMEM(block, F32),
                pltpu.VMEM(block, F32),
                pltpu.VMEM((chip_rows, head_w), BF16),
                pltpu.VMEM((2, chip_rows, head_w), BF16),
                dma(4), dma(4), dma(4), dma(4), dma(4), dma(18), dma(2 * RING, 2), dma(2, 2), dma(1), dma(1),
                dma(4), dma(4), dma(4), dma(4), dma(2), dma(2),
            ],
            compiler_params=pltpu.CompilerParams(collective_id=0, has_side_effects=True, vmem_limit_bytes=67043328),
            name='attention',
        )(hidden_loc, cache_len, cache_k, cache_v, norm1_gain.reshape(1, width), w_query, w_key, w_value, cos, sin, relq.reshape(1, rows), relk.reshape(chip_rows, 1))

        cw = 512 if half_w % 512 == 0 and half_w > 512 else 256
        nc = half_w // cw
        half_f = w_gate.shape[1] // 2
        uw = 256
        nu = half_f // uw
        nd = max(1, nc - 1)
        br = 2 * shard_rows
        return pl.pallas_call(
            mlp_kernel,
            out_shape=jax.ShapeDtypeStruct((shard_rows, width), BF16),
            in_specs=[VMEM, VMEM, VMEM, ANY, ANY, ANY, ANY],
            out_specs=VMEM,
            scratch_shapes=[
                pltpu.VMEM((nc, 2 * head_w, cw), BF16),
                pltpu.VMEM((nu, width, uw), BF16),
                pltpu.VMEM((nu, width, uw), BF16),
                pltpu.VMEM((nd, 2 * half_f, cw), BF16),
                pltpu.VMEM((nc, RING, br, cw), F32),
                pltpu.VMEM((nc, br, cw // 2), F32),
                pltpu.VMEM((nc, br, cw // 2), F32),
                pltpu.VMEM((nc, br, cw), F32),
                pltpu.VMEM((nc, br, cw), F32),
                pltpu.VMEM((2, RING, br, half_w), BF16),
                pltpu.VMEM((br, half_w), BF16),
                pltpu.VMEM((chip_rows, 2 * half_f), BF16),
                pltpu.VMEM((2, shard_rows, half_w), BF16),
                pltpu.VMEM((2, shard_rows, half_w), BF16),
                dma(nc), dma(nu), dma(nu), dma(nd), dma(2, nc), dma(2, nc), dma(2, nc), dma(2, nc),
                dma(4, nc), dma(4, nc), dma(4, nc), dma(4, nc), dma(nu), dma(nu), dma(1), dma(1),
            ],
            compiler_params=pltpu.CompilerParams(collective_id=1, has_side_effects=True, vmem_limit_bytes=67043328),
            name='mlp',
        )(attended, xres, norm2_gain.reshape(2, half_w), w_out, w_gate, w_up, w_down)

    return jax.shard_map(device_layer, mesh=mesh, in_specs=(token_spec, P(('dp', 'cp', 'tp')), P('dp'), token_spec, token_spec, P(), column_spec, column_spec, column_spec, row_spec, P(), column_spec, column_spec, row_spec), out_specs=token_spec, check_vma=False)
```

```python
import functools
import math
import jax
import jax.numpy as jnp
from jax import lax
from jax.experimental import pallas as pl
from jax.experimental.pallas import tpu as pltpu
from jax.sharding import PartitionSpec as P

HEAD_DIM = 128
ROPE_BASE = 500000.0
NORM_EPS = 1e-5
MESH = pl.DeviceIdType.MESH
F32 = jnp.float32
BF16 = jnp.bfloat16
M_INIT = -1e38
MASKED = -3e38
EXP_SCALE = math.log2(math.e) / math.sqrt(HEAD_DIM)
RING = 4
STEP = 512
ANY = pl.BlockSpec(memory_space=pl.ANY)
VMEM = pl.BlockSpec(memory_space=pltpu.VMEM)
SMEM = pl.BlockSpec(memory_space=pltpu.SMEM)


class Place:
    def __init__(self):
        self.y = lax.axis_index('tp')
        cp = lax.axis_index('cp')
        self.x = cp // 2
        self.core = cp % 2
        self.vx = self.x + self.core * (self.y - self.x)
        self.vy = self.y + self.core * (self.x - self.y)

    def at(self, dx=0, dy=0, core=None):
        return {'tp': (self.y + dy) % RING, 'cp': ((self.x + dx) % RING) * 2 + (self.core if core is None else core)}

    def mirrored(self, core):
        return {'tp': self.x, 'cp': self.y * 2 + core}


def remote(src, dst, send_sem, recv_sem, device):
    return pltpu.make_async_remote_copy(src_ref=src, dst_ref=dst, send_sem=send_sem, recv_sem=recv_sem, device_id=device, device_id_type=MESH)


def barrier(devices):
    sem = pltpu.get_barrier_semaphore()
    for device in devices:
        pl.semaphore_signal(sem, inc=1, device_id=device, device_id_type=MESH)
    pl.semaphore_wait(sem, len(devices))


def ring_gather(pos, right, left, block, half, sends, recvs, own=None, partner=None, core=None, psends=None, precvs=None, between=None):
    prev, nxt, far = (pos + 3) % RING, (pos + 1) % RING, (pos + 2) % RING
    mine = block(pos, core) if own is None else own
    to_right = remote(mine, block(pos, core), sends.at[0], recvs.at[0], right)
    to_left = remote(mine, block(pos, core), sends.at[1], recvs.at[1], left)
    to_right.start()
    to_left.start()
    copies = [to_right, to_left]
    given = []

    def give(p, i, source=None):
        if partner is not None:
            copy = remote(block(p, core) if source is None else source, block(p, core), psends.at[i], precvs.at[i], partner)
            copy.start()
            given.append(copy)

    give(pos, 0, mine)
    remote(block(prev, core), block(prev, core), sends.at[0], recvs.at[0], left).wait_recv()
    fwd_right = remote(half(prev, core, 0), half(prev, core, 0), sends.at[2], recvs.at[2], right)
    fwd_right.start()
    give(prev, 1)
    remote(block(nxt, core), block(nxt, core), sends.at[1], recvs.at[1], right).wait_recv()
    fwd_left = remote(half(nxt, core, 1), half(nxt, core, 1), sends.at[3], recvs.at[3], left)
    fwd_left.start()
    give(nxt, 2)
    copies += [fwd_right, fwd_left]
    if between is not None:
        between()
    remote(half(far, core, 0), half(far, core, 0), sends.at[2], recvs.at[2], left).wait_recv()
    remote(half(far, core, 1), half(far, core, 1), sends.at[3], recvs.at[3], right).wait_recv()
    give(far, 3)
    if partner is not None:
        for i, p in enumerate((pos, prev, nxt, far)):
            remote(block(p, 1 - core), block(p, 1 - core), psends.at[i], precvs.at[i], partner).wait_recv()
    return copies + given


def attention_kernel(x_in, len_ref, ck, cv, gain, wq, wk, wv, cos_ref, sin_ref, relq_ref, relk_ref, o_out, xres_out,
                     xbuf, abuf, wqv, wkv, wvv, kbuf, vbuf, rk, rv, kaug, vt, qkv, qall, qaug, sa, sb, acc, r1l, r1r, r2l, r2r, otmp, obuf,
                     lsem, xs, xr, ps, pr, kvs, kvr, relay_r, ts, tr, qs, qr, rs, rr, os, orr):
    me = Place()
    x, y, core, vx, vy = me.x, me.y, me.core, me.vx, me.vy
    width = x_in.shape[1]
    half_w = width // 2
    slots = ck.shape[0]
    rows = qall.shape[0]
    chip_rows = rows // RING
    heads = acc.shape[0]
    head_w = heads * HEAD_DIM
    partner = me.at(core=1 - core)
    up, down = me.at(dy=1), me.at(dy=RING - 1)
    right, left = me.at(dx=1 - core, dy=core), me.at(dx=(1 - core) * (RING - 1), dy=core * (RING - 1))
    ahead, behind = me.at(dx=core, dy=1 - core), me.at(dx=core * (RING - 1), dy=(1 - core) * (RING - 1))
    moving = jnp.logical_and(core == 1, x != y)

    local = [
        pltpu.make_async_copy(x_in, xbuf.at[y, core], lsem.at[0]),
        pltpu.make_async_copy(wq.at[:, pl.ds(pl.multiple_of(core * head_w, head_w), head_w)], wqv, lsem.at[1]),
        pltpu.make_async_copy(wk.at[:, pl.ds(pl.multiple_of(core * HEAD_DIM, HEAD_DIM), HEAD_DIM)], wkv, lsem.at[2]),
        pltpu.make_async_copy(wv.at[:, pl.ds(pl.multiple_of(core * HEAD_DIM, HEAD_DIM), HEAD_DIM)], wvv, lsem.at[3]),
    ]
    local[0].start()
    for copy in local[1:]:
        copy.start()

    peers = [partner, me.mirrored(0), me.mirrored(1)]
    peers += [me.at(dy=d, core=c) for d in range(1, RING) for c in range(2)] + [me.at(dx=d, core=c) for d in range(1, RING) for c in range(2)]
    barrier(peers)

    def kv_lanes(head):
        return pl.ds(pl.multiple_of(head * HEAD_DIM, HEAD_DIM), HEAD_DIM)

    def target(role, d):
        return me.at(dx=d if role else 0, dy=0 if role else d, core=role)

    def target_lanes(role, d):
        return kv_lanes(2 * (((x if role else y) + d) % RING) + role)

    kv_copies = []

    def kv_send(src, dst, recv, device):
        copy = remote(src, dst, kvs.at[len(kv_copies)], recv, device)
        copy.start()
        kv_copies.append(copy)

    def send_near():
        other_vy = x + y - vy
        for i, (src, dst) in enumerate(((ck, kbuf), (cv, vbuf))):
            pltpu.make_async_copy(src.at[:, kv_lanes(2 * vy + core)], dst.at[core], kvr.at[core, i]).start()
            kv_send(src.at[:, kv_lanes(2 * other_vy + 1 - core)], dst.at[core], kvr.at[core, i], partner)
        for role in range(2):
            kv_send(ck.at[:, target_lanes(role, 2)], rk.at[core], relay_r.at[0, core], target(role, 1))
            kv_send(cv.at[:, target_lanes(role, 2)], rv.at[core], relay_r.at[1, core], target(role, RING - 1))

    def send_far():
        for i, (src, dst) in enumerate(((ck, kbuf), (cv, vbuf))):
            for role in range(2):
                for d, slot in ((1, 2), (3, 4)):
                    kv_send(src.at[:, target_lanes(role, d)], dst.at[slot + core], kvr.at[slot + core, i], target(role, d))
        for c in range(2):
            remote(rk.at[c], rk.at[c], kvs.at[0], relay_r.at[0, c], behind).wait_recv()
            kv_send(rk.at[c], kbuf.at[6 + c], kvr.at[6 + c, 0], ahead)
            remote(rv.at[c], rv.at[c], kvs.at[0], relay_r.at[1, c], ahead).wait_recv()
            kv_send(rv.at[c], vbuf.at[6 + c], kvr.at[6 + c, 1], behind)

    x_copies = ring_gather(
        y, up, down, lambda p, c: xbuf.at[p, c], lambda p, c, i: xbuf.at[p, c, :, pl.ds(i * half_w, half_w)],
        xs, xr, own=x_in, partner=partner, core=core, psends=ps, precvs=pr, between=send_near)
    local[0].wait()

    def norm_block(i, carry):
        values = xbuf[i].reshape(2 * xbuf.shape[2], width).astype(F32)
        inv = lax.rsqrt(jnp.mean(values * values, axis=-1, keepdims=True) + NORM_EPS)
        abuf[i] = (values * inv * gain[...].astype(F32)).astype(BF16)
        return carry

    lax.fori_loop(0, RING, norm_block, 0)
    xres_out[...] = xbuf[y, :, :, pl.ds(pl.multiple_of(core * half_w, half_w), half_w)].reshape(xres_out.shape)

    for copy in local[1:]:
        copy.wait()
    normed = abuf[...].reshape(chip_rows, width)
    cos, sin = cos_ref[...], sin_ref[...]

    def rotate(v):
        return (v * cos + pltpu.roll(v, HEAD_DIM // 2, 1) * sin).astype(BF16)

    q = jnp.dot(normed, wqv[...], preferred_element_type=F32)
    for h in range(heads):
        qkv[:, h * HEAD_DIM:(h + 1) * HEAD_DIM] = rotate(q[:, h * HEAD_DIM:(h + 1) * HEAD_DIM])
    qkv[:, head_w:head_w + HEAD_DIM] = rotate(jnp.dot(normed, wkv[...], preferred_element_type=F32))
    qkv[:, head_w + HEAD_DIM:] = jnp.dot(normed, wvv[...], preferred_element_type=F32).astype(BF16)

    def q_rows(p):
        return pl.ds(pl.multiple_of(p * chip_rows, chip_rows), chip_rows)

    across_in = remote(qkv, qall.at[q_rows(vx)], ts.at[0], tr.at[0], me.mirrored(core))
    mirror_send = remote(qkv, qall.at[q_rows(x)], ts.at[0], tr.at[0], me.mirrored(core))

    @pl.when(moving)
    def _():
        mirror_send.start()
        across_in.wait_recv()

    @pl.when(jnp.logical_not(moving))
    def _():
        qall[q_rows(vx), :] = qkv[...]

    q_copies = ring_gather(
        vx, right, left, lambda p, c: qall.at[q_rows(p), pl.ds(0, head_w)],
        lambda p, c, i: qall.at[q_rows(p), pl.ds(i * (head_w // 2), head_w // 2)], qs, qr, between=send_far)

    first_lane = jnp.where(lax.broadcasted_iota(jnp.int32, (rows, HEAD_DIM), 1) == 0, 1.0, 0.0).astype(BF16)
    for h in range(heads):
        qaug[h, :, 0:HEAD_DIM] = qall[:, h * HEAD_DIM:(h + 1) * HEAD_DIM]
        qaug[h, :, HEAD_DIM:] = first_lane

    tile = 256
    tiles = rows // tile
    contract_last = (((1,), (1,)), ((), ()))

    def finish(s_ref, e_top, vt_ref, h, j, first, depth):
        lanes = pl.ds(j * tile, tile)
        if first:
            m_new = jnp.maximum(e_top, M_INIT)
        else:
            m_old = acc[h, HEAD_DIM:HEAD_DIM + 1, lanes]
            l_old = acc[h, HEAD_DIM + 1:HEAD_DIM + 2, lanes]
            m_new = jnp.maximum(e_top, m_old)
        m_scaled = m_new * EXP_SCALE
        part_l, o = None, None
        step = min(STEP, depth)
        for k in range(0, depth, step):
            e = jnp.exp2(s_ref[k:k + step, :] * EXP_SCALE - m_scaled)
            total_e = jnp.sum(e.reshape(step // 8, 8, tile), axis=0)
            part_l = total_e if part_l is None else part_l + total_e
            term = jnp.dot(vt_ref[:, k:k + step], e.astype(BF16), preferred_element_type=F32)
            o = term if o is None else o + term
        l_new = jnp.sum(part_l, axis=0, keepdims=True)
        if not first:
            alpha = jnp.exp2((m_old - m_new) * EXP_SCALE)
            l_new = l_new + l_old * alpha
            o = o + acc[h, 0:HEAD_DIM, lanes] * alpha
        acc[h, 0:HEAD_DIM, lanes] = o
        acc[h, HEAD_DIM:HEAD_DIM + 1, lanes] = m_new
        acc[h, HEAD_DIM + 1:HEAD_DIM + 2, lanes] = l_new

    my_rows = q_rows(vx)
    vnew_t = qall[my_rows, head_w + HEAD_DIM:].T
    knew = qall[my_rows, head_w:head_w + HEAD_DIM]

    def new_head(h, carry):
        for j in range(tiles):
            s = lax.dot_general(knew, qaug[h, j * tile:(j + 1) * tile, 0:HEAD_DIM], contract_last, preferred_element_type=F32)
            causal = jnp.broadcast_to(relk_ref[...], s.shape) <= jnp.broadcast_to(relq_ref[:, j * tile:(j + 1) * tile], s.shape)
            s = jnp.where(causal, s, -jnp.inf)
            finish(s, jnp.max(s, axis=0, keepdims=True), vnew_t, h, j, True, chip_rows)
        return carry

    lax.fori_loop(0, heads, new_head, 0)
    cache_len = len_ref[0]
    slot_ids = lax.broadcasted_iota(jnp.int32, (slots, HEAD_DIM), 0)

    def scores(h, j, dst):
        s = lax.dot_general(kaug[...], qaug[h, j * tile:(j + 1) * tile, :], contract_last, preferred_element_type=F32)
        dst[...] = s
        return jnp.max(s, axis=0, keepdims=True)

    def source(s, carry):
        u, src_core = s // 2, s % 2
        d = u + (u // 2) * (1 - 2 * (u % 2))
        src_x = (x - core * d + RING) % RING
        src_y = (y - (1 - core) * d + RING) % RING
        base = ((2 * src_x + src_core) * RING + src_y) * slots
        for i, (src, dst) in enumerate(((ck, kbuf), (cv, vbuf))):
            pltpu.make_async_copy(src.at[:, pl.ds(0, HEAD_DIM)], dst.at[s], kvr.at[s, i]).wait()
        vt[...] = vbuf[s].T
        seen = slot_ids < cache_len - base
        kaug[:, 0:HEAD_DIM] = jnp.where(seen, kbuf[s].astype(F32), 0.0).astype(BF16)
        kaug[:, HEAD_DIM:] = jnp.where(seen, 0.0, MASKED).astype(BF16)

        def head(h, top_a):
            top_b = scores(h, 1, sb)
            finish(sa, top_a, vt, h, 0, False, slots)
            top_a = scores(jnp.minimum(h + 1, heads - 1), 0, sa)
            finish(sb, top_b, vt, h, 1, False, slots)
            return top_a

        lax.fori_loop(0, heads, head, scores(0, 0, sa))
        return carry

    lax.fori_loop(0, 2 * RING, source, 0)

    hh = heads // 2
    far, nxt, prev = (vx + 2) % RING, (vx + 1) % RING, (vx + 3) % RING
    p1 = [remote(acc.at[pl.ds(0, hh), :, q_rows(far)], r1l, rs.at[0], rr.at[0], right),
          remote(acc.at[pl.ds(hh, hh), :, q_rows(far)], r1r, rs.at[1], rr.at[1], left)]
    for copy in p1:
        copy.start()

    def merge(a, b):
        ma, mb = a[:, HEAD_DIM:HEAD_DIM + 1, :], b[:, HEAD_DIM:HEAD_DIM + 1, :]
        m = jnp.maximum(ma, mb)
        wa, wb = jnp.exp2((ma - m) * EXP_SCALE), jnp.exp2((mb - m) * EXP_SCALE)
        o = a[:, 0:HEAD_DIM, :] * wa + b[:, 0:HEAD_DIM, :] * wb
        l = a[:, HEAD_DIM + 1:HEAD_DIM + 2, :] * wa + b[:, HEAD_DIM + 1:HEAD_DIM + 2, :] * wb
        return o, m, l

    def merge_into(lo, p, other):
        o, m, l = merge(acc[lo:lo + hh, :, q_rows(p)], other[...])
        acc[lo:lo + hh, 0:HEAD_DIM, q_rows(p)] = o
        acc[lo:lo + hh, HEAD_DIM:HEAD_DIM + 1, q_rows(p)] = m
        acc[lo:lo + hh, HEAD_DIM + 1:HEAD_DIM + 2, q_rows(p)] = l

    p2 = [remote(acc.at[:, :, q_rows(nxt)], r2l, rs.at[2], rr.at[2], right),
          remote(acc.at[:, :, q_rows(prev)], r2r, rs.at[3], rr.at[3], left)]
    p1[0].wait_recv()
    merge_into(0, nxt, r1l)
    p2[0].start()
    p1[1].wait_recv()
    merge_into(hh, prev, r1r)
    p2[1].start()
    for copy in p2:
        copy.wait_recv()
    for h in range(heads):
        a, b, d = acc[h:h + 1, :, q_rows(vx)], r2l[h:h + 1], r2r[h:h + 1]
        o, m, l = merge(a, b)
        md = d[:, HEAD_DIM:HEAD_DIM + 1, :]
        top = jnp.maximum(m, md)
        w, wd = jnp.exp2((m - top) * EXP_SCALE), jnp.exp2((md - top) * EXP_SCALE)
        o = o * w + d[:, 0:HEAD_DIM, :] * wd
        l = l * w + d[:, HEAD_DIM + 1:HEAD_DIM + 2, :] * wd
        otmp[:, h * HEAD_DIM:(h + 1) * HEAD_DIM] = (o / l)[0].T.astype(BF16)

    other_at = {'tp': vy, 'cp': vx * 2 + 1 - core}
    other_out = remote(otmp, obuf.at[core], os.at[1], orr.at[1], other_at)
    other_out.start()
    same_out = remote(otmp, obuf.at[core], os.at[0], orr.at[0], me.mirrored(core))

    @pl.when(moving)
    def _():
        same_out.start()
        same_out.wait_recv()

    @pl.when(jnp.logical_not(moving))
    def _():
        obuf[core] = otmp[...]

    remote(otmp, obuf.at[1 - core], os.at[1], orr.at[1], partner).wait_recv()
    o_out[:, 0:head_w] = obuf[0]
    o_out[:, head_w:2 * head_w] = obuf[1]
    for copy in x_copies + kv_copies + q_copies + p1 + p2 + [other_out]:
        copy.wait_send()

    @pl.when(moving)
    def _():
        mirror_send.wait_send()
        same_out.wait_send()


def mlp_kernel(o_in, xres, gain, wo, wg, wu, wd, out,
               wgv, wuv, wdv, part, r1l, r1r, r2l, r2r, hbuf, hres, ubuf, fin, fbuf,
               wsem, s1, q1, s2, q2, hs, hr, ps, pr, us, ur, fs, fr):
    me = Place()
    y, core = me.y, me.core
    nc, _, _, cw = part.shape
    half_w = nc * cw
    width = 2 * half_w
    rows = o_in.shape[0]
    block_rows = rows // RING
    half_f = wgv.shape[1]
    uw = 256
    nu = half_f // uw
    partner = me.at(core=1 - core)
    up, down = me.at(dy=1), me.at(dy=RING - 1)
    far, nxt, prev = (y + 2) % RING, (y + 1) % RING, (y + 3) % RING
    col0 = core * half_w

    def lanes(start, size):
        return pl.ds(pl.multiple_of(start, 128), size)

    wo_rows, wd_rows = wo.shape[0], wd.shape[0]
    up_cols, out_cols = lanes(core * half_f, half_f), lanes(col0, half_w)
    wo_load = pltpu.make_async_copy(wo.at[:, out_cols], wdv.at[pl.ds(0, wo_rows), :], wsem.at[0])
    wd_load = pltpu.make_async_copy(wd.at[pl.ds(wo_rows, wd_rows - wo_rows), out_cols], wdv.at[pl.ds(wo_rows, wd_rows - wo_rows), :], wsem.at[1])
    wd_late = pltpu.make_async_copy(wd.at[pl.ds(0, wo_rows), out_cols], wdv.at[pl.ds(0, wo_rows), :], wsem.at[2])
    wg_load = pltpu.make_async_copy(wg.at[:, up_cols], wgv, wsem.at[3])
    wu_load = pltpu.make_async_copy(wu.at[:, up_cols], wuv, wsem.at[4])
    for copy in (wo_load, wg_load, wu_load, wd_load):
        copy.start()

    barrier([up, down, partner])

    hc = cw // 2

    def first_sends(j):
        return (remote(part.at[j, far, :, pl.ds(0, hc)], r1l.at[j], s1.at[0, j], q1.at[0, j], up),
                remote(part.at[j, far, :, pl.ds(hc, hc)], r1r.at[j], s1.at[1, j], q1.at[1, j], down))

    def second_sends(j):
        return (remote(part.at[j, nxt], r2l.at[j], s2.at[0, j], q2.at[0, j], up),
                remote(part.at[j, prev], r2r.at[j], s2.at[1, j], q2.at[1, j], down))

    def relay(j, carry):
        a, b = first_sends(j)
        a.wait_recv()
        part[j, nxt, :, 0:hc] = part[j, nxt, :, 0:hc] + r1l[j]
        b.wait_recv()
        part[j, prev, :, hc:cw] = part[j, prev, :, hc:cw] + r1r[j]
        for copy in second_sends(j):
            copy.start()
        return carry

    def total(j):
        for copy in second_sends(j):
            copy.wait_recv()
        return part[j, y] + r2l[j] + r2r[j]

    def drain(j, carry):
        for copy in first_sends(j) + second_sends(j):
            copy.wait_send()
        return carry

    attended = o_in[...]
    wo_load.wait()

    def out_chunk(j, carry):
        part[j] = jnp.dot(attended, wdv[0:wo_rows, lanes(j * cw, cw)], preferred_element_type=F32).reshape(RING, block_rows, cw)
        for copy in first_sends(j):
            copy.start()
        return carry

    lax.fori_loop(0, nc, out_chunk, 0)
    wd_late.start()
    lax.fori_loop(0, nc, relay, 0)

    def h_piece(c, p, j):
        return hbuf.at[c, p, :, lanes(j * cw, cw)]

    def h_half(c, p, j, i):
        return hbuf.at[c, p, :, lanes(j * cw + i * hc, hc)]

    def h_steps(j):
        return (remote(h_piece(core, y, j), h_piece(core, y, j), hs.at[0, j], hr.at[0, j], up),
                remote(h_piece(core, y, j), h_piece(core, y, j), hs.at[1, j], hr.at[1, j], down),
                remote(h_half(core, prev, j, 0), h_half(core, prev, j, 0), hs.at[2, j], hr.at[2, j], up),
                remote(h_half(core, nxt, j, 1), h_half(core, nxt, j, 1), hs.at[3, j], hr.at[3, j], down))

    def h_give(j, i, p, c):
        return remote(h_piece(c, p, j), h_piece(c, p, j), ps.at[i, j], pr.at[i, j], partner)

    def mid_chunk(j, carry):
        c = lanes(j * cw, cw)
        mid = (xres[:, c].astype(F32) + total(j)).astype(BF16)
        hres[:, c] = mid
        hbuf[core, y, :, c] = mid
        for copy in h_steps(j)[:2] + (h_give(j, 0, y, core),):
            copy.start()
        return carry

    lax.fori_loop(0, nc, mid_chunk, 0)

    def h_forward(j, carry):
        steps = h_steps(j)
        remote(h_piece(core, prev, j), h_piece(core, prev, j), hs.at[0, j], hr.at[0, j], down).wait_recv()
        steps[2].start()
        h_give(j, 1, prev, core).start()
        remote(h_piece(core, nxt, j), h_piece(core, nxt, j), hs.at[1, j], hr.at[1, j], up).wait_recv()
        steps[3].start()
        h_give(j, 2, nxt, core).start()
        return carry

    lax.fori_loop(0, nc, h_forward, 0)

    def h_last(j, carry):
        remote(h_half(core, far, j, 0), h_half(core, far, j, 0), hs.at[2, j], hr.at[2, j], down).wait_recv()
        remote(h_half(core, far, j, 1), h_half(core, far, j, 1), hs.at[3, j], hr.at[3, j], up).wait_recv()
        h_give(j, 3, far, core).start()
        return carry

    lax.fori_loop(0, nc, h_last, 0)

    def h_end(j, carry):
        for i, p in enumerate((y, prev, nxt, far)):
            h_give(j, i, p, 1 - core).wait_recv()
        for copy in h_steps(j):
            copy.wait_send()
        for i, p in enumerate((y, prev, nxt, far)):
            h_give(j, i, p, core).wait_send()
        return carry

    lax.fori_loop(0, nc, h_end, 0)
    lax.fori_loop(0, nc, drain, 0)

    def norm_block(i, carry):
        v0, v1 = hbuf[0, i].astype(F32), hbuf[1, i].astype(F32)
        mean = (jnp.sum(v0 * v0, axis=-1, keepdims=True) + jnp.sum(v1 * v1, axis=-1, keepdims=True)) / width
        inv = lax.rsqrt(mean + NORM_EPS)
        hbuf[0, i] = (v0 * inv * gain[0:1, :].astype(F32)).astype(BF16)
        hbuf[1, i] = (v1 * inv * gain[1:2, :].astype(F32)).astype(BF16)
        return carry

    lax.fori_loop(0, RING, norm_block, 0)
    b0, b1 = hbuf[0].reshape(rows, half_w), hbuf[1].reshape(rows, half_w)

    def u_copy(j, c):
        at = ubuf.at[:, lanes(c * half_f + j * uw, uw)]
        return remote(at, at, us.at[j], ur.at[j], partner)

    def up_chunk(j, carry):
        c = lanes(j * uw, uw)
        gate = jnp.dot(b0, wgv[0:half_w, c], preferred_element_type=F32) + jnp.dot(b1, wgv[half_w:width, c], preferred_element_type=F32)
        upper = jnp.dot(b0, wuv[0:half_w, c], preferred_element_type=F32) + jnp.dot(b1, wuv[half_w:width, c], preferred_element_type=F32)
        ubuf[:, lanes(core * half_f + j * uw, uw)] = (jax.nn.silu(gate) * upper).astype(BF16)
        u_copy(j, core).start()
        return carry

    wg_load.wait()
    wu_load.wait()
    lax.fori_loop(0, nu, up_chunk, 0)
    wd_load.wait()
    wd_late.wait()
    for j in range(nu):
        u_copy(j, 1 - core).wait_recv()

    def down_chunk(j, carry):
        part[j] = jnp.dot(ubuf[...], wdv[:, lanes(j * cw, cw)], preferred_element_type=F32).reshape(RING, block_rows, cw)
        for copy in first_sends(j):
            copy.start()
        return carry

    lax.fori_loop(0, nc, down_chunk, 0)
    lax.fori_loop(0, nc, relay, 0)

    def last_chunk(j, carry):
        c = lanes(j * cw, cw)
        fin[:, :, c] = (hres[:, c].astype(F32) + total(j)).astype(BF16).reshape(2, block_rows // 2, cw)
        return carry

    lax.fori_loop(0, nc, last_chunk, 0)
    swap = remote(fin.at[1 - core], fbuf.at[core], fs.at[0], fr.at[0], partner)
    swap.start()
    own = fin[core]
    out[:, lanes(col0, half_w)] = own
    remote(fin.at[core], fbuf.at[1 - core], fs.at[0], fr.at[0], partner).wait_recv()
    out[:, lanes((1 - core) * half_w, half_w)] = fbuf[1 - core]
    for j in range(nu):
        u_copy(j, core).wait_send()
    lax.fori_loop(0, nc, drain, 0)
    swap.wait_send()


def dma(*shape):
    return pltpu.SemaphoreType.DMA(shape)


def relative_positions(r, shards):
    x, y, core, w = r >> 7, (r >> 5) & 3, (r >> 4) & 1, r & 15
    k = (2 * x + core) * RING + y
    run = jnp.where(w < 8, k, 2 * shards - 1 - k)
    return run * 8 + (w & 7)


def solution(mesh):
    token_spec = P(('dp', 'cp', 'tp'), None)
    column_spec = P(None, 'tp')
    row_spec = P('tp', None)
    shards = mesh.shape['tp'] * mesh.shape['cp']

    def device_layer(hidden_loc, pos_loc, cache_len, cache_k, cache_v, norm1_gain, w_query, w_key, w_value, w_out, norm2_gain, w_gate, w_up, w_down):
        shard_rows, width = hidden_loc.shape
        half_w = width // 2
        chip_rows = 2 * RING * shard_rows
        rows = RING * chip_rows
        slots = cache_k.shape[0]
        head_w = w_query.shape[1] // 2
        heads = head_w // HEAD_DIM
        half = HEAD_DIM // 2
        cp, y = lax.axis_index('cp'), lax.axis_index('tp')
        ring_row = jnp.where(cp % 2 == 0, cp // 2, y)
        relk = relative_positions(ring_row * chip_rows + lax.broadcasted_iota(jnp.int32, (chip_rows, 1), 0), shards)
        relq = relative_positions(lax.broadcasted_iota(jnp.int32, (1, rows), 1), shards)
        lane = jnp.arange(HEAD_DIM, dtype=jnp.int32)
        rel = relative_positions((lax.axis_index('cp') // 2) * chip_rows + jnp.arange(chip_rows, dtype=jnp.int32), shards)
        inv_freq = 1.0 / (ROPE_BASE ** ((lane % half).astype(F32) * (2.0 / HEAD_DIM)))
        angles = (cache_len[0] + rel).astype(F32)[:, None] * inv_freq[None, :]
        cos, sin = jnp.cos(angles), jnp.sin(angles) * jnp.where(lane < half, -1.0, 1.0)[None, :]
        block = (heads, HEAD_DIM + 8, chip_rows)
        part_block = (heads // 2,) + block[1:]
        attended, xres = pl.pallas_call(
            attention_kernel,
            out_shape=(jax.ShapeDtypeStruct((chip_rows, 2 * head_w), BF16), jax.ShapeDtypeStruct((2 * shard_rows, half_w), BF16)),
            in_specs=[ANY, SMEM, ANY, ANY, VMEM, ANY, ANY, ANY, VMEM, VMEM, VMEM, VMEM],
            out_specs=(VMEM, VMEM),
            scratch_shapes=[
                pltpu.VMEM((RING, 2, shard_rows, width), BF16),
                pltpu.VMEM((RING, 2 * shard_rows, width), BF16),
                pltpu.VMEM((width, head_w), BF16),
                pltpu.VMEM((width, HEAD_DIM), BF16),
                pltpu.VMEM((width, HEAD_DIM), BF16),
                pltpu.VMEM((2 * RING, slots, HEAD_DIM), BF16),
                pltpu.VMEM((2 * RING, slots, HEAD_DIM), BF16),
                pltpu.VMEM((2, slots, HEAD_DIM), BF16),
                pltpu.VMEM((2, slots, HEAD_DIM), BF16),
                pltpu.VMEM((slots, 2 * HEAD_DIM), BF16),
                pltpu.VMEM((HEAD_DIM, slots), BF16),
                pltpu.VMEM((chip_rows, head_w + 2 * HEAD_DIM), BF16),
                pltpu.VMEM((rows, head_w + 2 * HEAD_DIM), BF16),
                pltpu.VMEM((heads, rows, 2 * HEAD_DIM), BF16),
                pltpu.VMEM((slots, 256), F32),
                pltpu.VMEM((slots, 256), F32),
                pltpu.VMEM((heads, HEAD_DIM + 8, rows), F32),
                pltpu.VMEM(part_block, F32),
                pltpu.VMEM(part_block, F32),
                pltpu.VMEM(block, F32),
                pltpu.VMEM(block, F32),
                pltpu.VMEM((chip_rows, head_w), BF16),
                pltpu.VMEM((2, chip_rows, head_w), BF16),
                dma(4), dma(4), dma(4), dma(4), dma(4), dma(18), dma(2 * RING, 2), dma(2, 2), dma(1), dma(1),
                dma(4), dma(4), dma(4), dma(4), dma(2), dma(2),
            ],
            compiler_params=pltpu.CompilerParams(collective_id=0, has_side_effects=True, vmem_limit_bytes=67043328),
            name='attention',
        )(hidden_loc, cache_len, cache_k, cache_v, norm1_gain.reshape(1, width), w_query, w_key, w_value, cos, sin, relq, relk)

        cw = 512 if half_w % 512 == 0 and half_w > 512 else 256
        nc = half_w // cw
        half_f = w_gate.shape[1] // 2
        nu = half_f // 256
        br = 2 * shard_rows
        return pl.pallas_call(
            mlp_kernel,
            out_shape=jax.ShapeDtypeStruct((shard_rows, width), BF16),
            in_specs=[VMEM, VMEM, VMEM, ANY, ANY, ANY, ANY],
            out_specs=VMEM,
            scratch_shapes=[
                pltpu.VMEM((width, half_f), BF16),
                pltpu.VMEM((width, half_f), BF16),
                pltpu.VMEM((2 * half_f, half_w), BF16),
                pltpu.VMEM((nc, RING, br, cw), F32),
                pltpu.VMEM((nc, br, cw // 2), F32),
                pltpu.VMEM((nc, br, cw // 2), F32),
                pltpu.VMEM((nc, br, cw), F32),
                pltpu.VMEM((nc, br, cw), F32),
                pltpu.VMEM((2, RING, br, half_w), BF16),
                pltpu.VMEM((br, half_w), BF16),
                pltpu.VMEM((chip_rows, 2 * half_f), BF16),
                pltpu.VMEM((2, shard_rows, half_w), BF16),
                pltpu.VMEM((2, shard_rows, half_w), BF16),
                dma(5), dma(2, nc), dma(2, nc), dma(2, nc), dma(2, nc),
                dma(4, nc), dma(4, nc), dma(4, nc), dma(4, nc), dma(nu), dma(nu), dma(1), dma(1),
            ],
            compiler_params=pltpu.CompilerParams(collective_id=1, has_side_effects=True, vmem_limit_bytes=67043328),
            name='mlp',
        )(attended, xres, norm2_gain.reshape(2, half_w), w_out, w_gate, w_up, w_down)

    return jax.shard_map(device_layer, mesh=mesh, in_specs=(token_spec, P(('dp', 'cp', 'tp')), P('dp'), token_spec, token_spec, P(), column_spec, column_spec, column_spec, row_spec, P(), column_spec, column_spec, row_spec), out_specs=token_spec, check_vma=False)
```

```python
import functools
import math
import jax
import jax.numpy as jnp
from jax import lax
from jax.experimental import pallas as pl
from jax.experimental.pallas import tpu as pltpu
from jax.sharding import PartitionSpec as P

HEAD_DIM = 128
ROPE_BASE = 500000.0
NORM_EPS = 1e-5
MESH = pl.DeviceIdType.MESH
F32 = jnp.float32
BF16 = jnp.bfloat16
M_INIT = -1e38
MASKED = -3e38
EXP_SCALE = math.log2(math.e) / math.sqrt(HEAD_DIM)
RING = 4
STEP = 1024
ANY = pl.BlockSpec(memory_space=pl.ANY)
VMEM = pl.BlockSpec(memory_space=pltpu.VMEM)
SMEM = pl.BlockSpec(memory_space=pltpu.SMEM)


class Place:
    def __init__(self):
        self.y = lax.axis_index('tp')
        cp = lax.axis_index('cp')
        self.x = cp // 2
        self.core = cp % 2
        self.vx = self.x + self.core * (self.y - self.x)
        self.vy = self.y + self.core * (self.x - self.y)

    def at(self, dx=0, dy=0, core=None):
        return {'tp': (self.y + dy) % RING, 'cp': ((self.x + dx) % RING) * 2 + (self.core if core is None else core)}

    def mirrored(self, core):
        return {'tp': self.x, 'cp': self.y * 2 + core}


def remote(src, dst, send_sem, recv_sem, device):
    return pltpu.make_async_remote_copy(src_ref=src, dst_ref=dst, send_sem=send_sem, recv_sem=recv_sem, device_id=device, device_id_type=MESH)


def barrier(devices):
    sem = pltpu.get_barrier_semaphore()
    for device in devices:
        pl.semaphore_signal(sem, inc=1, device_id=device, device_id_type=MESH)
    pl.semaphore_wait(sem, len(devices))


def ring_gather(pos, right, left, block, half, sends, recvs, own=None, partner=None, core=None, psends=None, precvs=None, between=None):
    prev, nxt, far = (pos + 3) % RING, (pos + 1) % RING, (pos + 2) % RING
    mine = block(pos, core) if own is None else own
    to_right = remote(mine, block(pos, core), sends.at[0], recvs.at[0], right)
    to_left = remote(mine, block(pos, core), sends.at[1], recvs.at[1], left)
    to_right.start()
    to_left.start()
    copies = [to_right, to_left]
    given = []

    def give(p, i, source=None):
        if partner is not None:
            copy = remote(block(p, core) if source is None else source, block(p, core), psends.at[i], precvs.at[i], partner)
            copy.start()
            given.append(copy)

    give(pos, 0, mine)
    remote(block(prev, core), block(prev, core), sends.at[0], recvs.at[0], left).wait_recv()
    fwd_right = remote(half(prev, core, 0), half(prev, core, 0), sends.at[2], recvs.at[2], right)
    fwd_right.start()
    give(prev, 1)
    remote(block(nxt, core), block(nxt, core), sends.at[1], recvs.at[1], right).wait_recv()
    fwd_left = remote(half(nxt, core, 1), half(nxt, core, 1), sends.at[3], recvs.at[3], left)
    fwd_left.start()
    give(nxt, 2)
    copies += [fwd_right, fwd_left]
    if between is not None:
        between()
    remote(half(far, core, 0), half(far, core, 0), sends.at[2], recvs.at[2], left).wait_recv()
    remote(half(far, core, 1), half(far, core, 1), sends.at[3], recvs.at[3], right).wait_recv()
    give(far, 3)
    if partner is not None:
        for i, p in enumerate((pos, prev, nxt, far)):
            remote(block(p, 1 - core), block(p, 1 - core), psends.at[i], precvs.at[i], partner).wait_recv()
    return copies + given


def attention_kernel(shards, x_in, len_ref, ck, cv, gain, wq, wk, wv, cos_ref, sin_ref, o_out, xres_out,
                     xbuf, ckv, cvv, abuf, wqv, wkv, wvv, kbuf, vbuf, rk, rv, kaug, vt, qkv, qall, qaug, sa, sb, acc, r1l, r1r, r2l, r2r, otmp, obuf,
                     lsem, xs, xr, ps, pr, kvs, kvr, relay_r, ts, tr, qs, qr, rs, rr, os, orr):
    me = Place()
    x, y, core, vx, vy = me.x, me.y, me.core, me.vx, me.vy
    width = x_in.shape[1]
    half_w = width // 2
    slots = ck.shape[0]
    rows = qall.shape[0]
    chip_rows = rows // RING
    heads = acc.shape[0]
    head_w = heads * HEAD_DIM
    partner = me.at(core=1 - core)
    up, down = me.at(dy=1), me.at(dy=RING - 1)
    right, left = me.at(dx=1 - core, dy=core), me.at(dx=(1 - core) * (RING - 1), dy=core * (RING - 1))
    ahead, behind = me.at(dx=core, dy=1 - core), me.at(dx=core * (RING - 1), dy=(1 - core) * (RING - 1))
    moving = jnp.logical_and(core == 1, x != y)

    local = [
        pltpu.make_async_copy(x_in, xbuf.at[y, core], lsem.at[0]),
        pltpu.make_async_copy(ck, ckv, lsem.at[4]),
        pltpu.make_async_copy(cv, cvv, lsem.at[5]),
        pltpu.make_async_copy(wq.at[:, pl.ds(pl.multiple_of(core * head_w, head_w), head_w)], wqv, lsem.at[1]),
        pltpu.make_async_copy(wk.at[:, pl.ds(pl.multiple_of(core * HEAD_DIM, HEAD_DIM), HEAD_DIM)], wkv, lsem.at[2]),
        pltpu.make_async_copy(wv.at[:, pl.ds(pl.multiple_of(core * HEAD_DIM, HEAD_DIM), HEAD_DIM)], wvv, lsem.at[3]),
    ]
    local[0].start()
    for copy in local[1:]:
        copy.start()

    peers = [partner, me.mirrored(0), me.mirrored(1)]
    peers += [me.at(dy=d, core=c) for d in range(1, RING) for c in range(2)] + [me.at(dx=d, core=c) for d in range(1, RING) for c in range(2)]
    barrier(peers)

    def kv_lanes(head):
        return pl.ds(pl.multiple_of(head * HEAD_DIM, HEAD_DIM), HEAD_DIM)

    def target(role, d):
        return me.at(dx=d if role else 0, dy=0 if role else d, core=role)

    def target_lanes(role, d):
        return kv_lanes(2 * (((x if role else y) + d) % RING) + role)

    kv_copies = []

    def kv_send(src, dst, recv, device):
        copy = remote(src, dst, kvs.at[len(kv_copies)], recv, device)
        copy.start()
        kv_copies.append(copy)

    def send_near():
        local[1].wait()
        local[2].wait()
        other_vy = x + y - vy
        for i, (src, dst) in enumerate(((ck, kbuf), (cv, vbuf))):
            pltpu.make_async_copy(src.at[:, kv_lanes(2 * vy + core)], dst.at[core], kvr.at[core, i]).start()
            kv_send((ckv, cvv)[i].at[:, kv_lanes(2 * other_vy + 1 - core)], dst.at[core], kvr.at[core, i], partner)
        for role in range(2):
            kv_send(ckv.at[:, target_lanes(role, 2)], rk.at[core], relay_r.at[0, core], target(role, 1))
            kv_send(cvv.at[:, target_lanes(role, 2)], rv.at[core], relay_r.at[1, core], target(role, RING - 1))

    def send_far():
        for i, (src, dst) in enumerate(((ckv, kbuf), (cvv, vbuf))):
            for role in range(2):
                for d, slot in ((1, 2), (3, 4)):
                    kv_send(src.at[:, target_lanes(role, d)], dst.at[slot + core], kvr.at[slot + core, i], target(role, d))
        for c in range(2):
            remote(rk.at[c], rk.at[c], kvs.at[0], relay_r.at[0, c], behind).wait_recv()
            kv_send(rk.at[c], kbuf.at[6 + c], kvr.at[6 + c, 0], ahead)
            remote(rv.at[c], rv.at[c], kvs.at[0], relay_r.at[1, c], ahead).wait_recv()
            kv_send(rv.at[c], vbuf.at[6 + c], kvr.at[6 + c, 1], behind)

    x_copies = ring_gather(
        y, up, down, lambda p, c: xbuf.at[p, c], lambda p, c, i: xbuf.at[p, c, :, pl.ds(i * half_w, half_w)],
        xs, xr, own=x_in, partner=partner, core=core, psends=ps, precvs=pr, between=send_near)
    local[0].wait()

    def norm_block(i, carry):
        values = xbuf[i].reshape(2 * xbuf.shape[2], width).astype(F32)
        inv = lax.rsqrt(jnp.mean(values * values, axis=-1, keepdims=True) + NORM_EPS)
        abuf[i] = (values * inv * gain[...].reshape(1, width).astype(F32)).astype(BF16)
        return carry

    lax.fori_loop(0, RING, norm_block, 0)
    xres_out[...] = xbuf[y, :, :, pl.ds(pl.multiple_of(core * half_w, half_w), half_w)].reshape(xres_out.shape)

    for copy in local[3:]:
        copy.wait()
    normed = abuf[...].reshape(chip_rows, width)
    cos, sin = cos_ref[...], sin_ref[...]

    def rotate(v):
        return (v * cos + pltpu.roll(v, HEAD_DIM // 2, 1) * sin).astype(BF16)

    q = jnp.dot(normed, wqv[...], preferred_element_type=F32)
    for h in range(heads):
        qkv[:, h * HEAD_DIM:(h + 1) * HEAD_DIM] = rotate(q[:, h * HEAD_DIM:(h + 1) * HEAD_DIM])
    qkv[:, head_w:head_w + HEAD_DIM] = rotate(jnp.dot(normed, wkv[...], preferred_element_type=F32))
    qkv[:, head_w + HEAD_DIM:] = jnp.dot(normed, wvv[...], preferred_element_type=F32).astype(BF16)

    def q_rows(p):
        return pl.ds(pl.multiple_of(p * chip_rows, chip_rows), chip_rows)

    across_in = remote(qkv, qall.at[q_rows(vx)], ts.at[0], tr.at[0], me.mirrored(core))
    mirror_send = remote(qkv, qall.at[q_rows(x)], ts.at[0], tr.at[0], me.mirrored(core))

    @pl.when(moving)
    def _():
        mirror_send.start()
        across_in.wait_recv()

    @pl.when(jnp.logical_not(moving))
    def _():
        qall[q_rows(vx), :] = qkv[...]

    q_copies = ring_gather(
        vx, right, left, lambda p, c: qall.at[q_rows(p), pl.ds(0, head_w)],
        lambda p, c, i: qall.at[q_rows(p), pl.ds(i * (head_w // 2), head_w // 2)], qs, qr, between=send_far)

    first_lane = jnp.where(lax.broadcasted_iota(jnp.int32, (rows, HEAD_DIM), 1) == 0, 1.0, 0.0).astype(BF16)
    for h in range(heads):
        qaug[h, :, 0:HEAD_DIM] = qall[:, h * HEAD_DIM:(h + 1) * HEAD_DIM]
        qaug[h, :, HEAD_DIM:] = first_lane

    tile = 256
    tiles = rows // tile
    contract_last = (((1,), (1,)), ((), ()))

    def finish(s_ref, e_top, vt_ref, h, j, first, depth):
        lanes = pl.ds(j * tile, tile)
        if first:
            m_new = jnp.maximum(e_top, M_INIT)
        else:
            m_old = acc[h, HEAD_DIM:HEAD_DIM + 1, lanes]
            l_old = acc[h, HEAD_DIM + 1:HEAD_DIM + 2, lanes]
            m_new = jnp.maximum(e_top, m_old)
        m_scaled = m_new * EXP_SCALE
        part_l, o = None, None
        step = min(STEP, depth)
        for k in range(0, depth, step):
            e = jnp.exp2(s_ref[k:k + step, :] * EXP_SCALE - m_scaled)
            total_e = jnp.sum(e.reshape(step // 8, 8, tile), axis=0)
            part_l = total_e if part_l is None else part_l + total_e
            term = jnp.dot(vt_ref[:, k:k + step], e.astype(BF16), preferred_element_type=F32)
            o = term if o is None else o + term
        l_new = jnp.sum(part_l, axis=0, keepdims=True)
        if not first:
            alpha = jnp.exp2((m_old - m_new) * EXP_SCALE)
            l_new = l_new + l_old * alpha
            o = o + acc[h, 0:HEAD_DIM, lanes] * alpha
        acc[h, 0:HEAD_DIM, lanes] = o
        acc[h, HEAD_DIM:HEAD_DIM + 1, lanes] = m_new
        acc[h, HEAD_DIM + 1:HEAD_DIM + 2, lanes] = l_new

    my_rows = q_rows(vx)
    vnew_t = qall[my_rows, head_w + HEAD_DIM:].T
    knew = qall[my_rows, head_w:head_w + HEAD_DIM]

    def new_head(h, carry):
        for j in range(tiles):
            s = lax.dot_general(knew, qaug[h, j * tile:(j + 1) * tile, 0:HEAD_DIM], contract_last, preferred_element_type=F32)
            relk = relative_positions(vx * chip_rows + lax.broadcasted_iota(jnp.int32, s.shape, 0), shards)
            relq = relative_positions(j * tile + lax.broadcasted_iota(jnp.int32, s.shape, 1), shards)
            causal = relk <= relq
            s = jnp.where(causal, s, -jnp.inf)
            finish(s, jnp.max(s, axis=0, keepdims=True), vnew_t, h, j, True, chip_rows)
        return carry

    lax.fori_loop(0, heads, new_head, 0)
    cache_len = len_ref[0]
    slot_ids = lax.broadcasted_iota(jnp.int32, (slots, HEAD_DIM), 0)

    def scores(h, j, dst):
        s = lax.dot_general(kaug[...], qaug[h, j * tile:(j + 1) * tile, :], contract_last, preferred_element_type=F32)
        dst[...] = s
        return jnp.max(s, axis=0, keepdims=True)

    def source(s, carry):
        u, src_core = s // 2, s % 2
        d = u + (u // 2) * (1 - 2 * (u % 2))
        src_x = (x - core * d + RING) % RING
        src_y = (y - (1 - core) * d + RING) % RING
        base = ((2 * src_x + src_core) * RING + src_y) * slots
        for i, (src, dst) in enumerate(((ckv, kbuf), (cvv, vbuf))):
            pltpu.make_async_copy(src.at[:, pl.ds(0, HEAD_DIM)], dst.at[s], kvr.at[s, i]).wait()
        vt[...] = vbuf[s].T
        seen = slot_ids < cache_len - base
        kaug[:, 0:HEAD_DIM] = jnp.where(seen, kbuf[s].astype(F32), 0.0).astype(BF16)
        kaug[:, HEAD_DIM:] = jnp.where(seen, 0.0, MASKED).astype(BF16)

        top_a = scores(0, 0, sa)
        for h in range(heads):
            top_b = scores(h, 1, sb)
            finish(sa, top_a, vt, h, 0, False, slots)
            if h + 1 < heads:
                top_a = scores(h + 1, 0, sa)
            finish(sb, top_b, vt, h, 1, False, slots)
        return carry

    lax.fori_loop(0, 2 * RING, source, 0)

    hh = heads // 2
    far, nxt, prev = (vx + 2) % RING, (vx + 1) % RING, (vx + 3) % RING
    p1 = [remote(acc.at[pl.ds(0, hh), :, q_rows(far)], r1l, rs.at[0], rr.at[0], right),
          remote(acc.at[pl.ds(hh, hh), :, q_rows(far)], r1r, rs.at[1], rr.at[1], left)]
    for copy in p1:
        copy.start()

    def merge(a, b):
        ma, mb = a[:, HEAD_DIM:HEAD_DIM + 1, :], b[:, HEAD_DIM:HEAD_DIM + 1, :]
        m = jnp.maximum(ma, mb)
        wa, wb = jnp.exp2((ma - m) * EXP_SCALE), jnp.exp2((mb - m) * EXP_SCALE)
        o = a[:, 0:HEAD_DIM, :] * wa + b[:, 0:HEAD_DIM, :] * wb
        l = a[:, HEAD_DIM + 1:HEAD_DIM + 2, :] * wa + b[:, HEAD_DIM + 1:HEAD_DIM + 2, :] * wb
        return o, m, l

    def merge_into(lo, p, other):
        o, m, l = merge(acc[lo:lo + hh, :, q_rows(p)], other[...])
        acc[lo:lo + hh, 0:HEAD_DIM, q_rows(p)] = o
        acc[lo:lo + hh, HEAD_DIM:HEAD_DIM + 1, q_rows(p)] = m
        acc[lo:lo + hh, HEAD_DIM + 1:HEAD_DIM + 2, q_rows(p)] = l

    p2 = [remote(acc.at[:, :, q_rows(nxt)], r2l, rs.at[2], rr.at[2], right),
          remote(acc.at[:, :, q_rows(prev)], r2r, rs.at[3], rr.at[3], left)]
    p1[0].wait_recv()
    merge_into(0, nxt, r1l)
    p2[0].start()
    p1[1].wait_recv()
    merge_into(hh, prev, r1r)
    p2[1].start()
    for copy in p2:
        copy.wait_recv()
    for h in range(heads):
        a, b, d = acc[h:h + 1, :, q_rows(vx)], r2l[h:h + 1], r2r[h:h + 1]
        o, m, l = merge(a, b)
        md = d[:, HEAD_DIM:HEAD_DIM + 1, :]
        top = jnp.maximum(m, md)
        w, wd = jnp.exp2((m - top) * EXP_SCALE), jnp.exp2((md - top) * EXP_SCALE)
        o = o * w + d[:, 0:HEAD_DIM, :] * wd
        l = l * w + d[:, HEAD_DIM + 1:HEAD_DIM + 2, :] * wd
        otmp[:, h * HEAD_DIM:(h + 1) * HEAD_DIM] = (o / l)[0].T.astype(BF16)

    other_at = {'tp': vy, 'cp': vx * 2 + 1 - core}
    other_out = remote(otmp, obuf.at[core], os.at[1], orr.at[1], other_at)
    other_out.start()
    same_out = remote(otmp, obuf.at[core], os.at[0], orr.at[0], me.mirrored(core))

    @pl.when(moving)
    def _():
        same_out.start()
        same_out.wait_recv()

    @pl.when(jnp.logical_not(moving))
    def _():
        obuf[core] = otmp[...]

    remote(otmp, obuf.at[1 - core], os.at[1], orr.at[1], partner).wait_recv()
    o_out[:, 0:head_w] = obuf[0]
    o_out[:, head_w:2 * head_w] = obuf[1]
    for copy in x_copies + kv_copies + q_copies + p1 + p2 + [other_out]:
        copy.wait_send()

    @pl.when(moving)
    def _():
        mirror_send.wait_send()
        same_out.wait_send()


def mlp_kernel(o_in, xres, gain, wo, wg, wu, wd, out,
               wgv, wuv, wdv, part, r1l, r1r, r2l, r2r, hbuf, hres, ubuf, fin, fbuf,
               wsem, s1, q1, s2, q2, hs, hr, ps, pr, us, ur, fs, fr):
    me = Place()
    y, core = me.y, me.core
    nc, _, _, cw = part.shape
    half_w = nc * cw
    width = 2 * half_w
    rows = o_in.shape[0]
    block_rows = rows // RING
    half_f = wgv.shape[1]
    uw = 256
    nu = half_f // uw
    partner = me.at(core=1 - core)
    up, down = me.at(dy=1), me.at(dy=RING - 1)
    far, nxt, prev = (y + 2) % RING, (y + 1) % RING, (y + 3) % RING
    col0 = core * half_w

    def lanes(start, size):
        return pl.ds(pl.multiple_of(start, 128), size)

    wo_rows, wd_rows = wo.shape[0], wd.shape[0]
    up_cols, out_cols = lanes(core * half_f, half_f), lanes(col0, half_w)
    wo_load = pltpu.make_async_copy(wo.at[:, out_cols], wdv.at[pl.ds(0, wo_rows), :], wsem.at[0])
    wd_load = pltpu.make_async_copy(wd.at[pl.ds(wo_rows, wd_rows - wo_rows), out_cols], wdv.at[pl.ds(wo_rows, wd_rows - wo_rows), :], wsem.at[1])
    wd_late = pltpu.make_async_copy(wd.at[pl.ds(0, wo_rows), out_cols], wdv.at[pl.ds(0, wo_rows), :], wsem.at[2])
    wg_load = pltpu.make_async_copy(wg.at[:, up_cols], wgv, wsem.at[3])
    wu_load = pltpu.make_async_copy(wu.at[:, up_cols], wuv, wsem.at[4])
    for copy in (wo_load, wg_load, wu_load, wd_load):
        copy.start()

    barrier([up, down, partner])

    hc = cw // 2

    def first_sends(j):
        return (remote(part.at[j, far, :, pl.ds(0, hc)], r1l.at[j], s1.at[0, j], q1.at[0, j], up),
                remote(part.at[j, far, :, pl.ds(hc, hc)], r1r.at[j], s1.at[1, j], q1.at[1, j], down))

    def second_sends(j):
        return (remote(part.at[j, nxt], r2l.at[j], s2.at[0, j], q2.at[0, j], up),
                remote(part.at[j, prev], r2r.at[j], s2.at[1, j], q2.at[1, j], down))

    def relay(j, carry):
        a, b = first_sends(j)
        a.wait_recv()
        part[j, nxt, :, 0:hc] = part[j, nxt, :, 0:hc] + r1l[j]
        b.wait_recv()
        part[j, prev, :, hc:cw] = part[j, prev, :, hc:cw] + r1r[j]
        for copy in second_sends(j):
            copy.start()
        return carry

    def total(j):
        for copy in second_sends(j):
            copy.wait_recv()
        return part[j, y] + r2l[j] + r2r[j]

    def drain(j, carry):
        for copy in first_sends(j) + second_sends(j):
            copy.wait_send()
        return carry

    attended = o_in[...]
    wo_load.wait()

    def out_chunk(j, carry):
        part[j] = jnp.dot(attended, wdv[0:wo_rows, lanes(j * cw, cw)], preferred_element_type=F32).reshape(RING, block_rows, cw)
        for copy in first_sends(j):
            copy.start()
        return carry

    lax.fori_loop(0, nc, out_chunk, 0)
    wd_late.start()
    lax.fori_loop(0, nc, relay, 0)

    def h_piece(c, p, j):
        return hbuf.at[c, p, :, lanes(j * cw, cw)]

    def h_half(c, p, j, i):
        return hbuf.at[c, p, :, lanes(j * cw + i * hc, hc)]

    def h_steps(j):
        return (remote(h_piece(core, y, j), h_piece(core, y, j), hs.at[0, j], hr.at[0, j], up),
                remote(h_piece(core, y, j), h_piece(core, y, j), hs.at[1, j], hr.at[1, j], down),
                remote(h_half(core, prev, j, 0), h_half(core, prev, j, 0), hs.at[2, j], hr.at[2, j], up),
                remote(h_half(core, nxt, j, 1), h_half(core, nxt, j, 1), hs.at[3, j], hr.at[3, j], down))

    def h_give(j, i, p, c):
        return remote(h_piece(c, p, j), h_piece(c, p, j), ps.at[i, j], pr.at[i, j], partner)

    def mid_chunk(j, carry):
        c = lanes(j * cw, cw)
        mid = (xres[:, c].astype(F32) + total(j)).astype(BF16)
        hres[:, c] = mid
        hbuf[core, y, :, c] = mid
        for copy in h_steps(j)[:2] + (h_give(j, 0, y, core),):
            copy.start()
        return carry

    lax.fori_loop(0, nc, mid_chunk, 0)

    def h_forward(j, carry):
        steps = h_steps(j)
        remote(h_piece(core, prev, j), h_piece(core, prev, j), hs.at[0, j], hr.at[0, j], down).wait_recv()
        steps[2].start()
        h_give(j, 1, prev, core).start()
        remote(h_piece(core, nxt, j), h_piece(core, nxt, j), hs.at[1, j], hr.at[1, j], up).wait_recv()
        steps[3].start()
        h_give(j, 2, nxt, core).start()
        return carry

    lax.fori_loop(0, nc, h_forward, 0)

    def h_last(j, carry):
        remote(h_half(core, far, j, 0), h_half(core, far, j, 0), hs.at[2, j], hr.at[2, j], down).wait_recv()
        remote(h_half(core, far, j, 1), h_half(core, far, j, 1), hs.at[3, j], hr.at[3, j], up).wait_recv()
        h_give(j, 3, far, core).start()
        return carry

    lax.fori_loop(0, nc, h_last, 0)

    def h_end(j, carry):
        for i, p in enumerate((y, prev, nxt, far)):
            h_give(j, i, p, 1 - core).wait_recv()
        for copy in h_steps(j):
            copy.wait_send()
        for i, p in enumerate((y, prev, nxt, far)):
            h_give(j, i, p, core).wait_send()
        return carry

    lax.fori_loop(0, nc, h_end, 0)
    lax.fori_loop(0, nc, drain, 0)

    def norm_block(i, carry):
        v0, v1 = hbuf[0, i].astype(F32), hbuf[1, i].astype(F32)
        mean = (jnp.sum(v0 * v0, axis=-1, keepdims=True) + jnp.sum(v1 * v1, axis=-1, keepdims=True)) / width
        inv = lax.rsqrt(mean + NORM_EPS)
        hbuf[0, i] = (v0 * inv * gain[0:half_w].reshape(1, half_w).astype(F32)).astype(BF16)
        hbuf[1, i] = (v1 * inv * gain[half_w:width].reshape(1, half_w).astype(F32)).astype(BF16)
        return carry

    lax.fori_loop(0, RING, norm_block, 0)
    b0, b1 = hbuf[0].reshape(rows, half_w), hbuf[1].reshape(rows, half_w)

    def u_copy(j, c):
        at = ubuf.at[:, lanes(c * half_f + j * uw, uw)]
        return remote(at, at, us.at[j], ur.at[j], partner)

    def up_chunk(j, carry):
        c = lanes(j * uw, uw)
        gate = jnp.dot(b0, wgv[0:half_w, c], preferred_element_type=F32) + jnp.dot(b1, wgv[half_w:width, c], preferred_element_type=F32)
        upper = jnp.dot(b0, wuv[0:half_w, c], preferred_element_type=F32) + jnp.dot(b1, wuv[half_w:width, c], preferred_element_type=F32)
        ubuf[:, lanes(core * half_f + j * uw, uw)] = (jax.nn.silu(gate) * upper).astype(BF16)
        u_copy(j, core).start()
        return carry

    wg_load.wait()
    wu_load.wait()
    lax.fori_loop(0, nu, up_chunk, 0)
    wd_load.wait()
    wd_late.wait()
    for j in range(nu):
        u_copy(j, 1 - core).wait_recv()

    def down_chunk(j, carry):
        part[j] = jnp.dot(ubuf[...], wdv[:, lanes(j * cw, cw)], preferred_element_type=F32).reshape(RING, block_rows, cw)
        for copy in first_sends(j):
            copy.start()
        return carry

    lax.fori_loop(0, nc, down_chunk, 0)
    lax.fori_loop(0, nc, relay, 0)

    def last_chunk(j, carry):
        c = lanes(j * cw, cw)
        fin[:, :, c] = (hres[:, c].astype(F32) + total(j)).astype(BF16).reshape(2, block_rows // 2, cw)
        return carry

    lax.fori_loop(0, nc, last_chunk, 0)
    swap = remote(fin.at[1 - core], fbuf.at[core], fs.at[0], fr.at[0], partner)
    swap.start()
    own = fin[core]
    out[:, lanes(col0, half_w)] = own
    remote(fin.at[core], fbuf.at[1 - core], fs.at[0], fr.at[0], partner).wait_recv()
    out[:, lanes((1 - core) * half_w, half_w)] = fbuf[1 - core]
    for j in range(nu):
        u_copy(j, core).wait_send()
    lax.fori_loop(0, nc, drain, 0)
    swap.wait_send()


def dma(*shape):
    return pltpu.SemaphoreType.DMA(shape)


def relative_positions(r, shards):
    x, y, core, w = r >> 7, (r >> 5) & 3, (r >> 4) & 1, r & 15
    k = (2 * x + core) * RING + y
    run = jnp.where(w < 8, k, 2 * shards - 1 - k)
    return run * 8 + (w & 7)


def solution(mesh):
    token_spec = P(('dp', 'cp', 'tp'), None)
    column_spec = P(None, 'tp')
    row_spec = P('tp', None)
    shards = mesh.shape['tp'] * mesh.shape['cp']

    def device_layer(hidden_loc, pos_loc, cache_len, cache_k, cache_v, norm1_gain, w_query, w_key, w_value, w_out, norm2_gain, w_gate, w_up, w_down):
        shard_rows, width = hidden_loc.shape
        half_w = width // 2
        chip_rows = 2 * RING * shard_rows
        rows = RING * chip_rows
        slots = cache_k.shape[0]
        head_w = w_query.shape[1] // 2
        heads = head_w // HEAD_DIM
        half = HEAD_DIM // 2
        lane = jnp.arange(HEAD_DIM, dtype=jnp.int32)
        rel = relative_positions((lax.axis_index('cp') // 2) * chip_rows + jnp.arange(chip_rows, dtype=jnp.int32), shards)
        inv_freq = 1.0 / (ROPE_BASE ** ((lane % half).astype(F32) * (2.0 / HEAD_DIM)))
        angles = (cache_len[0] + rel).astype(F32)[:, None] * inv_freq[None, :]
        cos, sin = jnp.cos(angles), jnp.sin(angles) * jnp.where(lane < half, -1.0, 1.0)[None, :]
        block = (heads, HEAD_DIM + 8, chip_rows)
        part_block = (heads // 2,) + block[1:]
        attended, xres = pl.pallas_call(
            functools.partial(attention_kernel, shards),
            out_shape=(jax.ShapeDtypeStruct((chip_rows, 2 * head_w), BF16), jax.ShapeDtypeStruct((2 * shard_rows, half_w), BF16)),
            in_specs=[ANY, SMEM, ANY, ANY, VMEM, ANY, ANY, ANY, VMEM, VMEM],
            out_specs=(VMEM, VMEM),
            scratch_shapes=[
                pltpu.VMEM((RING, 2, shard_rows, width), BF16),
                pltpu.VMEM(cache_k.shape, BF16),
                pltpu.VMEM(cache_v.shape, BF16),
                pltpu.VMEM((RING, 2 * shard_rows, width), BF16),
                pltpu.VMEM((width, head_w), BF16),
                pltpu.VMEM((width, HEAD_DIM), BF16),
                pltpu.VMEM((width, HEAD_DIM), BF16),
                pltpu.VMEM((2 * RING, slots, HEAD_DIM), BF16),
                pltpu.VMEM((2 * RING, slots, HEAD_DIM), BF16),
                pltpu.VMEM((2, slots, HEAD_DIM), BF16),
                pltpu.VMEM((2, slots, HEAD_DIM), BF16),
                pltpu.VMEM((slots, 2 * HEAD_DIM), BF16),
                pltpu.VMEM((HEAD_DIM, slots), BF16),
                pltpu.VMEM((chip_rows, head_w + 2 * HEAD_DIM), BF16),
                pltpu.VMEM((rows, head_w + 2 * HEAD_DIM), BF16),
                pltpu.VMEM((heads, rows, 2 * HEAD_DIM), BF16),
                pltpu.VMEM((slots, 256), F32),
                pltpu.VMEM((slots, 256), F32),
                pltpu.VMEM((heads, HEAD_DIM + 8, rows), F32),
                pltpu.VMEM(part_block, F32),
                pltpu.VMEM(part_block, F32),
                pltpu.VMEM(block, F32),
                pltpu.VMEM(block, F32),
                pltpu.VMEM((chip_rows, head_w), BF16),
                pltpu.VMEM((2, chip_rows, head_w), BF16),
                dma(6), dma(4), dma(4), dma(4), dma(4), dma(18), dma(2 * RING, 2), dma(2, 2), dma(1), dma(1),
                dma(4), dma(4), dma(4), dma(4), dma(2), dma(2),
            ],
            compiler_params=pltpu.CompilerParams(collective_id=0, has_side_effects=True, vmem_limit_bytes=67043328),
            name='attention',
        )(hidden_loc, cache_len, cache_k, cache_v, norm1_gain, w_query, w_key, w_value, cos, sin)

        cw = 512 if half_w % 512 == 0 and half_w > 512 else 256
        nc = half_w // cw
        half_f = w_gate.shape[1] // 2
        nu = half_f // 256
        br = 2 * shard_rows
        return pl.pallas_call(
            mlp_kernel,
            out_shape=jax.ShapeDtypeStruct((shard_rows, width), BF16),
            in_specs=[VMEM, VMEM, VMEM, ANY, ANY, ANY, ANY],
            out_specs=VMEM,
            scratch_shapes=[
                pltpu.VMEM((width, half_f), BF16),
                pltpu.VMEM((width, half_f), BF16),
                pltpu.VMEM((2 * half_f, half_w), BF16),
                pltpu.VMEM((nc, RING, br, cw), F32),
                pltpu.VMEM((nc, br, cw // 2), F32),
                pltpu.VMEM((nc, br, cw // 2), F32),
                pltpu.VMEM((nc, br, cw), F32),
                pltpu.VMEM((nc, br, cw), F32),
                pltpu.VMEM((2, RING, br, half_w), BF16),
                pltpu.VMEM((br, half_w), BF16),
                pltpu.VMEM((chip_rows, 2 * half_f), BF16),
                pltpu.VMEM((2, shard_rows, half_w), BF16),
                pltpu.VMEM((2, shard_rows, half_w), BF16),
                dma(5), dma(2, nc), dma(2, nc), dma(2, nc), dma(2, nc),
                dma(4, nc), dma(4, nc), dma(4, nc), dma(4, nc), dma(nu), dma(nu), dma(1), dma(1),
            ],
            compiler_params=pltpu.CompilerParams(collective_id=1, has_side_effects=True, vmem_limit_bytes=67043328),
            name='mlp',
        )(attended, xres, norm2_gain, w_out, w_gate, w_up, w_down)

    return jax.shard_map(device_layer, mesh=mesh, in_specs=(token_spec, P(('dp', 'cp', 'tp')), P('dp'), token_spec, token_spec, P(), column_spec, column_spec, column_spec, row_spec, P(), column_spec, column_spec, row_spec), out_specs=token_spec, check_vma=False)
```

```python
import functools
import math
import jax
import jax.numpy as jnp
from jax import lax
from jax.experimental import pallas as pl
from jax.experimental.pallas import tpu as pltpu
from jax.sharding import PartitionSpec as P

HEAD_DIM = 128
ROPE_BASE = 500000.0
NORM_EPS = 1e-5
MESH = pl.DeviceIdType.MESH
F32 = jnp.float32
BF16 = jnp.bfloat16
M_INIT = -1e38
MASKED = -3e38
EXP_SCALE = math.log2(math.e) / math.sqrt(HEAD_DIM)
RING = 4
STEP = 1024
ANY = pl.BlockSpec(memory_space=pl.ANY)
VMEM = pl.BlockSpec(memory_space=pltpu.VMEM)
SMEM = pl.BlockSpec(memory_space=pltpu.SMEM)


class Place:
    def __init__(self):
        self.y = lax.axis_index('tp')
        cp = lax.axis_index('cp')
        self.x = cp // 2
        self.core = cp % 2
        self.vx = self.x + self.core * (self.y - self.x)
        self.vy = self.y + self.core * (self.x - self.y)

    def at(self, dx=0, dy=0, core=None):
        return {'tp': (self.y + dy) % RING, 'cp': ((self.x + dx) % RING) * 2 + (self.core if core is None else core)}

    def mirrored(self, core):
        return {'tp': self.x, 'cp': self.y * 2 + core}


def remote(src, dst, send_sem, recv_sem, device):
    return pltpu.make_async_remote_copy(src_ref=src, dst_ref=dst, send_sem=send_sem, recv_sem=recv_sem, device_id=device, device_id_type=MESH)


def barrier(devices):
    sem = pltpu.get_barrier_semaphore()
    for device in devices:
        pl.semaphore_signal(sem, inc=1, device_id=device, device_id_type=MESH)
    pl.semaphore_wait(sem, len(devices))


def ring_gather(pos, right, left, block, half, sends, recvs, own=None, partner=None, core=None, psends=None, precvs=None, between=None):
    prev, nxt, far = (pos + 3) % RING, (pos + 1) % RING, (pos + 2) % RING
    mine = block(pos, core) if own is None else own
    to_right = remote(mine, block(pos, core), sends.at[0], recvs.at[0], right)
    to_left = remote(mine, block(pos, core), sends.at[1], recvs.at[1], left)
    to_right.start()
    to_left.start()
    copies = [to_right, to_left]
    given = []

    def give(p, i, source=None):
        if partner is not None:
            copy = remote(block(p, core) if source is None else source, block(p, core), psends.at[i], precvs.at[i], partner)
            copy.start()
            given.append(copy)

    give(pos, 0, mine)
    remote(block(prev, core), block(prev, core), sends.at[0], recvs.at[0], left).wait_recv()
    fwd_right = remote(half(prev, core, 0), half(prev, core, 0), sends.at[2], recvs.at[2], right)
    fwd_right.start()
    give(prev, 1)
    remote(block(nxt, core), block(nxt, core), sends.at[1], recvs.at[1], right).wait_recv()
    fwd_left = remote(half(nxt, core, 1), half(nxt, core, 1), sends.at[3], recvs.at[3], left)
    fwd_left.start()
    give(nxt, 2)
    copies += [fwd_right, fwd_left]
    if between is not None:
        between()
    remote(half(far, core, 0), half(far, core, 0), sends.at[2], recvs.at[2], left).wait_recv()
    remote(half(far, core, 1), half(far, core, 1), sends.at[3], recvs.at[3], right).wait_recv()
    give(far, 3)
    if partner is not None:
        for i, p in enumerate((pos, prev, nxt, far)):
            remote(block(p, 1 - core), block(p, 1 - core), psends.at[i], precvs.at[i], partner).wait_recv()
    return copies + given


def attention_kernel(shards, x_in, len_ref, ck, cv, gain, wq, wk, wv, cos_ref, sin_ref, o_out, xres_out,
                     xbuf, ckv, cvv, abuf, wqv, wkv, wvv, kbuf, vbuf, rk, rv, kaug, vt, qkv, qall, qaug, sa, sb, acc, r1l, r1r, r2l, r2r, otmp, obuf,
                     lsem, xs, xr, ps, pr, kvs, kvr, relay_r, qs, qr, rs, rr, os, orr):
    me = Place()
    x, y, core, vx, vy = me.x, me.y, me.core, me.vx, me.vy
    width = x_in.shape[1]
    half_w = width // 2
    slots = ck.shape[0]
    rows = qall.shape[0]
    chip_rows = rows // RING
    heads = acc.shape[0]
    head_w = heads * HEAD_DIM
    partner = me.at(core=1 - core)
    up, down = me.at(dy=1), me.at(dy=RING - 1)
    right, left = me.at(dx=1 - core, dy=core), me.at(dx=(1 - core) * (RING - 1), dy=core * (RING - 1))
    ahead, behind = me.at(dx=core, dy=1 - core), me.at(dx=core * (RING - 1), dy=(1 - core) * (RING - 1))
    moving = jnp.logical_and(core == 1, x != y)

    local = [
        pltpu.make_async_copy(x_in, xbuf.at[y, core], lsem.at[0]),
        pltpu.make_async_copy(ck, ckv, lsem.at[4]),
        pltpu.make_async_copy(cv, cvv, lsem.at[5]),
        pltpu.make_async_copy(wq.at[:, pl.ds(pl.multiple_of(core * head_w, head_w), head_w)], wqv, lsem.at[1]),
        pltpu.make_async_copy(wk.at[:, pl.ds(pl.multiple_of(core * HEAD_DIM, HEAD_DIM), HEAD_DIM)], wkv, lsem.at[2]),
        pltpu.make_async_copy(wv.at[:, pl.ds(pl.multiple_of(core * HEAD_DIM, HEAD_DIM), HEAD_DIM)], wvv, lsem.at[3]),
    ]
    local[0].start()
    for copy in local[1:]:
        copy.start()

    peers = [me.at(dx, dy, c) for dx in range(RING) for dy in range(RING) for c in range(2)]
    barrier(peers)

    def kv_lanes(head):
        return pl.ds(pl.multiple_of(head * HEAD_DIM, HEAD_DIM), HEAD_DIM)

    def target(role, d):
        return me.at(dx=d if role else 0, dy=0 if role else d, core=role)

    def target_lanes(role, d):
        return kv_lanes(2 * (((x if role else y) + d) % RING) + role)

    kv_copies = []

    def kv_send(src, dst, recv, device):
        copy = remote(src, dst, kvs.at[len(kv_copies)], recv, device)
        copy.start()
        kv_copies.append(copy)

    def send_near():
        local[1].wait()
        local[2].wait()
        other_vy = x + y - vy
        for i, (src, dst) in enumerate(((ck, kbuf), (cv, vbuf))):
            pltpu.make_async_copy(src.at[:, kv_lanes(2 * vy + core)], dst.at[core], kvr.at[core, i]).start()
            kv_send((ckv, cvv)[i].at[:, kv_lanes(2 * other_vy + 1 - core)], dst.at[core], kvr.at[core, i], partner)
        for role in range(2):
            kv_send(ckv.at[:, target_lanes(role, 2)], rk.at[core], relay_r.at[0, core], target(role, 1))
            kv_send(cvv.at[:, target_lanes(role, 2)], rv.at[core], relay_r.at[1, core], target(role, RING - 1))

    def send_direct(i, src, dst):
        for role in range(2):
            for d, slot in ((1, 2), (3, 4)):
                kv_send(src.at[:, target_lanes(role, d)], dst.at[slot + core], kvr.at[slot + core, i], target(role, d))

    def send_early():
        send_near()
        send_direct(0, ckv, kbuf)

    def send_late():
        send_direct(1, cvv, vbuf)
        for c in range(2):
            remote(rk.at[c], rk.at[c], kvs.at[0], relay_r.at[0, c], behind).wait_recv()
            kv_send(rk.at[c], kbuf.at[6 + c], kvr.at[6 + c, 0], ahead)
            remote(rv.at[c], rv.at[c], kvs.at[0], relay_r.at[1, c], ahead).wait_recv()
            kv_send(rv.at[c], vbuf.at[6 + c], kvr.at[6 + c, 1], behind)

    x_copies = ring_gather(
        y, up, down, lambda p, c: xbuf.at[p, c], lambda p, c, i: xbuf.at[p, c, :, pl.ds(i * half_w, half_w)],
        xs, xr, own=x_in, partner=partner, core=core, psends=ps, precvs=pr, between=send_early)
    local[0].wait()

    def norm_block(i, carry):
        values = xbuf[i].reshape(2 * xbuf.shape[2], width).astype(F32)
        inv = lax.rsqrt(jnp.mean(values * values, axis=-1, keepdims=True) + NORM_EPS)
        abuf[i] = (values * inv * gain[...].reshape(1, width).astype(F32)).astype(BF16)
        return carry

    lax.fori_loop(0, RING, norm_block, 0)
    xres_out[...] = xbuf[y, :, :, pl.ds(pl.multiple_of(core * half_w, half_w), half_w)].reshape(xres_out.shape)

    for copy in local[3:]:
        copy.wait()
    normed = abuf[...].reshape(chip_rows, width)
    cos, sin = cos_ref[...], sin_ref[...]

    def rotate(v):
        return (v * cos + pltpu.roll(v, HEAD_DIM // 2, 1) * sin).astype(BF16)

    q = jnp.dot(normed, wqv[...], preferred_element_type=F32)
    for h in range(heads):
        qkv[:, h * HEAD_DIM:(h + 1) * HEAD_DIM] = rotate(q[:, h * HEAD_DIM:(h + 1) * HEAD_DIM])
    qkv[:, head_w:head_w + HEAD_DIM] = rotate(jnp.dot(normed, wkv[...], preferred_element_type=F32))
    qkv[:, head_w + HEAD_DIM:] = jnp.dot(normed, wvv[...], preferred_element_type=F32).astype(BF16)

    def q_rows(p):
        return pl.ds(pl.multiple_of(p * chip_rows, chip_rows), chip_rows)

    def reader(e):
        stepped = (x + e) % RING
        return {'tp': y + core * (stepped - y), 'cp': (stepped + core * (y - stepped)) * 2 + core}

    def q_part(e, block):
        at = qall.at[q_rows(block), pl.ds(0, head_w)]
        return remote(qkv.at[:, pl.ds(0, head_w)], at, qs.at[e], qr.at[e], reader(e))

    mirror_send = remote(qkv, qall.at[q_rows(x)], qs.at[0], qr.at[0], me.mirrored(core))

    @pl.when(moving)
    def _():
        mirror_send.start()

    @pl.when(jnp.logical_not(moving))
    def _():
        qall[q_rows(vx), :] = qkv[...]

    q_copies = [q_part(e, x) for e in (1, 3, 2)]
    for copy in q_copies:
        copy.start()
    send_late()
    for e in (1, 3, 2):
        q_part(e, (vx - e + RING) % RING).wait_recv()

    @pl.when(moving)
    def _():
        remote(qkv, qall.at[q_rows(vx)], qs.at[0], qr.at[0], me.mirrored(core)).wait_recv()

    first_lane = jnp.where(lax.broadcasted_iota(jnp.int32, (rows, HEAD_DIM), 1) == 0, 1.0, 0.0).astype(BF16)
    for h in range(heads):
        qaug[h, :, 0:HEAD_DIM] = qall[:, h * HEAD_DIM:(h + 1) * HEAD_DIM]
        qaug[h, :, HEAD_DIM:] = first_lane

    tile = 256
    tiles = rows // tile
    contract_last = (((1,), (1,)), ((), ()))

    def finish(s_ref, e_top, vt_ref, h, j, first, depth):
        lanes = pl.ds(j * tile, tile)
        if first:
            m_new = jnp.maximum(e_top, M_INIT)
        else:
            m_old = acc[h, HEAD_DIM:HEAD_DIM + 1, lanes]
            l_old = acc[h, HEAD_DIM + 1:HEAD_DIM + 2, lanes]
            m_new = jnp.maximum(e_top, m_old)
        m_scaled = m_new * EXP_SCALE
        part_l, o = None, None
        step = min(STEP, depth)
        for k in range(0, depth, step):
            e = jnp.exp2(s_ref[k:k + step, :] * EXP_SCALE - m_scaled)
            total_e = jnp.sum(e.reshape(step // 8, 8, tile), axis=0)
            part_l = total_e if part_l is None else part_l + total_e
            term = jnp.dot(vt_ref[:, k:k + step], e.astype(BF16), preferred_element_type=F32)
            o = term if o is None else o + term
        l_new = jnp.sum(part_l, axis=0, keepdims=True)
        if not first:
            alpha = jnp.exp2((m_old - m_new) * EXP_SCALE)
            l_new = l_new + l_old * alpha
            o = o + acc[h, 0:HEAD_DIM, lanes] * alpha
        acc[h, 0:HEAD_DIM, lanes] = o
        acc[h, HEAD_DIM:HEAD_DIM + 1, lanes] = m_new
        acc[h, HEAD_DIM + 1:HEAD_DIM + 2, lanes] = l_new

    my_rows = q_rows(vx)
    vnew_t = qall[my_rows, head_w + HEAD_DIM:].T
    knew = qall[my_rows, head_w:head_w + HEAD_DIM]

    def new_head(h, carry):
        for j in range(tiles):
            s = lax.dot_general(knew, qaug[h, j * tile:(j + 1) * tile, 0:HEAD_DIM], contract_last, preferred_element_type=F32)
            relk = relative_positions(vx * chip_rows + lax.broadcasted_iota(jnp.int32, s.shape, 0), shards)
            relq = relative_positions(j * tile + lax.broadcasted_iota(jnp.int32, s.shape, 1), shards)
            causal = relk <= relq
            s = jnp.where(causal, s, -jnp.inf)
            finish(s, jnp.max(s, axis=0, keepdims=True), vnew_t, h, j, True, chip_rows)
        return carry

    lax.fori_loop(0, heads, new_head, 0)
    cache_len = len_ref[0]
    slot_ids = lax.broadcasted_iota(jnp.int32, (slots, HEAD_DIM), 0)

    def scores(h, j, dst):
        s = lax.dot_general(kaug[...], qaug[h, j * tile:(j + 1) * tile, :], contract_last, preferred_element_type=F32)
        dst[...] = s
        return jnp.max(s, axis=0, keepdims=True)

    def source(s, carry):
        u, src_core = s // 2, s % 2
        d = u + (u // 2) * (1 - 2 * (u % 2))
        src_x = (x - core * d + RING) % RING
        src_y = (y - (1 - core) * d + RING) % RING
        base = ((2 * src_x + src_core) * RING + src_y) * slots
        for i, (src, dst) in enumerate(((ckv, kbuf), (cvv, vbuf))):
            pltpu.make_async_copy(src.at[:, pl.ds(0, HEAD_DIM)], dst.at[s], kvr.at[s, i]).wait()
        vt[...] = vbuf[s].T
        seen = slot_ids < cache_len - base
        kaug[:, 0:HEAD_DIM] = jnp.where(seen, kbuf[s].astype(F32), 0.0).astype(BF16)
        kaug[:, HEAD_DIM:] = jnp.where(seen, 0.0, MASKED).astype(BF16)

        top_a = scores(0, 0, sa)
        for h in range(heads):
            top_b = scores(h, 1, sb)
            finish(sa, top_a, vt, h, 0, False, slots)
            if h + 1 < heads:
                top_a = scores(h + 1, 0, sa)
            finish(sb, top_b, vt, h, 1, False, slots)
        return carry

    lax.fori_loop(0, 2 * RING, source, 0)

    hh = heads // 2
    far, nxt, prev = (vx + 2) % RING, (vx + 1) % RING, (vx + 3) % RING
    p1 = [remote(acc.at[pl.ds(0, hh), :, q_rows(far)], r1l, rs.at[0], rr.at[0], right),
          remote(acc.at[pl.ds(hh, hh), :, q_rows(far)], r1r, rs.at[1], rr.at[1], left)]
    for copy in p1:
        copy.start()

    def merge(a, b):
        ma, mb = a[:, HEAD_DIM:HEAD_DIM + 1, :], b[:, HEAD_DIM:HEAD_DIM + 1, :]
        m = jnp.maximum(ma, mb)
        wa, wb = jnp.exp2((ma - m) * EXP_SCALE), jnp.exp2((mb - m) * EXP_SCALE)
        o = a[:, 0:HEAD_DIM, :] * wa + b[:, 0:HEAD_DIM, :] * wb
        l = a[:, HEAD_DIM + 1:HEAD_DIM + 2, :] * wa + b[:, HEAD_DIM + 1:HEAD_DIM + 2, :] * wb
        return o, m, l

    def merge_into(lo, p, other):
        o, m, l = merge(acc[lo:lo + hh, :, q_rows(p)], other[...])
        acc[lo:lo + hh, 0:HEAD_DIM, q_rows(p)] = o
        acc[lo:lo + hh, HEAD_DIM:HEAD_DIM + 1, q_rows(p)] = m
        acc[lo:lo + hh, HEAD_DIM + 1:HEAD_DIM + 2, q_rows(p)] = l

    p2 = [remote(acc.at[:, :, q_rows(nxt)], r2l, rs.at[2], rr.at[2], right),
          remote(acc.at[:, :, q_rows(prev)], r2r, rs.at[3], rr.at[3], left)]
    p1[0].wait_recv()
    merge_into(0, nxt, r1l)
    p2[0].start()
    p1[1].wait_recv()
    merge_into(hh, prev, r1r)
    p2[1].start()
    for copy in p2:
        copy.wait_recv()
    for h in range(heads):
        a, b, d = acc[h:h + 1, :, q_rows(vx)], r2l[h:h + 1], r2r[h:h + 1]
        o, m, l = merge(a, b)
        md = d[:, HEAD_DIM:HEAD_DIM + 1, :]
        top = jnp.maximum(m, md)
        w, wd = jnp.exp2((m - top) * EXP_SCALE), jnp.exp2((md - top) * EXP_SCALE)
        o = o * w + d[:, 0:HEAD_DIM, :] * wd
        l = l * w + d[:, HEAD_DIM + 1:HEAD_DIM + 2, :] * wd
        otmp[:, h * HEAD_DIM:(h + 1) * HEAD_DIM] = (o / l)[0].T.astype(BF16)

    other_at = {'tp': vy, 'cp': vx * 2 + 1 - core}
    other_out = remote(otmp, obuf.at[core], os.at[1], orr.at[1], other_at)
    other_out.start()
    same_out = remote(otmp, obuf.at[core], os.at[0], orr.at[0], me.mirrored(core))

    @pl.when(moving)
    def _():
        same_out.start()
        same_out.wait_recv()

    @pl.when(jnp.logical_not(moving))
    def _():
        obuf[core] = otmp[...]

    remote(otmp, obuf.at[1 - core], os.at[1], orr.at[1], partner).wait_recv()
    o_out[:, 0:head_w] = obuf[0]
    o_out[:, head_w:2 * head_w] = obuf[1]
    for copy in x_copies + kv_copies + q_copies + p1 + p2 + [other_out]:
        copy.wait_send()

    @pl.when(moving)
    def _():
        mirror_send.wait_send()
        same_out.wait_send()


def mlp_kernel(o_in, xres, gain, wo, wg, wu, wd, out,
               wgv, wuv, wdv, part, r1l, r1r, r2l, r2r, hbuf, hres, ubuf, fin, fbuf,
               wsem, s1, q1, s2, q2, hs, hr, ps, pr, us, ur, fs, fr):
    me = Place()
    y, core = me.y, me.core
    nc, _, _, cw = part.shape
    half_w = nc * cw
    width = 2 * half_w
    rows = o_in.shape[0]
    block_rows = rows // RING
    half_f = wgv.shape[1]
    uw = 256
    nu = half_f // uw
    partner = me.at(core=1 - core)
    up, down = me.at(dy=1), me.at(dy=RING - 1)
    far, nxt, prev = (y + 2) % RING, (y + 1) % RING, (y + 3) % RING
    col0 = core * half_w

    def lanes(start, size):
        return pl.ds(pl.multiple_of(start, 128), size)

    wo_rows, wd_rows = wo.shape[0], wd.shape[0]
    up_cols, out_cols = lanes(core * half_f, half_f), lanes(col0, half_w)
    wo_load = pltpu.make_async_copy(wo.at[:, out_cols], wdv.at[pl.ds(0, wo_rows), :], wsem.at[0])
    wd_load = pltpu.make_async_copy(wd.at[pl.ds(wo_rows, wd_rows - wo_rows), out_cols], wdv.at[pl.ds(wo_rows, wd_rows - wo_rows), :], wsem.at[1])
    wd_late = pltpu.make_async_copy(wd.at[pl.ds(0, wo_rows), out_cols], wdv.at[pl.ds(0, wo_rows), :], wsem.at[2])
    wg_load = pltpu.make_async_copy(wg.at[:, up_cols], wgv, wsem.at[3])
    wu_load = pltpu.make_async_copy(wu.at[:, up_cols], wuv, wsem.at[4])
    for copy in (wo_load, wg_load, wu_load, wd_load):
        copy.start()

    barrier([up, down, partner])

    hc = cw // 2

    def first_sends(j):
        return (remote(part.at[j, far, :, pl.ds(0, hc)], r1l.at[j], s1.at[0, j], q1.at[0, j], up),
                remote(part.at[j, far, :, pl.ds(hc, hc)], r1r.at[j], s1.at[1, j], q1.at[1, j], down))

    def second_sends(j):
        return (remote(part.at[j, nxt], r2l.at[j], s2.at[0, j], q2.at[0, j], up),
                remote(part.at[j, prev], r2r.at[j], s2.at[1, j], q2.at[1, j], down))

    def relay(j, carry):
        a, b = first_sends(j)
        a.wait_recv()
        part[j, nxt, :, 0:hc] = part[j, nxt, :, 0:hc] + r1l[j]
        b.wait_recv()
        part[j, prev, :, hc:cw] = part[j, prev, :, hc:cw] + r1r[j]
        for copy in second_sends(j):
            copy.start()
        return carry

    def total(j):
        for copy in second_sends(j):
            copy.wait_recv()
        return part[j, y] + r2l[j] + r2r[j]

    def drain(j, carry):
        for copy in first_sends(j) + second_sends(j):
            copy.wait_send()
        return carry

    attended = o_in[...]
    wo_load.wait()

    def out_chunk(j, carry):
        part[j] = jnp.dot(attended, wdv[0:wo_rows, lanes(j * cw, cw)], preferred_element_type=F32).reshape(RING, block_rows, cw)
        for copy in first_sends(j):
            copy.start()
        return carry

    lax.fori_loop(0, nc, out_chunk, 0)
    wd_late.start()
    lax.fori_loop(0, nc, relay, 0)

    def h_piece(c, p, j):
        return hbuf.at[c, p, :, lanes(j * cw, cw)]

    def h_half(c, p, j, i):
        return hbuf.at[c, p, :, lanes(j * cw + i * hc, hc)]

    def h_steps(j):
        return (remote(h_piece(core, y, j), h_piece(core, y, j), hs.at[0, j], hr.at[0, j], up),
                remote(h_piece(core, y, j), h_piece(core, y, j), hs.at[1, j], hr.at[1, j], down),
                remote(h_half(core, prev, j, 0), h_half(core, prev, j, 0), hs.at[2, j], hr.at[2, j], up),
                remote(h_half(core, nxt, j, 1), h_half(core, nxt, j, 1), hs.at[3, j], hr.at[3, j], down))

    def h_give(j, i, p, c):
        return remote(h_piece(c, p, j), h_piece(c, p, j), ps.at[i, j], pr.at[i, j], partner)

    def mid_chunk(j, carry):
        c = lanes(j * cw, cw)
        mid = (xres[:, c].astype(F32) + total(j)).astype(BF16)
        hres[:, c] = mid
        hbuf[core, y, :, c] = mid
        for copy in h_steps(j)[:2] + (h_give(j, 0, y, core),):
            copy.start()
        return carry

    lax.fori_loop(0, nc, mid_chunk, 0)

    def h_forward(j, carry):
        steps = h_steps(j)
        remote(h_piece(core, prev, j), h_piece(core, prev, j), hs.at[0, j], hr.at[0, j], down).wait_recv()
        steps[2].start()
        h_give(j, 1, prev, core).start()
        remote(h_piece(core, nxt, j), h_piece(core, nxt, j), hs.at[1, j], hr.at[1, j], up).wait_recv()
        steps[3].start()
        h_give(j, 2, nxt, core).start()
        return carry

    lax.fori_loop(0, nc, h_forward, 0)

    def h_last(j, carry):
        remote(h_half(core, far, j, 0), h_half(core, far, j, 0), hs.at[2, j], hr.at[2, j], down).wait_recv()
        remote(h_half(core, far, j, 1), h_half(core, far, j, 1), hs.at[3, j], hr.at[3, j], up).wait_recv()
        h_give(j, 3, far, core).start()
        return carry

    lax.fori_loop(0, nc, h_last, 0)

    def h_end(j, carry):
        for i, p in enumerate((y, prev, nxt, far)):
            h_give(j, i, p, 1 - core).wait_recv()
        for copy in h_steps(j):
            copy.wait_send()
        for i, p in enumerate((y, prev, nxt, far)):
            h_give(j, i, p, core).wait_send()
        return carry

    lax.fori_loop(0, nc, h_end, 0)
    lax.fori_loop(0, nc, drain, 0)

    def norm_block(i, carry):
        v0, v1 = hbuf[0, i].astype(F32), hbuf[1, i].astype(F32)
        mean = (jnp.sum(v0 * v0, axis=-1, keepdims=True) + jnp.sum(v1 * v1, axis=-1, keepdims=True)) / width
        inv = lax.rsqrt(mean + NORM_EPS)
        hbuf[0, i] = (v0 * inv * gain[0:half_w].reshape(1, half_w).astype(F32)).astype(BF16)
        hbuf[1, i] = (v1 * inv * gain[half_w:width].reshape(1, half_w).astype(F32)).astype(BF16)
        return carry

    lax.fori_loop(0, RING, norm_block, 0)
    b0, b1 = hbuf[0].reshape(rows, half_w), hbuf[1].reshape(rows, half_w)

    def u_copy(j, c):
        at = ubuf.at[:, lanes(c * half_f + j * uw, uw)]
        return remote(at, at, us.at[j], ur.at[j], partner)

    def up_chunk(j, carry):
        c = lanes(j * uw, uw)
        gate = jnp.dot(b0, wgv[0:half_w, c], preferred_element_type=F32) + jnp.dot(b1, wgv[half_w:width, c], preferred_element_type=F32)
        upper = jnp.dot(b0, wuv[0:half_w, c], preferred_element_type=F32) + jnp.dot(b1, wuv[half_w:width, c], preferred_element_type=F32)
        ubuf[:, lanes(core * half_f + j * uw, uw)] = (jax.nn.silu(gate) * upper).astype(BF16)
        u_copy(j, core).start()
        return carry

    wg_load.wait()
    wu_load.wait()
    lax.fori_loop(0, nu, up_chunk, 0)
    wd_load.wait()
    wd_late.wait()
    for j in range(nu):
        u_copy(j, 1 - core).wait_recv()

    def down_chunk(j, carry):
        part[j] = jnp.dot(ubuf[...], wdv[:, lanes(j * cw, cw)], preferred_element_type=F32).reshape(RING, block_rows, cw)
        for copy in first_sends(j):
            copy.start()
        return carry

    lax.fori_loop(0, nc, down_chunk, 0)
    lax.fori_loop(0, nc, relay, 0)

    def last_chunk(j, carry):
        c = lanes(j * cw, cw)
        fin[:, :, c] = (hres[:, c].astype(F32) + total(j)).astype(BF16).reshape(2, block_rows // 2, cw)
        return carry

    lax.fori_loop(0, nc, last_chunk, 0)
    swap = remote(fin.at[1 - core], fbuf.at[core], fs.at[0], fr.at[0], partner)
    swap.start()
    own = fin[core]
    out[:, lanes(col0, half_w)] = own
    remote(fin.at[core], fbuf.at[1 - core], fs.at[0], fr.at[0], partner).wait_recv()
    out[:, lanes((1 - core) * half_w, half_w)] = fbuf[1 - core]
    for j in range(nu):
        u_copy(j, core).wait_send()
    lax.fori_loop(0, nc, drain, 0)
    swap.wait_send()


def dma(*shape):
    return pltpu.SemaphoreType.DMA(shape)


def relative_positions(r, shards):
    x, y, core, w = r >> 7, (r >> 5) & 3, (r >> 4) & 1, r & 15
    k = (2 * x + core) * RING + y
    run = jnp.where(w < 8, k, 2 * shards - 1 - k)
    return run * 8 + (w & 7)


def solution(mesh):
    token_spec = P(('dp', 'cp', 'tp'), None)
    column_spec = P(None, 'tp')
    row_spec = P('tp', None)
    shards = mesh.shape['tp'] * mesh.shape['cp']

    def device_layer(hidden_loc, pos_loc, cache_len, cache_k, cache_v, norm1_gain, w_query, w_key, w_value, w_out, norm2_gain, w_gate, w_up, w_down):
        shard_rows, width = hidden_loc.shape
        half_w = width // 2
        chip_rows = 2 * RING * shard_rows
        rows = RING * chip_rows
        slots = cache_k.shape[0]
        head_w = w_query.shape[1] // 2
        heads = head_w // HEAD_DIM
        half = HEAD_DIM // 2
        lane = jnp.arange(HEAD_DIM, dtype=jnp.int32)
        rel = relative_positions((lax.axis_index('cp') // 2) * chip_rows + jnp.arange(chip_rows, dtype=jnp.int32), shards)
        inv_freq = 1.0 / (ROPE_BASE ** ((lane % half).astype(F32) * (2.0 / HEAD_DIM)))
        angles = (cache_len[0] + rel).astype(F32)[:, None] * inv_freq[None, :]
        cos, sin = jnp.cos(angles), jnp.sin(angles) * jnp.where(lane < half, -1.0, 1.0)[None, :]
        block = (heads, HEAD_DIM + 8, chip_rows)
        part_block = (heads // 2,) + block[1:]
        attended, xres = pl.pallas_call(
            functools.partial(attention_kernel, shards),
            out_shape=(jax.ShapeDtypeStruct((chip_rows, 2 * head_w), BF16), jax.ShapeDtypeStruct((2 * shard_rows, half_w), BF16)),
            in_specs=[ANY, SMEM, ANY, ANY, VMEM, ANY, ANY, ANY, VMEM, VMEM],
            out_specs=(VMEM, VMEM),
            scratch_shapes=[
                pltpu.VMEM((RING, 2, shard_rows, width), BF16),
                pltpu.VMEM(cache_k.shape, BF16),
                pltpu.VMEM(cache_v.shape, BF16),
                pltpu.VMEM((RING, 2 * shard_rows, width), BF16),
                pltpu.VMEM((width, head_w), BF16),
                pltpu.VMEM((width, HEAD_DIM), BF16),
                pltpu.VMEM((width, HEAD_DIM), BF16),
                pltpu.VMEM((2 * RING, slots, HEAD_DIM), BF16),
                pltpu.VMEM((2 * RING, slots, HEAD_DIM), BF16),
                pltpu.VMEM((2, slots, HEAD_DIM), BF16),
                pltpu.VMEM((2, slots, HEAD_DIM), BF16),
                pltpu.VMEM((slots, 2 * HEAD_DIM), BF16),
                pltpu.VMEM((HEAD_DIM, slots), BF16),
                pltpu.VMEM((chip_rows, head_w + 2 * HEAD_DIM), BF16),
                pltpu.VMEM((rows, head_w + 2 * HEAD_DIM), BF16),
                pltpu.VMEM((heads, rows, 2 * HEAD_DIM), BF16),
                pltpu.VMEM((slots, 256), F32),
                pltpu.VMEM((slots, 256), F32),
                pltpu.VMEM((heads, HEAD_DIM + 8, rows), F32),
                pltpu.VMEM(part_block, F32),
                pltpu.VMEM(part_block, F32),
                pltpu.VMEM(block, F32),
                pltpu.VMEM(block, F32),
                pltpu.VMEM((chip_rows, head_w), BF16),
                pltpu.VMEM((2, chip_rows, head_w), BF16),
                dma(6), dma(4), dma(4), dma(4), dma(4), dma(18), dma(2 * RING, 2), dma(2, 2),
                dma(4), dma(4), dma(4), dma(4), dma(2), dma(2),
            ],
            compiler_params=pltpu.CompilerParams(collective_id=0, has_side_effects=True, vmem_limit_bytes=67043328),
            name='attention',
        )(hidden_loc, cache_len, cache_k, cache_v, norm1_gain, w_query, w_key, w_value, cos, sin)

        cw = 512 if half_w % 512 == 0 and half_w > 512 else 256
        nc = half_w // cw
        half_f = w_gate.shape[1] // 2
        nu = half_f // 256
        br = 2 * shard_rows
        return pl.pallas_call(
            mlp_kernel,
            out_shape=jax.ShapeDtypeStruct((shard_rows, width), BF16),
            in_specs=[VMEM, VMEM, VMEM, ANY, ANY, ANY, ANY],
            out_specs=VMEM,
            scratch_shapes=[
                pltpu.VMEM((width, half_f), BF16),
                pltpu.VMEM((width, half_f), BF16),
                pltpu.VMEM((2 * half_f, half_w), BF16),
                pltpu.VMEM((nc, RING, br, cw), F32),
                pltpu.VMEM((nc, br, cw // 2), F32),
                pltpu.VMEM((nc, br, cw // 2), F32),
                pltpu.VMEM((nc, br, cw), F32),
                pltpu.VMEM((nc, br, cw), F32),
                pltpu.VMEM((2, RING, br, half_w), BF16),
                pltpu.VMEM((br, half_w), BF16),
                pltpu.VMEM((chip_rows, 2 * half_f), BF16),
                pltpu.VMEM((2, shard_rows, half_w), BF16),
                pltpu.VMEM((2, shard_rows, half_w), BF16),
                dma(5), dma(2, nc), dma(2, nc), dma(2, nc), dma(2, nc),
                dma(4, nc), dma(4, nc), dma(4, nc), dma(4, nc), dma(nu), dma(nu), dma(1), dma(1),
            ],
            compiler_params=pltpu.CompilerParams(collective_id=1, has_side_effects=True, vmem_limit_bytes=67043328),
            name='mlp',
        )(attended, xres, norm2_gain, w_out, w_gate, w_up, w_down)

    return jax.shard_map(device_layer, mesh=mesh, in_specs=(token_spec, P(('dp', 'cp', 'tp')), P('dp'), token_spec, token_spec, P(), column_spec, column_spec, column_spec, row_spec, P(), column_spec, column_spec, row_spec), out_specs=token_spec, check_vma=False)
```

```python
import functools
import math
import jax
import jax.numpy as jnp
from jax import lax
from jax.experimental import pallas as pl
from jax.experimental.pallas import tpu as pltpu
from jax.sharding import PartitionSpec as P

HEAD_DIM = 128
ROPE_BASE = 500000.0
NORM_EPS = 1e-5
MESH = pl.DeviceIdType.MESH
F32 = jnp.float32
BF16 = jnp.bfloat16
M_INIT = -1e38
MASKED = -3e38
EXP_SCALE = math.log2(math.e) / math.sqrt(HEAD_DIM)
RING = 4
STEP = 1024
ANY = pl.BlockSpec(memory_space=pl.ANY)
VMEM = pl.BlockSpec(memory_space=pltpu.VMEM)
SMEM = pl.BlockSpec(memory_space=pltpu.SMEM)


class Place:
    def __init__(self):
        self.y = lax.axis_index('tp')
        cp = lax.axis_index('cp')
        self.x = cp // 2
        self.core = cp % 2
        self.vx = self.x + self.core * (self.y - self.x)
        self.vy = self.y + self.core * (self.x - self.y)

    def at(self, dx=0, dy=0, core=None):
        return {'tp': (self.y + dy) % RING, 'cp': ((self.x + dx) % RING) * 2 + (self.core if core is None else core)}

    def mirrored(self, core):
        return {'tp': self.x, 'cp': self.y * 2 + core}


def remote(src, dst, send_sem, recv_sem, device):
    return pltpu.make_async_remote_copy(src_ref=src, dst_ref=dst, send_sem=send_sem, recv_sem=recv_sem, device_id=device, device_id_type=MESH)


def barrier(devices):
    sem = pltpu.get_barrier_semaphore()
    for device in devices:
        pl.semaphore_signal(sem, inc=1, device_id=device, device_id_type=MESH)
    pl.semaphore_wait(sem, len(devices))


def ring_gather(pos, right, left, block, half, own, sends, recvs, partner, core, psends, precvs, between):
    prev, nxt, far = (pos + RING - 1) % RING, (pos + 1) % RING, (pos + 2) % RING

    def step(i, ref, device):
        return remote(ref, ref, sends.at[i], recvs.at[i], device)

    def give(i, p, c):
        return remote(block(p, c), block(p, c), psends.at[i], precvs.at[i], partner)

    to_partner = remote(own, block(pos, core), psends.at[0], precvs.at[0], partner)
    copies = [remote(own, block(pos, core), sends.at[i], recvs.at[i], device) for i, device in enumerate((right, left))] + [to_partner]
    for copy in copies:
        copy.start()
    order = (pos, prev, nxt, far)
    for i, came, onward in ((0, left, right), (1, right, left)):
        p = order[i + 1]
        step(i, block(p, core), came).wait_recv()
        forward = [step(i + 2, half(p, core, i), onward), give(i + 1, p, core)]
        for copy in forward:
            copy.start()
        copies += forward
    between()
    for i, came in enumerate((left, right)):
        step(i + 2, half(far, core, i), came).wait_recv()
    last = give(RING - 1, far, core)
    last.start()
    for i, p in enumerate(order):
        give(i, p, 1 - core).wait_recv()
    return copies + [last]


def attention_kernel(shards, x_in, len_ref, ck, cv, gain, wq, wk, wv, cos_ref, sin_ref, o_out, xres_out,
                     xbuf, ckv, cvv, abuf, wqv, wkv, wvv, kbuf, vbuf, rk, rv, kaug, vt, qkv, qall, qaug, sa, sb, acc, r1l, r1r, r2l, r2r, otmp, obuf,
                     lsem, xs, xr, ps, pr, kvs, kvr, relay_r, ts, tr, qs, qr, rs, rr, os, orr):
    me = Place()
    x, y, core, vx, vy = me.x, me.y, me.core, me.vx, me.vy
    width = x_in.shape[1]
    half_w = width // 2
    slots = ck.shape[0]
    rows = qall.shape[0]
    chip_rows = rows // RING
    heads = acc.shape[0]
    head_w = heads * HEAD_DIM
    partner = me.at(core=1 - core)
    up, down = me.at(dy=1), me.at(dy=RING - 1)
    right, left = me.at(dx=1 - core, dy=core), me.at(dx=(1 - core) * (RING - 1), dy=core * (RING - 1))
    ahead, behind = me.at(dx=core, dy=1 - core), me.at(dx=core * (RING - 1), dy=(1 - core) * (RING - 1))
    moving = jnp.logical_and(core == 1, x != y)

    local = [
        pltpu.make_async_copy(x_in, xbuf.at[y, core], lsem.at[0]),
        pltpu.make_async_copy(ck, ckv, lsem.at[4]),
        pltpu.make_async_copy(cv, cvv, lsem.at[5]),
        pltpu.make_async_copy(wq.at[:, pl.ds(pl.multiple_of(core * head_w, head_w), head_w)], wqv, lsem.at[1]),
        pltpu.make_async_copy(wk.at[:, pl.ds(pl.multiple_of(core * HEAD_DIM, HEAD_DIM), HEAD_DIM)], wkv, lsem.at[2]),
        pltpu.make_async_copy(wv.at[:, pl.ds(pl.multiple_of(core * HEAD_DIM, HEAD_DIM), HEAD_DIM)], wvv, lsem.at[3]),
    ]
    local[0].start()
    for copy in local[1:]:
        copy.start()

    peers = [partner, me.mirrored(0), me.mirrored(1)]
    peers += [me.at(dy=d, core=c) for d in range(1, RING) for c in range(2)] + [me.at(dx=d, core=c) for d in range(1, RING) for c in range(2)]
    barrier(peers)

    def kv_lanes(head):
        return pl.ds(pl.multiple_of(head * HEAD_DIM, HEAD_DIM), HEAD_DIM)

    def target(role, d):
        return me.at(dx=d if role else 0, dy=0 if role else d, core=role)

    def target_lanes(role, d):
        return kv_lanes(2 * (((x if role else y) + d) % RING) + role)

    kv_copies = []

    def kv_send(src, dst, recv, device):
        copy = remote(src, dst, kvs.at[len(kv_copies)], recv, device)
        copy.start()
        kv_copies.append(copy)

    def send_near():
        local[1].wait()
        local[2].wait()
        other_vy = x + y - vy
        for i, (src, dst) in enumerate(((ck, kbuf), (cv, vbuf))):
            pltpu.make_async_copy(src.at[:, kv_lanes(2 * vy + core)], dst.at[core], kvr.at[core, i]).start()
            kv_send((ckv, cvv)[i].at[:, kv_lanes(2 * other_vy + 1 - core)], dst.at[core], kvr.at[core, i], partner)
        for role in range(2):
            kv_send(ckv.at[:, target_lanes(role, 2)], rk.at[core], relay_r.at[0, core], target(role, 1))
            kv_send(cvv.at[:, target_lanes(role, 2)], rv.at[core], relay_r.at[1, core], target(role, RING - 1))

    def send_far():
        for i, (src, dst) in enumerate(((ckv, kbuf), (cvv, vbuf))):
            for role in range(2):
                for d, slot in ((1, 2), (3, 4)):
                    kv_send(src.at[:, target_lanes(role, d)], dst.at[slot + core], kvr.at[slot + core, i], target(role, d))
        for c in range(2):
            remote(rk.at[c], rk.at[c], kvs.at[0], relay_r.at[0, c], behind).wait_recv()
            kv_send(rk.at[c], kbuf.at[6 + c], kvr.at[6 + c, 0], ahead)
            remote(rv.at[c], rv.at[c], kvs.at[0], relay_r.at[1, c], ahead).wait_recv()
            kv_send(rv.at[c], vbuf.at[6 + c], kvr.at[6 + c, 1], behind)

    x_copies = ring_gather(
        y, up, down, lambda p, c: xbuf.at[p, c], lambda p, c, i: xbuf.at[p, c, :, pl.ds(i * half_w, half_w)],
        x_in, xs, xr, partner, core, ps, pr, send_near)
    local[0].wait()

    def norm_block(i, carry):
        values = xbuf[i].reshape(2 * xbuf.shape[2], width).astype(F32)
        inv = lax.rsqrt(jnp.mean(values * values, axis=-1, keepdims=True) + NORM_EPS)
        abuf[i] = (values * inv * gain[...].reshape(1, width).astype(F32)).astype(BF16)
        return carry

    lax.fori_loop(0, RING, norm_block, 0)
    xres_out[...] = xbuf[y, :, :, pl.ds(pl.multiple_of(core * half_w, half_w), half_w)].reshape(xres_out.shape)

    for copy in local[3:]:
        copy.wait()
    normed = abuf[...].reshape(chip_rows, width)
    cos, sin = cos_ref[...], sin_ref[...]

    def rotate(v):
        return (v * cos + pltpu.roll(v, HEAD_DIM // 2, 1) * sin).astype(BF16)

    q = jnp.dot(normed, wqv[...], preferred_element_type=F32)
    for h in range(heads):
        qkv[:, h * HEAD_DIM:(h + 1) * HEAD_DIM] = rotate(q[:, h * HEAD_DIM:(h + 1) * HEAD_DIM])
    qkv[:, head_w:head_w + HEAD_DIM] = rotate(jnp.dot(normed, wkv[...], preferred_element_type=F32))
    qkv[:, head_w + HEAD_DIM:] = jnp.dot(normed, wvv[...], preferred_element_type=F32).astype(BF16)

    def q_rows(p):
        return pl.ds(pl.multiple_of(p * chip_rows, chip_rows), chip_rows)

    qh = head_w // 2
    cuts = (pl.ds(0, qh), pl.ds(qh, qh + 2 * HEAD_DIM))

    def mirror_part(i, block):
        return remote(qkv.at[:, cuts[i]], qall.at[q_rows(block), cuts[i]], ts.at[i], tr.at[i], me.mirrored(core))

    def ring_part(i, step, p, half, device):
        at = qall.at[q_rows(p), pl.ds(i * qh, qh) if half is None else pl.ds(i * qh + half * (qh // 2), qh // 2)]
        return remote(at, at, qs.at[i, step], qr.at[i, step], device)

    @pl.when(moving)
    def _():
        for i in range(2):
            mirror_part(i, x).start()

    @pl.when(jnp.logical_not(moving))
    def _():
        qall[q_rows(vx), :] = qkv[...]

    far, nxt, prev = (vx + 2) % RING, (vx + 1) % RING, (vx + 3) % RING
    q_copies = []
    for i in range(2):
        @pl.when(moving)
        def _():
            mirror_part(i, vx).wait_recv()

        q_copies += [ring_part(i, 0, vx, None, right), ring_part(i, 1, vx, None, left)]
        for copy in q_copies[-2:]:
            copy.start()
    for i in range(2):
        ring_part(i, 0, prev, None, left).wait_recv()
        q_copies.append(ring_part(i, 2, prev, 0, right))
        q_copies[-1].start()
        ring_part(i, 1, nxt, None, right).wait_recv()
        q_copies.append(ring_part(i, 3, nxt, 1, left))
        q_copies[-1].start()
    send_far()
    for i in range(2):
        ring_part(i, 2, far, 0, left).wait_recv()
        ring_part(i, 3, far, 1, right).wait_recv()

    first_lane = jnp.where(lax.broadcasted_iota(jnp.int32, (rows, HEAD_DIM), 1) == 0, 1.0, 0.0).astype(BF16)
    for h in range(heads):
        qaug[h, :, 0:HEAD_DIM] = qall[:, h * HEAD_DIM:(h + 1) * HEAD_DIM]
        qaug[h, :, HEAD_DIM:] = first_lane

    tile = 256
    tiles = rows // tile
    contract_last = (((1,), (1,)), ((), ()))

    def finish(s_ref, e_top, vt_ref, h, j, first, depth):
        lanes = pl.ds(j * tile, tile)
        if first:
            m_new = jnp.maximum(e_top, M_INIT)
        else:
            m_old = acc[h, HEAD_DIM:HEAD_DIM + 1, lanes]
            l_old = acc[h, HEAD_DIM + 1:HEAD_DIM + 2, lanes]
            m_new = jnp.maximum(e_top, m_old)
        m_scaled = m_new * EXP_SCALE
        part_l, o = None, None
        step = min(STEP, depth)
        for k in range(0, depth, step):
            e = jnp.exp2(s_ref[k:k + step, :] * EXP_SCALE - m_scaled)
            total_e = jnp.sum(e.reshape(step // 8, 8, tile), axis=0)
            part_l = total_e if part_l is None else part_l + total_e
            term = jnp.dot(vt_ref[:, k:k + step], e.astype(BF16), preferred_element_type=F32)
            o = term if o is None else o + term
        l_new = jnp.sum(part_l, axis=0, keepdims=True)
        if not first:
            alpha = jnp.exp2((m_old - m_new) * EXP_SCALE)
            l_new = l_new + l_old * alpha
            o = o + acc[h, 0:HEAD_DIM, lanes] * alpha
        acc[h, 0:HEAD_DIM, lanes] = o
        acc[h, HEAD_DIM:HEAD_DIM + 1, lanes] = m_new
        acc[h, HEAD_DIM + 1:HEAD_DIM + 2, lanes] = l_new

    my_rows = q_rows(vx)
    vnew_t = qall[my_rows, head_w + HEAD_DIM:].T
    knew = qall[my_rows, head_w:head_w + HEAD_DIM]

    def new_head(h, carry):
        for j in range(tiles):
            s = lax.dot_general(knew, qaug[h, j * tile:(j + 1) * tile, 0:HEAD_DIM], contract_last, preferred_element_type=F32)
            relk = relative_positions(vx * chip_rows + lax.broadcasted_iota(jnp.int32, s.shape, 0), shards)
            relq = relative_positions(j * tile + lax.broadcasted_iota(jnp.int32, s.shape, 1), shards)
            causal = relk <= relq
            s = jnp.where(causal, s, -jnp.inf)
            finish(s, jnp.max(s, axis=0, keepdims=True), vnew_t, h, j, True, chip_rows)
        return carry

    lax.fori_loop(0, heads, new_head, 0)
    cache_len = len_ref[0]
    slot_ids = lax.broadcasted_iota(jnp.int32, (slots, HEAD_DIM), 0)

    def scores(h, j, dst):
        s = lax.dot_general(kaug[...], qaug[h, j * tile:(j + 1) * tile, :], contract_last, preferred_element_type=F32)
        dst[...] = s
        return jnp.max(s, axis=0, keepdims=True)

    def source(s, carry):
        u, src_core = s // 2, s % 2
        d = u + (u // 2) * (1 - 2 * (u % 2))
        src_x = (x - core * d + RING) % RING
        src_y = (y - (1 - core) * d + RING) % RING
        base = ((2 * src_x + src_core) * RING + src_y) * slots
        for i, (src, dst) in enumerate(((ckv, kbuf), (cvv, vbuf))):
            pltpu.make_async_copy(src.at[:, pl.ds(0, HEAD_DIM)], dst.at[s], kvr.at[s, i]).wait()
        vt[...] = vbuf[s].T
        seen = slot_ids < cache_len - base
        kaug[:, 0:HEAD_DIM] = jnp.where(seen, kbuf[s].astype(F32), 0.0).astype(BF16)
        kaug[:, HEAD_DIM:] = jnp.where(seen, 0.0, MASKED).astype(BF16)

        top_a = scores(0, 0, sa)
        for h in range(heads):
            top_b = scores(h, 1, sb)
            finish(sa, top_a, vt, h, 0, False, slots)
            if h + 1 < heads:
                top_a = scores(h + 1, 0, sa)
            finish(sb, top_b, vt, h, 1, False, slots)
        return carry

    lax.fori_loop(0, 2 * RING, source, 0)

    hh = heads // 2
    lower, upper = pl.ds(0, hh), pl.ds(hh, hh)

    def second(i, heads_at, p, dst, device):
        return remote(acc.at[heads_at, :, q_rows(p)], dst.at[heads_at], rs.at[i], rr.at[i], device)

    p1 = [remote(acc.at[lower, :, q_rows(far)], r1l, rs.at[0], rr.at[0], right),
          remote(acc.at[upper, :, q_rows(far)], r1r, rs.at[1], rr.at[1], left)]
    p2 = [second(2, upper, nxt, r2l, right), second(3, lower, prev, r2r, left),
          second(4, lower, nxt, r2l, right), second(5, upper, prev, r2r, left)]
    for copy in p1 + p2[:2]:
        copy.start()

    def merge(a, b):
        ma, mb = a[:, HEAD_DIM:HEAD_DIM + 1, :], b[:, HEAD_DIM:HEAD_DIM + 1, :]
        m = jnp.maximum(ma, mb)
        wa, wb = jnp.exp2((ma - m) * EXP_SCALE), jnp.exp2((mb - m) * EXP_SCALE)
        o = a[:, 0:HEAD_DIM, :] * wa + b[:, 0:HEAD_DIM, :] * wb
        l = a[:, HEAD_DIM + 1:HEAD_DIM + 2, :] * wa + b[:, HEAD_DIM + 1:HEAD_DIM + 2, :] * wb
        return o, m, l

    def merge_into(lo, p, other):
        o, m, l = merge(acc[lo:lo + hh, :, q_rows(p)], other[...])
        acc[lo:lo + hh, 0:HEAD_DIM, q_rows(p)] = o
        acc[lo:lo + hh, HEAD_DIM:HEAD_DIM + 1, q_rows(p)] = m
        acc[lo:lo + hh, HEAD_DIM + 1:HEAD_DIM + 2, q_rows(p)] = l

    p1[0].wait_recv()
    merge_into(0, nxt, r1l)
    p2[2].start()
    p1[1].wait_recv()
    merge_into(hh, prev, r1r)
    p2[3].start()
    for copy in p2:
        copy.wait_recv()
    def cross_part(i):
        at = pl.ds(i * qh, qh)
        return remote(otmp.at[:, at], obuf.at[core, :, at], os.at[0, i], orr.at[0, i], me.mirrored(core))

    def give_part(i, c):
        at = obuf.at[c, :, pl.ds(i * qh, qh)]
        return remote(at, at, os.at[1, i], orr.at[1, i], partner)

    for h in range(heads):
        a, b, d = acc[h:h + 1, :, q_rows(vx)], r2l[h:h + 1], r2r[h:h + 1]
        o, m, l = merge(a, b)
        md = d[:, HEAD_DIM:HEAD_DIM + 1, :]
        top = jnp.maximum(m, md)
        w, wd = jnp.exp2((m - top) * EXP_SCALE), jnp.exp2((md - top) * EXP_SCALE)
        o = o * w + d[:, 0:HEAD_DIM, :] * wd
        l = l * w + d[:, HEAD_DIM + 1:HEAD_DIM + 2, :] * wd
        otmp[:, h * HEAD_DIM:(h + 1) * HEAD_DIM] = (o / l)[0].T.astype(BF16)
        if h % hh == hh - 1:
            part = h // hh

            @pl.when(moving)
            def _():
                cross_part(part).start()

            @pl.when(jnp.logical_not(moving))
            def _():
                obuf[core, :, part * qh:(part + 1) * qh] = otmp[:, part * qh:(part + 1) * qh]

    for i in range(2):
        @pl.when(moving)
        def _():
            cross_part(i).wait_recv()

        give_part(i, core).start()
    for i in range(2):
        give_part(i, 1 - core).wait_recv()
    o_out[:, 0:head_w] = obuf[0]
    o_out[:, head_w:2 * head_w] = obuf[1]
    for copy in x_copies + kv_copies + q_copies + p1 + p2 + [give_part(0, core), give_part(1, core)]:
        copy.wait_send()

    @pl.when(moving)
    def _():
        for i in range(2):
            mirror_part(i, x).wait_send()
            cross_part(i).wait_send()


def mlp_kernel(o_in, xres, gain, wo, wg, wu, wd, out,
               wgv, wuv, wdv, part, r1l, r1r, r2l, r2r, hbuf, hres, ubuf, fin, fbuf,
               wsem, s1, q1, s2, q2, hs, hr, ps, pr, us, ur, fs, fr):
    me = Place()
    y, core = me.y, me.core
    nc, _, _, cw = part.shape
    half_w = nc * cw
    width = 2 * half_w
    rows = o_in.shape[0]
    block_rows = rows // RING
    half_f = wgv.shape[1]
    uw = 256
    nu = half_f // uw
    partner = me.at(core=1 - core)
    up, down = me.at(dy=1), me.at(dy=RING - 1)
    far, nxt, prev = (y + 2) % RING, (y + 1) % RING, (y + 3) % RING
    col0 = core * half_w

    def lanes(start, size):
        return pl.ds(pl.multiple_of(start, 128), size)

    wo_rows, wd_rows = wo.shape[0], wd.shape[0]
    up_cols, out_cols = lanes(core * half_f, half_f), lanes(col0, half_w)
    wo_load = pltpu.make_async_copy(wo.at[:, out_cols], wdv.at[pl.ds(0, wo_rows), :], wsem.at[0])
    wd_load = pltpu.make_async_copy(wd.at[pl.ds(wo_rows, wd_rows - wo_rows), out_cols], wdv.at[pl.ds(wo_rows, wd_rows - wo_rows), :], wsem.at[1])
    wd_late = pltpu.make_async_copy(wd.at[pl.ds(0, wo_rows), out_cols], wdv.at[pl.ds(0, wo_rows), :], wsem.at[2])
    wg_load = pltpu.make_async_copy(wg.at[:, up_cols], wgv, wsem.at[3])
    wu_load = pltpu.make_async_copy(wu.at[:, up_cols], wuv, wsem.at[4])
    for copy in (wo_load, wg_load, wu_load, wd_load):
        copy.start()

    barrier([up, down, partner])

    hc = cw // 2

    def first_sends(j):
        return (remote(part.at[j, far, :, pl.ds(0, hc)], r1l.at[j], s1.at[0, j], q1.at[0, j], up),
                remote(part.at[j, far, :, pl.ds(hc, hc)], r1r.at[j], s1.at[1, j], q1.at[1, j], down))

    def second_sends(j):
        return (remote(part.at[j, nxt], r2l.at[j], s2.at[0, j], q2.at[0, j], up),
                remote(part.at[j, prev], r2r.at[j], s2.at[1, j], q2.at[1, j], down))

    def relay(j, carry):
        a, b = first_sends(j)
        a.wait_recv()
        part[j, nxt, :, 0:hc] = part[j, nxt, :, 0:hc] + r1l[j]
        b.wait_recv()
        part[j, prev, :, hc:cw] = part[j, prev, :, hc:cw] + r1r[j]
        for copy in second_sends(j):
            copy.start()
        return carry

    def total(j):
        for copy in second_sends(j):
            copy.wait_recv()
        return part[j, y] + r2l[j] + r2r[j]

    def drain(j, carry):
        for copy in first_sends(j) + second_sends(j):
            copy.wait_send()
        return carry

    attended = o_in[...]
    wo_load.wait()

    def out_chunk(j, carry):
        part[j] = jnp.dot(attended, wdv[0:wo_rows, lanes(j * cw, cw)], preferred_element_type=F32).reshape(RING, block_rows, cw)
        for copy in first_sends(j):
            copy.start()
        return carry

    lax.fori_loop(0, nc, out_chunk, 0)
    wd_late.start()
    lax.fori_loop(0, nc, relay, 0)

    def h_piece(c, p, j):
        return hbuf.at[c, p, :, lanes(j * cw, cw)]

    def h_half(c, p, j, i):
        return hbuf.at[c, p, :, lanes(j * cw + i * hc, hc)]

    def h_steps(j):
        return (remote(h_piece(core, y, j), h_piece(core, y, j), hs.at[0, j], hr.at[0, j], up),
                remote(h_piece(core, y, j), h_piece(core, y, j), hs.at[1, j], hr.at[1, j], down),
                remote(h_half(core, prev, j, 0), h_half(core, prev, j, 0), hs.at[2, j], hr.at[2, j], up),
                remote(h_half(core, nxt, j, 1), h_half(core, nxt, j, 1), hs.at[3, j], hr.at[3, j], down))

    def h_give(j, i, p, c):
        return remote(h_piece(c, p, j), h_piece(c, p, j), ps.at[i, j], pr.at[i, j], partner)

    def mid_chunk(j, carry):
        c = lanes(j * cw, cw)
        mid = (xres[:, c].astype(F32) + total(j)).astype(BF16)
        hres[:, c] = mid
        hbuf[core, y, :, c] = mid
        for copy in h_steps(j)[:2] + (h_give(j, 0, y, core),):
            copy.start()
        return carry

    lax.fori_loop(0, nc, mid_chunk, 0)

    def h_forward(j, carry):
        steps = h_steps(j)
        remote(h_piece(core, prev, j), h_piece(core, prev, j), hs.at[0, j], hr.at[0, j], down).wait_recv()
        steps[2].start()
        h_give(j, 1, prev, core).start()
        remote(h_piece(core, nxt, j), h_piece(core, nxt, j), hs.at[1, j], hr.at[1, j], up).wait_recv()
        steps[3].start()
        h_give(j, 2, nxt, core).start()
        return carry

    lax.fori_loop(0, nc, h_forward, 0)

    def h_last(j, carry):
        remote(h_half(core, far, j, 0), h_half(core, far, j, 0), hs.at[2, j], hr.at[2, j], down).wait_recv()
        remote(h_half(core, far, j, 1), h_half(core, far, j, 1), hs.at[3, j], hr.at[3, j], up).wait_recv()
        h_give(j, 3, far, core).start()
        return carry

    lax.fori_loop(0, nc, h_last, 0)

    def h_end(j, carry):
        for i, p in enumerate((y, prev, nxt, far)):
            h_give(j, i, p, 1 - core).wait_recv()
        for copy in h_steps(j):
            copy.wait_send()
        for i, p in enumerate((y, prev, nxt, far)):
            h_give(j, i, p, core).wait_send()
        return carry

    lax.fori_loop(0, nc, h_end, 0)
    lax.fori_loop(0, nc, drain, 0)

    def norm_block(i, carry):
        v0, v1 = hbuf[0, i].astype(F32), hbuf[1, i].astype(F32)
        mean = (jnp.sum(v0 * v0, axis=-1, keepdims=True) + jnp.sum(v1 * v1, axis=-1, keepdims=True)) / width
        inv = lax.rsqrt(mean + NORM_EPS)
        hbuf[0, i] = (v0 * inv * gain[0:half_w].reshape(1, half_w).astype(F32)).astype(BF16)
        hbuf[1, i] = (v1 * inv * gain[half_w:width].reshape(1, half_w).astype(F32)).astype(BF16)
        return carry

    lax.fori_loop(0, RING, norm_block, 0)
    b0, b1 = hbuf[0].reshape(rows, half_w), hbuf[1].reshape(rows, half_w)

    def u_copy(j, c):
        at = ubuf.at[:, lanes(c * half_f + j * uw, uw)]
        return remote(at, at, us.at[j], ur.at[j], partner)

    def up_chunk(j, carry):
        c = lanes(j * uw, uw)
        gate = jnp.dot(b0, wgv[0:half_w, c], preferred_element_type=F32) + jnp.dot(b1, wgv[half_w:width, c], preferred_element_type=F32)
        upper = jnp.dot(b0, wuv[0:half_w, c], preferred_element_type=F32) + jnp.dot(b1, wuv[half_w:width, c], preferred_element_type=F32)
        ubuf[:, lanes(core * half_f + j * uw, uw)] = (jax.nn.silu(gate) * upper).astype(BF16)
        u_copy(j, core).start()
        return carry

    wg_load.wait()
    wu_load.wait()
    lax.fori_loop(0, nu, up_chunk, 0)
    wd_load.wait()
    wd_late.wait()
    for j in range(nu):
        u_copy(j, 1 - core).wait_recv()

    def down_chunk(j, carry):
        part[j] = jnp.dot(ubuf[...], wdv[:, lanes(j * cw, cw)], preferred_element_type=F32).reshape(RING, block_rows, cw)
        for copy in first_sends(j):
            copy.start()
        return carry

    lax.fori_loop(0, nc, down_chunk, 0)
    lax.fori_loop(0, nc, relay, 0)

    def last_chunk(j, carry):
        c = lanes(j * cw, cw)
        fin[:, :, c] = (hres[:, c].astype(F32) + total(j)).astype(BF16).reshape(2, block_rows // 2, cw)
        return carry

    lax.fori_loop(0, nc, last_chunk, 0)
    swap = remote(fin.at[1 - core], fbuf.at[core], fs.at[0], fr.at[0], partner)
    swap.start()
    own = fin[core]
    out[:, lanes(col0, half_w)] = own
    remote(fin.at[core], fbuf.at[1 - core], fs.at[0], fr.at[0], partner).wait_recv()
    out[:, lanes((1 - core) * half_w, half_w)] = fbuf[1 - core]
    for j in range(nu):
        u_copy(j, core).wait_send()
    lax.fori_loop(0, nc, drain, 0)
    swap.wait_send()


def dma(*shape):
    return pltpu.SemaphoreType.DMA(shape)


def relative_positions(r, shards):
    x, y, core, w = r >> 7, (r >> 5) & 3, (r >> 4) & 1, r & 15
    k = (2 * x + core) * RING + y
    run = jnp.where(w < 8, k, 2 * shards - 1 - k)
    return run * 8 + (w & 7)


def solution(mesh):
    token_spec = P(('dp', 'cp', 'tp'), None)
    column_spec = P(None, 'tp')
    row_spec = P('tp', None)
    shards = mesh.shape['tp'] * mesh.shape['cp']

    def device_layer(hidden_loc, pos_loc, cache_len, cache_k, cache_v, norm1_gain, w_query, w_key, w_value, w_out, norm2_gain, w_gate, w_up, w_down):
        shard_rows, width = hidden_loc.shape
        half_w = width // 2
        chip_rows = 2 * RING * shard_rows
        rows = RING * chip_rows
        slots = cache_k.shape[0]
        head_w = w_query.shape[1] // 2
        heads = head_w // HEAD_DIM
        half = HEAD_DIM // 2
        lane = jnp.arange(HEAD_DIM, dtype=jnp.int32)
        rel = relative_positions((lax.axis_index('cp') // 2) * chip_rows + jnp.arange(chip_rows, dtype=jnp.int32), shards)
        inv_freq = 1.0 / (ROPE_BASE ** ((lane % half).astype(F32) * (2.0 / HEAD_DIM)))
        angles = (cache_len[0] + rel).astype(F32)[:, None] * inv_freq[None, :]
        cos, sin = jnp.cos(angles), jnp.sin(angles) * jnp.where(lane < half, -1.0, 1.0)[None, :]
        block = (heads, HEAD_DIM + 8, chip_rows)
        part_block = (heads // 2,) + block[1:]
        attended, xres = pl.pallas_call(
            functools.partial(attention_kernel, shards),
            out_shape=(jax.ShapeDtypeStruct((chip_rows, 2 * head_w), BF16), jax.ShapeDtypeStruct((2 * shard_rows, half_w), BF16)),
            in_specs=[ANY, SMEM, ANY, ANY, VMEM, ANY, ANY, ANY, VMEM, VMEM],
            out_specs=(VMEM, VMEM),
            scratch_shapes=[
                pltpu.VMEM((RING, 2, shard_rows, width), BF16),
                pltpu.VMEM(cache_k.shape, BF16),
                pltpu.VMEM(cache_v.shape, BF16),
                pltpu.VMEM((RING, 2 * shard_rows, width), BF16),
                pltpu.VMEM((width, head_w), BF16),
                pltpu.VMEM((width, HEAD_DIM), BF16),
                pltpu.VMEM((width, HEAD_DIM), BF16),
                pltpu.VMEM((2 * RING, slots, HEAD_DIM), BF16),
                pltpu.VMEM((2 * RING, slots, HEAD_DIM), BF16),
                pltpu.VMEM((2, slots, HEAD_DIM), BF16),
                pltpu.VMEM((2, slots, HEAD_DIM), BF16),
                pltpu.VMEM((slots, 2 * HEAD_DIM), BF16),
                pltpu.VMEM((HEAD_DIM, slots), BF16),
                pltpu.VMEM((chip_rows, head_w + 2 * HEAD_DIM), BF16),
                pltpu.VMEM((rows, head_w + 2 * HEAD_DIM), BF16),
                pltpu.VMEM((heads, rows, 2 * HEAD_DIM), BF16),
                pltpu.VMEM((slots, 256), F32),
                pltpu.VMEM((slots, 256), F32),
                pltpu.VMEM((heads, HEAD_DIM + 8, rows), F32),
                pltpu.VMEM(part_block, F32),
                pltpu.VMEM(part_block, F32),
                pltpu.VMEM(block, F32),
                pltpu.VMEM(block, F32),
                pltpu.VMEM((chip_rows, head_w), BF16),
                pltpu.VMEM((2, chip_rows, head_w), BF16),
                dma(6), *[dma(RING)] * RING, dma(18), dma(2 * RING, 2), dma(2, 2), dma(2), dma(2),
                *[dma(2, RING)] * 2, *[dma(6)] * 2, *[dma(2, 2)] * 2,
            ],
            compiler_params=pltpu.CompilerParams(collective_id=0, has_side_effects=True, vmem_limit_bytes=67043328),
            name='attention',
        )(hidden_loc, cache_len, cache_k, cache_v, norm1_gain, w_query, w_key, w_value, cos, sin)

        cw = 512 if half_w % 512 == 0 and half_w > 512 else 256
        nc = half_w // cw
        half_f = w_gate.shape[1] // 2
        nu = half_f // 256
        br = 2 * shard_rows
        return pl.pallas_call(
            mlp_kernel,
            out_shape=jax.ShapeDtypeStruct((shard_rows, width), BF16),
            in_specs=[VMEM, VMEM, VMEM, ANY, ANY, ANY, ANY],
            out_specs=VMEM,
            scratch_shapes=[
                pltpu.VMEM((width, half_f), BF16),
                pltpu.VMEM((width, half_f), BF16),
                pltpu.VMEM((2 * half_f, half_w), BF16),
                pltpu.VMEM((nc, RING, br, cw), F32),
                pltpu.VMEM((nc, br, cw // 2), F32),
                pltpu.VMEM((nc, br, cw // 2), F32),
                pltpu.VMEM((nc, br, cw), F32),
                pltpu.VMEM((nc, br, cw), F32),
                pltpu.VMEM((2, RING, br, half_w), BF16),
                pltpu.VMEM((br, half_w), BF16),
                pltpu.VMEM((chip_rows, 2 * half_f), BF16),
                pltpu.VMEM((2, shard_rows, half_w), BF16),
                pltpu.VMEM((2, shard_rows, half_w), BF16),
                dma(5), *[dma(2, nc)] * RING,
                *[dma(RING, nc)] * RING, dma(nu), dma(nu), dma(1), dma(1),
            ],
            compiler_params=pltpu.CompilerParams(collective_id=1, has_side_effects=True, vmem_limit_bytes=67043328),
            name='mlp',
        )(attended, xres, norm2_gain, w_out, w_gate, w_up, w_down)

    return jax.shard_map(device_layer, mesh=mesh, in_specs=(token_spec, P(('dp', 'cp', 'tp')), P('dp'), token_spec, token_spec, P(), column_spec, column_spec, column_spec, row_spec, P(), column_spec, column_spec, row_spec), out_specs=token_spec, check_vma=False)
```
